32 devices in a mesh: section: 4 (over x, core), tensor: 4 (over z), dp: 2 (over y).
Axes of the slice: x: 2, y: 2, z: 4, core: 2. Of those that a mesh axis runs over, the one named last changes fastest.
Arguments:
- layer_in: bfloat16 [2, 2, 4, 2, 128, 2560], P(None, None, 'section', 'dp', 'tensor'), may hold values from -6 to 6
- carry_in: bfloat16 [2, 4, 2, 128, 2560], P(None, 'section', 'dp', 'tensor'), may hold values from -6 to 6
- top_grad: bfloat16 [1, 2, 128, 2560], P(None, 'dp', 'tensor'), may hold values from -6 to 6
- w_qkv: bfloat16 [2, 4, 2560, 2560], P(None, 'section', None, 'tensor'), may hold values from -1 to 1
- w_out: bfloat16 [2, 4, 2048, 2560], P(None, 'section', 'tensor'), may hold values from -0.125 to 0.125
- gain: float32 [2, 4, 2560], P(None, 'section'), may hold values from 0.5 to 1.5
Outputs:
- unit_grads: bfloat16 [2, 2, 4, 2, 128, 2560], P(None, None, 'section', 'dp', 'tensor')
- grad_qkv: bfloat16 [2, 4, 2560, 2560], P(None, 'section', 'dp', 'tensor')
- grad_out: bfloat16 [2, 4, 2048, 2560], P(None, 'section', ('tensor', 'dp'))
- grad_gain: float32 [2, 4, 2560], P(None, 'section')
The draws below stay inside these ranges and needn't reach their ends.
All inputs are finite; a program needn't handle non-finite values.
Results may differ from the reference program's by a relative error of at most 0.022.
The reference program's roundings to bfloat16 on the way count: a program that leaves them out, or rounds other values in their place, can miss the bound.
Values may be sent and summed in bfloat16 or wider, within the bound.
A program may use at most 128 MiB of HBM per device.

```python
import math
import jax
import jax.numpy as jnp
from jax import lax

D = 2560
KV = 4
HD = 64
SEQ = 128
TICKS = 2
GROUP = 8
HQ = 2048
QKV = 2560
SECTIONS = 4
REPLICAS = 2
N_TENSOR = 4


def draw_w_qkv(key, part):
    draw_shape = (2, SECTIONS, D, KV, GROUP + 2, HD)
    entries = jax.random.normal(key, draw_shape, jnp.float32) / jnp.sqrt(jnp.float32(D))
    return jnp.clip(entries, -1.0, 1.0).reshape(2, SECTIONS, D, KV * (GROUP + 2) * HD).astype(jnp.bfloat16)


def level_of(stream_key, shape, pieces, smallest, largest):
    def one(axis_at, parts):
        steps = jax.random.uniform(jax.random.fold_in(jax.random.fold_in(stream_key, 6), axis_at), (parts,), jnp.float32, smallest / len(pieces), largest / len(pieces))
        return jnp.repeat(jnp.exp(steps), shape[axis_at] // parts).reshape((-1,) + (1,) * (len(shape) - axis_at - 1))

    factor_of = one(*pieces[0])
    for cut in pieces[1:]:
        factor_of = factor_of * one(*cut)
    return factor_of


def gaussian(own_key, extent, spread, most, cuts=(), kind=jnp.bfloat16):
    values = spread * jax.random.normal(own_key, extent, jnp.float32)
    if cuts:
        values = values * level_of(own_key, extent, cuts, -0.22, 0.18)
    return jnp.clip(values, -most, most).astype(kind)


def setup_inputs(seed: int = 0) -> dict:
    arg_keys = jax.random.split(jax.random.key(seed), 7)
    return {
        "layer_in": gaussian(arg_keys[0], (TICKS, 2, SECTIONS, REPLICAS, SEQ, D), 1.0, 6.0, ((2, 4), (3, 2), (4, 4))),
        "carry_in": gaussian(arg_keys[1], (2, SECTIONS, REPLICAS, SEQ, D), 1.0, 6.0, ((1, 4), (2, 2), (3, 4))),
        "top_grad": gaussian(arg_keys[2], (TICKS - 1, REPLICAS, SEQ, D), 1.0, 6.0, ((1, 2), (2, 4))),
        "w_qkv": draw_w_qkv(jax.random.fold_in(arg_keys[6], 71), 0),
        "w_out": gaussian(arg_keys[4], (2, SECTIONS, HQ, D), HQ ** -0.5, 0.125, ((1, 4), (2, 4))),
        "gain": jnp.clip(1.0 + 0.1 * jax.random.normal(arg_keys[5], (2, SECTIONS, D), jnp.float32), 0.5, 1.5),
    }


epsilon = 1e-06
rope_base = 1000000.0

def rope_tables(length, head_width):
    half_width = head_width // 2
    exponent = jnp.arange(half_width, dtype=jnp.float32) * (2.0 / head_width)
    frequency = rope_base ** (-exponent)
    angle = jnp.arange(length, dtype=jnp.float32)[:, None] * frequency[None, :]
    return (jnp.cos(angle), jnp.sin(angle))

def rotate(values, cosine_table, sine_table, direction):
    half_width = values.shape[-1] // 2
    table_shape = (values.shape[0],) + (1,) * (values.ndim - 2) + (half_width,)
    cosine = cosine_table.reshape(table_shape)
    sine_part = direction * sine_table.reshape(table_shape)
    lower_half = values[..., :half_width]
    upper_half = values[..., half_width:]
    return jnp.concatenate([lower_half * cosine - upper_half * sine_part, upper_half * cosine + lower_half * sine_part], axis=-1)

def layer_backward(layer_rows, grad_output, weight_qkv, weight_out, gain_row):
    length = layer_rows.shape[0]
    cosine_table, sine_table = rope_tables(length, HD)
    inputs_float = layer_rows.astype(jnp.float32)
    inverse = lax.rsqrt(lax.optimization_barrier(jnp.mean(inputs_float * inputs_float, axis=-1, keepdims=True)) + epsilon)
    unit_rows = inputs_float * inverse
    normed = (unit_rows * gain_row).astype(jnp.bfloat16)
    projected = jnp.dot(normed, weight_qkv, preferred_element_type=jnp.float32).reshape(length, KV, GROUP + 2, HD)
    query_rot = rotate(projected[:, :, :GROUP], cosine_table, sine_table, 1.0).astype(jnp.bfloat16)
    key_rot = rotate(projected[:, :, GROUP], cosine_table, sine_table, 1.0).astype(jnp.bfloat16)
    value_rows = projected[:, :, GROUP + 1].astype(jnp.bfloat16)
    query_float = query_rot.astype(jnp.float32)
    key_float = key_rot.astype(jnp.float32)
    value_float = value_rows.astype(jnp.float32)
    score_scale = 1.0 / math.sqrt(HD)
    scores = jnp.einsum('tkgd,ukd->kgtu', query_float, key_float) * score_scale
    causal_mask = jnp.arange(length)[:, None] >= jnp.arange(length)[None, :]
    scores = jnp.where(causal_mask, scores, -1e+30)
    exponentials = jnp.exp(scores - lax.optimization_barrier(jnp.max(scores, axis=-1, keepdims=True)))
    softmax_rows = exponentials / lax.optimization_barrier(jnp.sum(exponentials, axis=-1, keepdims=True))
    softmax_low = softmax_rows.astype(jnp.bfloat16)
    softmax_float = softmax_low.astype(jnp.float32)
    attended = jnp.einsum('kgtu,ukd->tkgd', softmax_float, value_float).astype(jnp.bfloat16).reshape(length, HQ)
    grad_attended = jnp.dot(grad_output, weight_out.T, preferred_element_type=jnp.float32).astype(jnp.bfloat16)
    grad_heads = grad_attended.reshape(length, KV, GROUP, HD).astype(jnp.float32)
    grad_softmax = jnp.einsum('tkgd,ukd->kgtu', grad_heads, value_float)
    row_total = lax.optimization_barrier(jnp.sum(softmax_rows * grad_softmax, axis=-1, keepdims=True))
    grad_scores = (softmax_rows * (grad_softmax - row_total) * score_scale).astype(jnp.bfloat16)
    grad_score_float = grad_scores.astype(jnp.float32)
    grad_value = jnp.einsum('kgtu,tkgd->ukd', softmax_float, grad_heads)
    grad_query = rotate(jnp.einsum('kgtu,ukd->tkgd', grad_score_float, key_float), cosine_table, sine_table, -1.0)
    grad_key = rotate(jnp.einsum('kgtu,tkgd->ukd', grad_score_float, query_float), cosine_table, sine_table, -1.0)
    grad_projected = jnp.concatenate([grad_query, grad_key[:, :, None], grad_value[:, :, None]], axis=2)
    grad_projected = grad_projected.reshape(length, QKV).astype(jnp.bfloat16)
    block_width = QKV // N_TENSOR
    grad_normed = jnp.zeros((length, D), jnp.float32)
    for column_block in range(N_TENSOR):
        lower = column_block * block_width
        block_term = jnp.dot(grad_projected[:, lower:lower + block_width], weight_qkv[:, lower:lower + block_width].T, preferred_element_type=jnp.float32)
        grad_normed = grad_normed + block_term.astype(jnp.bfloat16).astype(jnp.float32)
    grad_unit = grad_normed * gain_row
    grad_rows = inverse * (grad_unit - unit_rows * lax.optimization_barrier(jnp.mean(grad_unit * unit_rows, axis=-1, keepdims=True)))
    grad_input = (grad_output.astype(jnp.float32) + grad_rows).astype(jnp.bfloat16)
    grad_scale = lax.optimization_barrier(jnp.sum(grad_normed * unit_rows, axis=0))
    grad_wqkv = jnp.dot(normed.T, grad_projected, preferred_element_type=jnp.float32)
    grad_wout = jnp.dot(attended.T, grad_output, preferred_element_type=jnp.float32)
    return (grad_input, grad_wqkv, grad_wout, grad_scale)

def reference(layer_in, carry_in, top_grad, w_qkv, w_out, gain):
    ticks = layer_in.shape[0]
    sections = layer_in.shape[2]
    per_replica = (jnp.moveaxis(layer_in, 3, 0), jnp.moveaxis(carry_in, 2, 0), jnp.moveaxis(top_grad, 1, 0))

    def one_replica(totals, slices):
        layer_rows, carried, fresh_grads = slices
        sum_qkv = jnp.zeros(w_qkv.shape, jnp.float32)
        sum_out = jnp.zeros(w_out.shape, jnp.float32)
        gain_total = totals[2]
        produced = {}
        per_tick = []
        for position in range(ticks):
            current = {}
            for member in (1, 0):
                for section_index in range(sections):
                    if position == 0:
                        incoming = carried[member, section_index]
                    elif member == 1 and section_index == 0:
                        incoming = fresh_grads[position - 1]
                    elif member == 1:
                        incoming = produced[1, section_index - 1]
                    elif section_index == sections - 1:
                        incoming = produced[1, section_index]
                    else:
                        incoming = produced[0, section_index + 1]
                    outcome = layer_backward(layer_rows[position, member, section_index], incoming, w_qkv[member, section_index], w_out[member, section_index], gain[member, section_index])
                    current[member, section_index] = outcome[0]
                    sum_qkv = sum_qkv.at[member, section_index].add(outcome[1])
                    sum_out = sum_out.at[member, section_index].add(outcome[2])
                    gain_total = gain_total.at[member, section_index].add(outcome[3])
            produced = current
            per_tick.append(jnp.stack([jnp.stack([current[member, index] for index in range(sections)]) for member in (0, 1)]))
        new_qkv = totals[0] + sum_qkv.astype(jnp.bfloat16).astype(jnp.float32)
        new_out = totals[1] + sum_out.astype(jnp.bfloat16).astype(jnp.float32)
        return ((new_qkv, new_out, gain_total), jnp.stack(per_tick))
    start_totals = (jnp.zeros(w_qkv.shape, jnp.float32), jnp.zeros(w_out.shape, jnp.float32), jnp.zeros(gain.shape, jnp.float32))
    totals, grads_all = lax.scan(one_replica, start_totals, per_replica)
    unit_grads = jnp.moveaxis(grads_all, 0, 3)
    return (unit_grads, totals[0].astype(jnp.bfloat16), totals[1].astype(jnp.bfloat16), totals[2])
```

```python
import functools
import math

import jax
import jax.numpy as jnp
from jax import lax
from jax.experimental import pallas as pl
from jax.experimental.pallas import tpu as pltpu
from jax.sharding import PartitionSpec as P

HD = 64
GROUP = 8

epsilon = 1e-06
rope_base = 1000000.0


MESH = pl.DeviceIdType.MESH
PARTS = 2

contract_rows = (((0,), (0,)), ((), ()))
contract_cols = (((1,), (1,)), ((), ()))


def from_behind(value, axis, steps):
    count = lax.axis_size(axis)
    first, last = (max(0, -steps), min(count, count - steps))
    return lax.ppermute(value, axis, [(source, source + steps) for source in range(first, last)])


def from_ahead(value, axis, steps):
    count = lax.axis_size(axis)
    return lax.ppermute(value, axis, [((i + steps) % count, i) for i in range(count)])


def rope_tables(positions, head_width):
    half_width = head_width // 2
    exponent = jnp.arange(half_width, dtype=jnp.float32) * (2.0 / head_width)
    frequency = rope_base ** (-exponent)
    angle = positions.astype(jnp.float32)[:, None] * frequency[None, :]
    return (jnp.cos(angle), jnp.sin(angle))


def rotate(values, cosine_table, sine_table, direction):
    half_width = values.shape[-1] // 2
    table_shape = (values.shape[0],) + (1,) * (values.ndim - 2) + (half_width,)
    cosine = cosine_table.reshape(table_shape)
    sine_part = direction * sine_table.reshape(table_shape)
    lower_half = values[..., :half_width]
    upper_half = values[..., half_width:]
    return jnp.concatenate(
        [
            lower_half * cosine - upper_half * sine_part,
            upper_half * cosine + lower_half * sine_part,
        ],
        axis=-1,
    )


def unit_compute(normed, grad_full, w_qkv, w_out, tables, mask):
    length = normed.shape[0]
    kv_local = w_out.shape[0] // (GROUP * HD)
    cosine_table, sine_table = tables
    score_scale = 1.0 / math.sqrt(HD)
    projected = jnp.dot(normed, w_qkv, preferred_element_type=jnp.float32)
    projected = projected.reshape(length, kv_local, GROUP + 2, HD)
    query_rot = rotate(projected[:, :, :GROUP], cosine_table, sine_table, 1.0).astype(jnp.bfloat16)
    key_rot = rotate(projected[:, :, GROUP], cosine_table, sine_table, 1.0).astype(jnp.bfloat16)
    value_rows = projected[:, :, GROUP + 1].astype(jnp.bfloat16)
    f32 = dict(preferred_element_type=jnp.float32)
    scores = jnp.einsum("tkgd,ukd->kgtu", query_rot, key_rot, **f32) * score_scale
    scores = jnp.where(mask, scores, -1e30)
    exponentials = jnp.exp(scores - jnp.max(scores, axis=-1, keepdims=True))
    softmax_rows = exponentials / jnp.sum(exponentials, axis=-1, keepdims=True)
    softmax_low = softmax_rows.astype(jnp.bfloat16)
    attended = jnp.einsum("kgtu,ukd->tkgd", softmax_low, value_rows, **f32)
    attended = attended.astype(jnp.bfloat16).reshape(length, kv_local * GROUP * HD)
    grad_attended = lax.dot_general(grad_full, w_out, contract_cols, **f32).astype(jnp.bfloat16)
    grad_heads = grad_attended.reshape(length, kv_local, GROUP, HD)
    grad_softmax = jnp.einsum("tkgd,ukd->kgtu", grad_heads, value_rows, **f32)
    row_total = jnp.sum(softmax_rows * grad_softmax, axis=-1, keepdims=True)
    grad_scores = (softmax_rows * (grad_softmax - row_total) * score_scale).astype(jnp.bfloat16)
    grad_value = jnp.einsum("kgtu,tkgd->ukd", softmax_low, grad_heads, **f32)
    grad_query = rotate(
        jnp.einsum("kgtu,ukd->tkgd", grad_scores, key_rot, **f32), cosine_table, sine_table, -1.0
    )
    grad_key = rotate(
        jnp.einsum("kgtu,tkgd->ukd", grad_scores, query_rot, **f32), cosine_table, sine_table, -1.0
    )
    grad_projected = jnp.concatenate(
        [grad_query, grad_key[:, :, None], grad_value[:, :, None]], axis=2
    )
    grad_projected = grad_projected.reshape(length, kv_local * (GROUP + 2) * HD)
    grad_projected = grad_projected.astype(jnp.bfloat16)
    partial = lax.dot_general(grad_projected, w_qkv, contract_cols, **f32).astype(jnp.bfloat16)
    return attended, grad_projected, partial


def local_permutes(layer_in, carry_in, top_grad, w_qkv, w_out, gain):
    ticks = layer_in.shape[0]
    own = layer_in.shape[4]
    n_tensor = lax.axis_size("tensor")
    n_dp = lax.axis_size("dp")
    me_tensor = lax.axis_index("tensor")
    me_dp = lax.axis_index("dp")
    section_index = lax.axis_index("section")
    at_first = section_index == 0
    at_last = section_index == lax.axis_size("section") - 1
    owners = (me_tensor + jnp.arange(n_tensor)) % n_tensor
    positions = (owners[:, None] * own + jnp.arange(own)[None, :]).reshape(-1)
    tables = rope_tables(positions, HD)
    mask = positions[:, None] >= positions[None, :]
    layer_rows = layer_in[:, :, 0, 0]
    carried = carry_in[:, 0, 0]
    fresh_grads = top_grad[:, 0]
    weight_qkv = w_qkv[:, 0]
    weight_out = w_out[:, 0]
    gain_rows = gain[:, 0]

    def gather(value):
        return jnp.concatenate(
            [value] + [from_ahead(value, "tensor", k) for k in range(1, n_tensor)], axis=0
        )

    def scatter_sum(partial):
        total = partial[:own].astype(jnp.float32)
        for k in range(1, n_tensor):
            chunk = partial[k * own : (k + 1) * own]
            total = total + from_ahead(chunk, "tensor", -k).astype(jnp.float32)
        return total

    def columns_of(value, index):
        width = value.shape[1] // n_dp
        return lax.dynamic_slice_in_dim(value, index * width, width, axis=1)

    def exchange(value, cut):
        if cut:
            return [columns_of(value, me_dp)] + [
                from_ahead(columns_of(value, (me_dp - k) % n_dp), "dp", k) for k in range(1, n_dp)
            ]
        return [value] + [from_ahead(value, "dp", k) for k in range(1, n_dp)]

    members = (1, 0)
    unit_rows, inverse, normed = {}, {}, {}
    for t in range(ticks):
        for m in members:
            rows = layer_rows[t, m].astype(jnp.float32)
            inverse[t, m] = lax.rsqrt(jnp.mean(rows * rows, axis=-1, keepdims=True) + epsilon)
            unit_rows[t, m] = rows * inverse[t, m]
            normed[t, m] = (unit_rows[t, m] * gain_rows[m]).astype(jnp.bfloat16)
    inputs = [carried[0], carried[1]]
    factors = {}
    per_tick = []
    gain_totals = [0.0, 0.0]
    for t in range(ticks):
        outcome = [None, None]
        for m in members:
            dy = inputs[m]
            full_normed = gather(normed[t, m])
            full_grad = gather(dy)
            attended, grad_projected, partial = unit_compute(
                full_normed, full_grad, weight_qkv[m], weight_out[m], tables, mask
            )
            factors[t, m] = (
                exchange(full_normed, True),
                exchange(grad_projected, False),
                exchange(attended, True),
                exchange(full_grad, False),
            )
            grad_normed = scatter_sum(partial)
            grad_unit = grad_normed * gain_rows[m]
            unit = unit_rows[t, m]
            grad_rows = inverse[t, m] * (
                grad_unit - unit * jnp.mean(grad_unit * unit, axis=-1, keepdims=True)
            )
            outcome[m] = (dy.astype(jnp.float32) + grad_rows).astype(jnp.bfloat16)
            gain_totals[m] = gain_totals[m] + jnp.sum(grad_normed * unit, axis=0)
        if t + 1 < ticks:
            upward = from_behind(outcome[1], "section", 1)
            downward = from_behind(outcome[0], "section", -1)
            inputs = [
                jnp.where(at_last, outcome[1], downward),
                jnp.where(at_first, fresh_grads[t], upward),
            ]
        per_tick.append(jnp.stack(outcome))

    def weight_grad(m, left, right):
        total = None
        for k in range(n_dp):
            a = jnp.concatenate([factors[t, m][left][k] for t in range(ticks)], axis=0)
            b = jnp.concatenate([factors[t, m][right][k] for t in range(ticks)], axis=0)
            part = lax.dot_general(a, b, contract_rows, preferred_element_type=jnp.float32)
            part = part.astype(jnp.bfloat16).astype(jnp.float32)
            total = part if total is None else total + part
        return total.astype(jnp.bfloat16)

    grad_qkv = jnp.stack([weight_grad(m, 0, 1) for m in (0, 1)])
    grad_out = jnp.stack([weight_grad(m, 2, 3) for m in (0, 1)])
    gain_total = lax.psum(jnp.stack(gain_totals), ("tensor", "dp"))
    return (
        jnp.stack(per_tick)[:, :, None, None],
        grad_qkv[:, None],
        grad_out[:, None],
        gain_total[:, None],
    )


def fused(
    n, reps, ticks, sections, own,
    x_hbm, carry, top, gain_hbm, wq_hbm, wo_hbm, cos_hbm, sin_hbm,
    out, gq_out, go_out, gain_out,
    wq, wo, xb, gain, cos_ref, sin_ref,
    nrm, dyb, gpb, attb, pnrm, pdy, pgp, patt, pb, rb, smb, qsb, kb, vb, gtot, grecv, gsum,
    w_sem, x_sem, c_sem, t_sem, g_send, g_recv, r_send, r_recv, s_send, s_recv, d_send, d_recv,
    gain_send, gain_recv,
):
    f32 = jnp.float32
    bf16 = jnp.bfloat16
    me = lax.axis_index("tensor")
    rep = lax.axis_index("dp")
    sec = lax.axis_index("section")
    length = n * own
    units = 2 * ticks
    hq = wo.shape[1]
    width = wq.shape[1]
    cols = wq.shape[2]
    groups = hq // (GROUP * HD)
    wn = width // reps
    wa = hq // reps
    scale = 1.0 / math.sqrt(HD)
    parts = PARTS if width % (PARTS * 128) == 0 else 1
    piece = width // parts

    def tensor_at(k):
        return {"tensor": lax.rem(me + k + n, n)}

    def dp_at(k):
        return {"dp": lax.rem(rep + k + reps, reps)}

    barrier = pltpu.get_barrier_semaphore()
    for a in range(n):
        for b in range(reps):
            if a or b:
                pl.semaphore_signal(
                    barrier, inc=1, device_id={**tensor_at(a), **dp_at(b)}, device_id_type=MESH
                )

    @pl.when(sec > 0)
    def _():
        pl.semaphore_signal(barrier, inc=1, device_id={"section": sec - 1}, device_id_type=MESH)

    @pl.when(sec < sections - 1)
    def _():
        pl.semaphore_signal(barrier, inc=1, device_id={"section": sec + 1}, device_id_type=MESH)

    def at_rows(t, i):
        return pl.ds(pl.multiple_of(t * length + i * own, own), own)

    def whole(t):
        return pl.ds(t * length, length)

    def lanes(h):
        return pl.ds(h * piece, piece)

    def unit_of(t, m):
        return 2 * t + m

    order = [(t, m) for t in range(ticks) for m in (1, 0)]

    x_copies = {}
    for t, m in order:
        u = unit_of(t, m)
        x_copies[t, m] = pltpu.make_async_copy(x_hbm.at[u], xb.at[u], x_sem.at[u])
    small = [
        pltpu.make_async_copy(src, dst, t_sem.at[k])
        for k, (src, dst) in enumerate(((gain_hbm, gain), (cos_hbm, cos_ref), (sin_hbm, sin_ref)))
    ]
    carry_copies = [
        pltpu.make_async_copy(carry.at[m], dyb.at[m, at_rows(0, me)], c_sem.at[m]) for m in (1, 0)
    ]
    top_copies = [
        pltpu.make_async_copy(top.at[t], dyb.at[1, at_rows(t + 1, me)], c_sem.at[2 + t])
        for t in range(ticks - 1)
    ]
    w_copies = [
        pltpu.make_async_copy(src.at[m], dst.at[m], w_sem.at[j, m])
        for m in (1, 0)
        for j, (src, dst) in enumerate(((wq_hbm, wq), (wo_hbm, wo)))
    ]
    small[0].start()
    x_copies[0, 1].start()
    for c in carry_copies:
        c.start()
    for t, m in order[1:]:
        x_copies[t, m].start()
    for c in small[1:]:
        c.start()

    @pl.when(sec == 0)
    def _():
        for c in top_copies:
            c.start()

    for c in w_copies:
        c.start()

    def normalize(t, m):
        u = unit_of(t, m)
        x_copies[t, m].wait()
        x = xb[u].astype(f32)
        inverse = lax.rsqrt(jnp.mean(x * x, axis=-1, keepdims=True) + epsilon)
        nrm[m, at_rows(t, me)] = (x * inverse * gain[m]).astype(bf16)

    small[0].wait()
    for t, m in order:
        normalize(t, m)
    for c in carry_copies:
        c.wait()
    gtot[...] = jnp.zeros_like(gtot)

    neighbours = jnp.where(sec > 0, 1, 0) + jnp.where(sec < sections - 1, 1, 0)
    with jax.named_scope("barrier"):
        pl.semaphore_wait(barrier, n * reps - 1 + neighbours)

    def remote(src, dst, send, recv, where):
        return pltpu.make_async_remote_copy(
            src_ref=src, dst_ref=dst, send_sem=send, recv_sem=recv, device_id=where,
            device_id_type=MESH,
        )

    def hop(which, t, m, i, h, up):
        u = unit_of(t, m)
        at = (nrm, dyb)[which].at[m, at_rows(t, i), lanes(h)]
        return remote(
            at, at, g_send.at[which, u, h, up, i], g_recv.at[which, u, h, i],
            tensor_at(1 if up else -1),
        )

    def dy_peer(t, m, i, h, j):
        u = unit_of(t, m)
        at = at_rows(t, i)
        return remote(
            dyb.at[m, at, lanes(h)], pdy.at[j - 1, m, at, lanes(h)],
            d_send.at[1, u, j], d_recv.at[1, u, j], dp_at(-j),
        )

    def nrm_peer(t, m, i, j):
        u = unit_of(t, m)
        peer = lax.rem(rep - j + reps, reps)
        at = at_rows(t, i)
        return remote(
            nrm.at[m, at, pl.ds(pl.multiple_of(peer * wn, 128), wn)], pnrm.at[j - 1, m, at],
            d_send.at[0, u, j], d_recv.at[0, u, j], dp_at(-j),
        )

    def rest_peer(which, t, m, j):
        u = unit_of(t, m)
        peer = lax.rem(rep - j + reps, reps)
        at = whole(t)
        src, dst = {
            2: (gpb.at[m, at], pgp),
            3: (attb.at[m, at, pl.ds(pl.multiple_of(peer * wa, 128), wa)], patt),
        }[which]
        return remote(
            src, dst.at[j - 1, m, at], d_send.at[which, u, j], d_recv.at[which, u, j], dp_at(-j)
        )

    def peer_total(which, t, m, j):
        u = unit_of(t, m)
        at = (pnrm, pdy, pgp, patt)[which].at[j - 1, m, whole(t)]
        return remote(at, at, d_send.at[which, u, j], d_recv.at[which, u, j], dp_at(-j))

    others = range(1, reps)
    far = range(1, n)

    def to_peers(which, t, m, i, h):
        for j in others:
            if which:
                dy_peer(t, m, i, h, j).start()
            elif h == parts - 1:
                nrm_peer(t, m, i, j).start()

    def own_to_peers(which, t, m):
        for h in range(parts):
            to_peers(which, t, m, me, h)

    def own_hops(which, t, m, edge=None):
        for h in range(parts):
            for up in (1, 0):
                sends = me < n - 1 if up else me > 0
                if edge is not None:
                    sends = (me == 0 if up else me == n - 1) if edge else (me > 0) & (me < n - 1)

                @pl.when(sends)
                def _():
                    hop(which, t, m, me, h, up).start()

    def arrivals(which, t, m, d, forward, source):
        for h in range(parts):
            for up in (1, 0):
                i = me - d if up else me + d
                inside = me >= d if up else me + d < n
                if source == "edge":
                    inside = me == d if up else me + d == n - 1
                elif source == "middle":
                    inside = me > d if up else me + d < n - 1
                middle = me < n - 1 if up else me > 0
                edge = me == n - 1 if up else me == 0

                @pl.when(inside & (middle if forward else edge))
                def _():
                    with jax.named_scope("wait_fwd" if forward else "wait_end"):
                        hop(which, t, m, i, h, up).wait_recv()
                    if forward:
                        hop(which, t, m, i, h, up).start()
                    to_peers(which, t, m, i, h)

    def fwd(what, t, m, *ds, source=None):
        for d in ds:
            if 0 < d < n - 1:
                for which in what:
                    arrivals(which, t, m, d, True, source)

    def end(what, t, m, *ds):
        for d in ds:
            if 0 < d < n:
                for which in what:
                    arrivals(which, t, m, d, False, None)

    def sum_copy(t, m, d, h, way):
        u = unit_of(t, m)
        i = me + d if way else me - d
        return remote(
            pb.at[u, pl.ds(pl.multiple_of(i * own, own), own), lanes(h)],
            rb.at[u, way, d - 1, :, lanes(h)],
            r_send.at[u, way, d, h], r_recv.at[u, way, d - 1, h], tensor_at(1 if way else -1),
        )

    def sum_arrived(t, m, d, h, way):
        u = unit_of(t, m)
        at = rb.at[u, way, d, :, lanes(h)]
        remote(
            at, at, r_send.at[u, way, d, h], r_recv.at[u, way, d, h], tensor_at(1)
        ).wait_recv()

    def sum_stage(t, m, stage):
        u = unit_of(t, m)
        for way in (1, 0):

            @pl.when(me == (stage if way else n - 1 - stage))
            def _():
                place = stage if way else n - 1 - stage
                for d in range(n - 1 - stage, 0, -1):
                    i = place + d if way else place - d
                    at = pl.ds(i * own, own)
                    for h in range(parts):
                        if stage:
                            with jax.named_scope("wait_sum"):
                                sum_arrived(t, m, d, h, way)
                            total = pb[u, at, lanes(h)].astype(f32)
                            total = total + rb[u, way, d, :, lanes(h)].astype(f32)
                            pb[u, at, lanes(h)] = total.astype(bf16)
                        sum_copy(t, m, d, h, way).start()

    def sums(t, m, *stages):
        for stage in stages:
            if 0 < stage < n - 1:
                sum_stage(t, m, stage)

    def sums_sent(t, m):
        for way in (1, 0):
            for stage in range(n - 1):

                @pl.when(me == (stage if way else n - 1 - stage))
                def _():
                    for d in range(n - 1 - stage, 0, -1):
                        for h in range(parts):
                            sum_copy(t, m, d, h, way).wait_send()

    def section_copy(t, m):
        step = 1 if m == 1 else -1
        return remote(
            out.at[unit_of(t, m)], dyb.at[m, at_rows(t + 1, me)], s_send.at[t, m],
            s_recv.at[t, m], {"section": sec + step},
        )

    def gain_copy(a, b):
        slot = a * reps + b
        return remote(
            gtot, grecv.at[slot], gain_send.at[slot], gain_recv.at[slot],
            {**tensor_at(-a), **dp_at(-b)},
        )

    def swap(values):
        wide = values.shape[1]
        lane = lax.broadcasted_iota(jnp.int32, values.shape, 1)
        low = lax.rem(lane, HD) < HD // 2
        return jnp.where(
            low, pltpu.roll(values, wide - HD // 2, 1), pltpu.roll(values, HD // 2, 1)
        )

    def dot(a, b, ca, cb):
        return lax.dot_general(a, b, (((ca,), (cb,)), ((), ())), preferred_element_type=f32)

    def stack_heads(values):
        return jnp.concatenate([values[:, h * HD : (h + 1) * HD] for h in range(GROUP)], axis=0)

    def spread_heads(values):
        return jnp.concatenate(
            [values[h * length : (h + 1) * length] for h in range(GROUP)], axis=1
        )

    def table(ref, wide):
        return jnp.concatenate([ref[...]] * (wide // 128), axis=1)

    span = (GROUP + 2) * HD

    def forward(t, m):
        u = unit_of(t, m)
        projected = dot(nrm[m, whole(t)], wq[m], 1, 0)
        rotated = projected * table(cos_ref, cols) + swap(projected) * table(sin_ref, cols)
        rotated = rotated.astype(bf16)
        row = lax.broadcasted_iota(jnp.int32, (length, length), 0)
        key_row = lax.broadcasted_iota(jnp.int32, (length, length), 1)
        bias = jnp.where(row >= key_row, 0.0, -1e30)
        for g in range(groups):
            at = g * span
            qs = stack_heads(rotated[:, at : at + GROUP * HD])
            key = rotated[:, at + GROUP * HD : at + (GROUP + 1) * HD]
            value = projected[:, at + (GROUP + 1) * HD : at + span].astype(bf16)
            scores = dot(qs, key, 1, 1) * scale
            scores = (scores.reshape(GROUP, length, length) + bias[None]).reshape(
                GROUP * length, length
            )
            e = jnp.exp(scores - jnp.max(scores, axis=-1, keepdims=True))
            sm = e / jnp.sum(e, axis=-1, keepdims=True)
            smb[u, g] = sm
            qsb[u, g] = qs
            kb[u, g] = key
            vb[u, g] = value
            attended = spread_heads(dot(sm.astype(bf16), value, 1, 0).astype(bf16))
            attb[m, whole(t), g * GROUP * HD : (g + 1) * GROUP * HD] = attended
        for j in others:
            rest_peer(3, t, m, j).start()

    def backward(t, m):
        u = unit_of(t, m)
        grad_att = dot(dyb[m, whole(t)], wo[m], 1, 1).astype(bf16)
        for g in range(groups):
            sm = smb[u, g]
            low = sm.astype(bf16)
            value = vb[u, g]
            gs = stack_heads(grad_att[:, g * GROUP * HD : (g + 1) * GROUP * HD])
            gsm = dot(gs, value, 1, 1)
            total = jnp.sum(sm * gsm, axis=-1, keepdims=True)
            gsc = (sm * (gsm - total) * scale).astype(bf16)
            g_value = dot(low, gs, 0, 0)
            g_query = spread_heads(dot(gsc, kb[u, g], 1, 0))
            g_key = dot(gsc, qsb[u, g], 0, 0)
            turned = jnp.concatenate([g_query, g_key, g_value], axis=1)
            back = turned * table(cos_ref, span) - swap(turned) * table(sin_ref, span)
            lane = lax.broadcasted_iota(jnp.int32, turned.shape, 1)
            back = jnp.where(lane < (GROUP + 1) * HD, back, turned)
            gpb[m, whole(t), g * span : (g + 1) * span] = back.astype(bf16)
        pb[u] = dot(gpb[m, whole(t)], wq[m], 1, 1).astype(bf16)
        sum_stage(t, m, 0)
        for j in others:
            rest_peer(2, t, m, j).start()

    def finish(t, m):
        u = unit_of(t, m)
        x = xb[u].astype(f32)
        inverse = lax.rsqrt(jnp.mean(x * x, axis=-1, keepdims=True) + epsilon)
        unit = x * inverse
        mine = pl.ds(pl.multiple_of(me * own, own), own)
        gsum[...] = pb[u, mine].astype(f32)
        for way in (1, 0):

            @pl.when(me > 0 if way else me < n - 1)
            def _():
                with jax.named_scope("wait_scatter"):
                    for h in range(parts):
                        sum_arrived(t, m, 0, h, way)
                gsum[...] = gsum[...] + rb[u, way, 0].astype(f32)

        gn = gsum[...]
        gu = gn * gain[m]
        grad = inverse * (gu - unit * jnp.mean(gu * unit, axis=-1, keepdims=True))
        out[u] = (dyb[m, at_rows(t, me)].astype(f32) + grad).astype(bf16)
        gtot[m] = gtot[m] + jnp.sum(gn * unit, axis=0, keepdims=True)

    def hand_over(t, m):
        if t + 1 == ticks:
            return

        @pl.when(sec < sections - 1 if m == 1 else sec > 0)
        def _():
            section_copy(t, m).start()

        if m == 1:

            @pl.when(sec == sections - 1)
            def _():
                dyb[0, at_rows(t + 1, me)] = out[unit_of(t, 1)]

    def taken_over(t, m):
        with jax.named_scope("wait_section"):

            @pl.when(sec > 0 if m == 1 else sec < sections - 1)
            def _():
                section_copy(t - 1, m).wait_recv()

            if m == 1:

                @pl.when(sec == 0)
                def _():
                    top_copies[t - 1].wait()

    def wait_peers(m, *kinds):
        with jax.named_scope("wait_dp"):
            for t in range(ticks):
                for which in kinds:
                    for j in others:
                        peer_total(which, t, m, j).wait_recv()

    def rounded(a, b):
        return dot(a, b, 0, 0).astype(bf16).astype(f32)

    def grad_out(m):
        wide = 512 if width % 512 == 0 else 128
        att_at = pl.ds(pl.multiple_of(rep * wa, 128), wa)

        @pl.loop(0, width // wide)
        def _(c):
            at = pl.ds(pl.multiple_of(c * wide, 128), wide)
            total = rounded(attb[m, :, att_at], dyb[m, :, at])
            for j in others:
                total = total + rounded(patt[j - 1, m], pdy[j - 1, m, :, at])
            go_out[m, :, at] = total.astype(bf16)

    def grad_qkv(m):
        block = 256 if wn % 256 == 0 else 128

        @pl.loop(0, wn // block)
        def _(c):
            own_at = pl.ds(pl.multiple_of(rep * wn + c * block, 128), block)
            at = pl.ds(pl.multiple_of(c * block, 128), block)
            total = rounded(nrm[m, :, own_at], gpb[m])
            for j in others:
                total = total + rounded(pnrm[j - 1, m, :, at], pgp[j - 1, m])
            gq_out[m, at] = total.astype(bf16)

    def grads_of(m):
        wait_peers(m, 1, 3)
        with jax.named_scope("grad_out"):
            grad_out(m)
        wait_peers(m, 0, 2)
        with jax.named_scope("grad_qkv"):
            grad_qkv(m)

    inner = range(1, n - 1)
    dy, x = 1, 0
    both = (dy, x)

    for m in (1, 0):
        for which in both:
            if m == 1:
                own_hops(which, 0, m)
            own_to_peers(which, 0, m)
    for t, m in order[2:]:
        own_to_peers(x, t, m)
    fwd(both, 0, 1, *inner)
    end(both, 0, 1, *inner)
    for which in both:
        own_hops(which, 0, 0)
    with jax.named_scope("wait_weights"):
        for c in w_copies:
            c.wait()
        for c in small[1:]:
            c.wait()
    end(both, 0, 1, n - 1)
    with jax.named_scope("forward"):
        forward(0, 1)
    with jax.named_scope("backward"):
        backward(0, 1)
    own_hops(x, 1, 1, edge=True)
    fwd(both, 0, 0, 1)
    end(both, 0, 0, 1)
    fwd(both, 0, 0, *inner[1:])
    end(both, 0, 0, *inner[1:])

    def give(which, t, m):
        fwd((which,), t, m, 1, source="middle")
        fwd((which,), t, m, 1, source="edge")

    for t in range(1, ticks):
        late = both if t == 1 else (dy,)
        if t > 1:
            own_hops(x, t, 1, edge=True)
        sums(t - 1, 1, 1)
        end(late, t - 1, 0, n - 1)
        if t == 1:
            with jax.named_scope("forward"):
                forward(t - 1, 0)
        sums(t - 1, 1, *inner[1:])
        own_hops(x, t, 1, edge=False)
        with jax.named_scope("backward"):
            backward(t - 1, 0)
        give(x, t, 1)
        finish(t - 1, 1)
        hand_over(t - 1, 1)
        fwd((x,), t, 1, *inner[1:])
        end((x,), t, 1, 1)
        taken_over(t, 1)
        own_to_peers(dy, t, 1)
        own_hops(dy, t, 1)
        end((x,), t, 1, *far[1:-1])
        fwd((dy,), t, 1, 1, source="middle")
        end((x,), t, 1, n - 1)
        with jax.named_scope("forward"):
            forward(t, 1)
        own_hops(x, t, 0, edge=True)
        sums(t - 1, 0, 1)
        fwd((dy,), t, 1, 1, source="edge")
        sums(t - 1, 0, *inner[1:])
        fwd((dy,), t, 1, *inner[1:])
        own_hops(x, t, 0, edge=False)
        end((dy,), t, 1, *far)
        with jax.named_scope("backward"):
            backward(t, 1)
        finish(t - 1, 0)
        hand_over(t - 1, 0)
        give(x, t, 0)
        fwd((x,), t, 0, *inner[1:])
        end((x,), t, 0, 1)
        taken_over(t, 0)
        own_to_peers(dy, t, 0)
        own_hops(dy, t, 0)
        end((x,), t, 0, *far[1:-1])
        fwd((dy,), t, 0, 1, source="middle")
        if t + 1 == ticks:
            sums(t, 1, 1)
        end((x,), t, 0, n - 1)
        with jax.named_scope("forward"):
            forward(t, 0)
        fwd((dy,), t, 0, 1, source="edge")
        fwd((dy,), t, 0, *inner[1:])
        if t + 1 == ticks:
            sums(t, 1, *inner[1:])
        end((dy,), t, 0, *(far if t + 1 == ticks else far[:-1]))

    last = ticks - 1
    with jax.named_scope("backward"):
        backward(last, 0)
    finish(last, 1)
    grads_of(1)
    sums(last, 0, *inner)
    finish(last, 0)
    for a in range(n):
        for b in range(reps):
            if a or b:
                gain_copy(a, b).start()
    grads_of(0)
    total = gtot[...]
    for a in range(n):
        for b in range(reps):
            if a or b:
                gain_copy(a, b).wait_recv()
                total = total + grecv[a * reps + b]
    gain_out[...] = total
    with jax.named_scope("wait_sends"):
        for t, m in order:
            sums_sent(t, m)
            for which in both:
                for h in range(parts):
                    for i in range(n):
                        for up in (1, 0):

                            @pl.when((me < n - 1) & (me >= i) if up else (me > 0) & (me <= i))
                            def _():
                                hop(which, t, m, i, h, up).wait_send()

            for j in others:
                for which in range(4):
                    peer_total(which, t, m, j).wait_send()
        for t in range(ticks - 1):

            @pl.when(sec < sections - 1)
            def _():
                section_copy(t, 1).wait_send()

            @pl.when(sec > 0)
            def _():
                section_copy(t, 0).wait_send()

        for a in range(n):
            for b in range(reps):
                if a or b:
                    gain_copy(a, b).wait_send()


def lane_tables(length):
    cosine, sine = rope_tables(jnp.arange(length), HD)
    copies = 128 // HD
    cosine = jnp.tile(jnp.concatenate([cosine, cosine], axis=1), (1, copies))
    sine = jnp.tile(jnp.concatenate([-sine, sine], axis=1), (1, copies))
    return cosine, sine


def local(layer_in, carry_in, top_grad, w_qkv, w_out, gain):
    ticks, own, width = layer_in.shape[0], layer_in.shape[4], layer_in.shape[5]
    n = lax.axis_size("tensor")
    reps = lax.axis_size("dp")
    sections = lax.axis_size("section")
    cols, hq = w_qkv.shape[3], w_out.shape[2]
    lined = (width // reps) % 128 == 0 and (hq // reps) % 128 == 0 and cols % 128 == 0
    if not lined or own % 16 or ticks < 2 or n < 3:
        return local_permutes(layer_in, carry_in, top_grad, w_qkv, w_out, gain)
    length = n * own
    units = 2 * ticks
    deep = ticks * length
    groups = hq // (GROUP * HD)
    wn, wa = width // reps, hq // reps
    f32, bf16 = jnp.float32, jnp.bfloat16
    parts = PARTS if width % (PARTS * 128) == 0 else 1
    with jax.ensure_compile_time_eval():
        cosine, sine = lane_tables(length)
    vmem = pl.BlockSpec(memory_space=pltpu.VMEM)
    hbm = pl.BlockSpec(memory_space=pl.ANY)
    dma = pltpu.SemaphoreType.DMA
    outs = pl.pallas_call(
        functools.partial(fused, n, reps, ticks, sections, own),
        out_shape=(
            jax.ShapeDtypeStruct((units, own, width), bf16),
            jax.ShapeDtypeStruct((2, wn, cols), bf16),
            jax.ShapeDtypeStruct((2, wa, width), bf16),
            jax.ShapeDtypeStruct((2, 1, width), f32),
        ),
        in_specs=[hbm] * 8,
        out_specs=(vmem,) * 4,
        scratch_shapes=[
            pltpu.VMEM((2, width, cols), bf16),
            pltpu.VMEM((2, hq, width), bf16),
            pltpu.VMEM((units, own, width), bf16),
            pltpu.VMEM((2, 1, width), f32),
            pltpu.VMEM((length, 128), f32),
            pltpu.VMEM((length, 128), f32),
            pltpu.VMEM((2, deep, width), bf16),
            pltpu.VMEM((2, deep, width), bf16),
            pltpu.VMEM((2, deep, cols), bf16),
            pltpu.VMEM((2, deep, hq), bf16),
            pltpu.VMEM((reps - 1, 2, deep, wn), bf16),
            pltpu.VMEM((reps - 1, 2, deep, width), bf16),
            pltpu.VMEM((reps - 1, 2, deep, cols), bf16),
            pltpu.VMEM((reps - 1, 2, deep, wa), bf16),
            pltpu.VMEM((units, length, width), bf16),
            pltpu.VMEM((units, 2, n - 1, own, width), bf16),
            pltpu.VMEM((units, groups, GROUP * length, length), f32),
            pltpu.VMEM((units, groups, GROUP * length, HD), bf16),
            pltpu.VMEM((units, groups, length, HD), bf16),
            pltpu.VMEM((units, groups, length, HD), bf16),
            pltpu.VMEM((2, 1, width), f32),
            pltpu.VMEM((n * reps, 2, 1, width), f32),
            pltpu.VMEM((own, width), f32),
            dma((2, 2)),
            dma((units,)),
            dma((1 + ticks,)),
            dma((3,)),
            dma((2, units, parts, 2, n)),
            dma((2, units, parts, n)),
            dma((units, 2, n, parts)),
            dma((units, 2, n, parts)),
            dma((ticks, 2)),
            dma((ticks, 2)),
            dma((4, units, reps)),
            dma((4, units, reps)),
            dma((n * reps,)),
            dma((n * reps,)),
        ],
        compiler_params=pltpu.CompilerParams(
            collective_id=0, has_side_effects=True, vmem_limit_bytes=64 * 1024 * 1024 - 65536
        ),
    )(
        layer_in[:, :, 0, 0].reshape(units, own, width),
        carry_in[:, 0, 0],
        top_grad[:, 0],
        gain,
        w_qkv[:, 0],
        w_out[:, 0],
        cosine,
        sine,
    )
    return (
        outs[0].reshape(ticks, 2, 1, 1, own, width),
        outs[1][:, None],
        outs[2][:, None],
        outs[3],
    )


def solution(mesh):
    in_specs = (
        P(None, None, "section", "dp", "tensor", None),
        P(None, "section", "dp", "tensor", None),
        P(None, "dp", "tensor", None),
        P(None, "section", None, "tensor"),
        P(None, "section", "tensor", None),
        P(None, "section", None),
    )
    out_specs = (
        P(None, None, "section", "dp", "tensor", None),
        P(None, "section", "dp", "tensor"),
        P(None, "section", ("tensor", "dp"), None),
        P(None, "section", None),
    )
    return jax.shard_map(local, mesh=mesh, in_specs=in_specs, out_specs=out_specs, check_vma=False)
```

```python
import functools
import math

import jax
import jax.numpy as jnp
from jax import lax
from jax.experimental import pallas as pl
from jax.experimental.pallas import tpu as pltpu
from jax.sharding import PartitionSpec as P

HD = 64
GROUP = 8

epsilon = 1e-06
rope_base = 1000000.0


MESH = pl.DeviceIdType.MESH
PARTS = 2

contract_rows = (((0,), (0,)), ((), ()))
contract_cols = (((1,), (1,)), ((), ()))


def from_behind(value, axis, steps):
    count = lax.axis_size(axis)
    first, last = (max(0, -steps), min(count, count - steps))
    return lax.ppermute(value, axis, [(source, source + steps) for source in range(first, last)])


def from_ahead(value, axis, steps):
    count = lax.axis_size(axis)
    return lax.ppermute(value, axis, [((i + steps) % count, i) for i in range(count)])


def rope_tables(positions, head_width):
    half_width = head_width // 2
    exponent = jnp.arange(half_width, dtype=jnp.float32) * (2.0 / head_width)
    frequency = rope_base ** (-exponent)
    angle = positions.astype(jnp.float32)[:, None] * frequency[None, :]
    return (jnp.cos(angle), jnp.sin(angle))


def rotate(values, cosine_table, sine_table, direction):
    half_width = values.shape[-1] // 2
    table_shape = (values.shape[0],) + (1,) * (values.ndim - 2) + (half_width,)
    cosine = cosine_table.reshape(table_shape)
    sine_part = direction * sine_table.reshape(table_shape)
    lower_half = values[..., :half_width]
    upper_half = values[..., half_width:]
    return jnp.concatenate(
        [
            lower_half * cosine - upper_half * sine_part,
            upper_half * cosine + lower_half * sine_part,
        ],
        axis=-1,
    )


def unit_compute(normed, grad_full, w_qkv, w_out, tables, mask):
    length = normed.shape[0]
    kv_local = w_out.shape[0] // (GROUP * HD)
    cosine_table, sine_table = tables
    score_scale = 1.0 / math.sqrt(HD)
    projected = jnp.dot(normed, w_qkv, preferred_element_type=jnp.float32)
    projected = projected.reshape(length, kv_local, GROUP + 2, HD)
    query_rot = rotate(projected[:, :, :GROUP], cosine_table, sine_table, 1.0).astype(jnp.bfloat16)
    key_rot = rotate(projected[:, :, GROUP], cosine_table, sine_table, 1.0).astype(jnp.bfloat16)
    value_rows = projected[:, :, GROUP + 1].astype(jnp.bfloat16)
    f32 = dict(preferred_element_type=jnp.float32)
    scores = jnp.einsum("tkgd,ukd->kgtu", query_rot, key_rot, **f32) * score_scale
    scores = jnp.where(mask, scores, -1e30)
    exponentials = jnp.exp(scores - jnp.max(scores, axis=-1, keepdims=True))
    softmax_rows = exponentials / jnp.sum(exponentials, axis=-1, keepdims=True)
    softmax_low = softmax_rows.astype(jnp.bfloat16)
    attended = jnp.einsum("kgtu,ukd->tkgd", softmax_low, value_rows, **f32)
    attended = attended.astype(jnp.bfloat16).reshape(length, kv_local * GROUP * HD)
    grad_attended = lax.dot_general(grad_full, w_out, contract_cols, **f32).astype(jnp.bfloat16)
    grad_heads = grad_attended.reshape(length, kv_local, GROUP, HD)
    grad_softmax = jnp.einsum("tkgd,ukd->kgtu", grad_heads, value_rows, **f32)
    row_total = jnp.sum(softmax_rows * grad_softmax, axis=-1, keepdims=True)
    grad_scores = (softmax_rows * (grad_softmax - row_total) * score_scale).astype(jnp.bfloat16)
    grad_value = jnp.einsum("kgtu,tkgd->ukd", softmax_low, grad_heads, **f32)
    grad_query = rotate(
        jnp.einsum("kgtu,ukd->tkgd", grad_scores, key_rot, **f32), cosine_table, sine_table, -1.0
    )
    grad_key = rotate(
        jnp.einsum("kgtu,tkgd->ukd", grad_scores, query_rot, **f32), cosine_table, sine_table, -1.0
    )
    grad_projected = jnp.concatenate(
        [grad_query, grad_key[:, :, None], grad_value[:, :, None]], axis=2
    )
    grad_projected = grad_projected.reshape(length, kv_local * (GROUP + 2) * HD)
    grad_projected = grad_projected.astype(jnp.bfloat16)
    partial = lax.dot_general(grad_projected, w_qkv, contract_cols, **f32).astype(jnp.bfloat16)
    return attended, grad_projected, partial


def local_permutes(layer_in, carry_in, top_grad, w_qkv, w_out, gain):
    ticks = layer_in.shape[0]
    own = layer_in.shape[4]
    n_tensor = lax.axis_size("tensor")
    n_dp = lax.axis_size("dp")
    me_tensor = lax.axis_index("tensor")
    me_dp = lax.axis_index("dp")
    section_index = lax.axis_index("section")
    at_first = section_index == 0
    at_last = section_index == lax.axis_size("section") - 1
    owners = (me_tensor + jnp.arange(n_tensor)) % n_tensor
    positions = (owners[:, None] * own + jnp.arange(own)[None, :]).reshape(-1)
    tables = rope_tables(positions, HD)
    mask = positions[:, None] >= positions[None, :]
    layer_rows = layer_in[:, :, 0, 0]
    carried = carry_in[:, 0, 0]
    fresh_grads = top_grad[:, 0]
    weight_qkv = w_qkv[:, 0]
    weight_out = w_out[:, 0]
    gain_rows = gain[:, 0]

    def gather(value):
        return jnp.concatenate(
            [value] + [from_ahead(value, "tensor", k) for k in range(1, n_tensor)], axis=0
        )

    def scatter_sum(partial):
        total = partial[:own].astype(jnp.float32)
        for k in range(1, n_tensor):
            chunk = partial[k * own : (k + 1) * own]
            total = total + from_ahead(chunk, "tensor", -k).astype(jnp.float32)
        return total

    def columns_of(value, index):
        width = value.shape[1] // n_dp
        return lax.dynamic_slice_in_dim(value, index * width, width, axis=1)

    def exchange(value, cut):
        if cut:
            return [columns_of(value, me_dp)] + [
                from_ahead(columns_of(value, (me_dp - k) % n_dp), "dp", k) for k in range(1, n_dp)
            ]
        return [value] + [from_ahead(value, "dp", k) for k in range(1, n_dp)]

    members = (1, 0)
    unit_rows, inverse, normed = {}, {}, {}
    for t in range(ticks):
        for m in members:
            rows = layer_rows[t, m].astype(jnp.float32)
            inverse[t, m] = lax.rsqrt(jnp.mean(rows * rows, axis=-1, keepdims=True) + epsilon)
            unit_rows[t, m] = rows * inverse[t, m]
            normed[t, m] = (unit_rows[t, m] * gain_rows[m]).astype(jnp.bfloat16)
    inputs = [carried[0], carried[1]]
    factors = {}
    per_tick = []
    gain_totals = [0.0, 0.0]
    for t in range(ticks):
        outcome = [None, None]
        for m in members:
            dy = inputs[m]
            full_normed = gather(normed[t, m])
            full_grad = gather(dy)
            attended, grad_projected, partial = unit_compute(
                full_normed, full_grad, weight_qkv[m], weight_out[m], tables, mask
            )
            factors[t, m] = (
                exchange(full_normed, True),
                exchange(grad_projected, False),
                exchange(attended, True),
                exchange(full_grad, False),
            )
            grad_normed = scatter_sum(partial)
            grad_unit = grad_normed * gain_rows[m]
            unit = unit_rows[t, m]
            grad_rows = inverse[t, m] * (
                grad_unit - unit * jnp.mean(grad_unit * unit, axis=-1, keepdims=True)
            )
            outcome[m] = (dy.astype(jnp.float32) + grad_rows).astype(jnp.bfloat16)
            gain_totals[m] = gain_totals[m] + jnp.sum(grad_normed * unit, axis=0)
        if t + 1 < ticks:
            upward = from_behind(outcome[1], "section", 1)
            downward = from_behind(outcome[0], "section", -1)
            inputs = [
                jnp.where(at_last, outcome[1], downward),
                jnp.where(at_first, fresh_grads[t], upward),
            ]
        per_tick.append(jnp.stack(outcome))

    def weight_grad(m, left, right):
        total = None
        for k in range(n_dp):
            a = jnp.concatenate([factors[t, m][left][k] for t in range(ticks)], axis=0)
            b = jnp.concatenate([factors[t, m][right][k] for t in range(ticks)], axis=0)
            part = lax.dot_general(a, b, contract_rows, preferred_element_type=jnp.float32)
            part = part.astype(jnp.bfloat16).astype(jnp.float32)
            total = part if total is None else total + part
        return total.astype(jnp.bfloat16)

    grad_qkv = jnp.stack([weight_grad(m, 0, 1) for m in (0, 1)])
    grad_out = jnp.stack([weight_grad(m, 2, 3) for m in (0, 1)])
    gain_total = lax.psum(jnp.stack(gain_totals), ("tensor", "dp"))
    return (
        jnp.stack(per_tick)[:, :, None, None],
        grad_qkv[:, None],
        grad_out[:, None],
        gain_total[:, None],
    )


def fused(
    n, reps, ticks, sections, own,
    x_hbm, carry, top, gain_hbm, wq_hbm, wo_hbm, cos_hbm, sin_hbm,
    out, gq_out, go_out, gain_out,
    wq, wo, xb, gain, cos_ref, sin_ref,
    nrm, dyb, gpb, attb, pnrm, pdy, pgp, patt, pb, rb, smb, qsb, kb, vb, gtot, grecv, gsum,
    w_sem, x_sem, c_sem, t_sem, g_send, g_recv, r_send, r_recv, s_send, s_recv, d_send, d_recv,
    gain_send, gain_recv,
):
    f32 = jnp.float32
    bf16 = jnp.bfloat16
    me = lax.axis_index("tensor")
    rep = lax.axis_index("dp")
    sec = lax.axis_index("section")
    length = n * own
    units = 2 * ticks
    hq = wo.shape[1]
    width = wq.shape[1]
    cols = wq.shape[2]
    groups = hq // (GROUP * HD)
    wn = width // reps
    wa = hq // reps
    scale = 1.0 / math.sqrt(HD)
    parts = PARTS if width % (PARTS * 128) == 0 else 1
    piece = width // parts

    def tensor_at(k):
        return {"tensor": lax.rem(me + k + n, n)}

    def dp_at(k):
        return {"dp": lax.rem(rep + k + reps, reps)}

    barrier = pltpu.get_barrier_semaphore()
    for a in range(n):
        for b in range(reps):
            if a or b:
                pl.semaphore_signal(
                    barrier, inc=1, device_id={**tensor_at(a), **dp_at(b)}, device_id_type=MESH
                )

    @pl.when(sec > 0)
    def _():
        pl.semaphore_signal(barrier, inc=1, device_id={"section": sec - 1}, device_id_type=MESH)

    @pl.when(sec < sections - 1)
    def _():
        pl.semaphore_signal(barrier, inc=1, device_id={"section": sec + 1}, device_id_type=MESH)

    def at_rows(t, i):
        return pl.ds(pl.multiple_of(t * length + i * own, own), own)

    def whole(t):
        return pl.ds(t * length, length)

    def lanes(h):
        return pl.ds(h * piece, piece)

    def unit_of(t, m):
        return 2 * t + m

    order = [(t, m) for t in range(ticks) for m in (1, 0)]

    x_copies = {}
    for t, m in order:
        u = unit_of(t, m)
        x_copies[t, m] = pltpu.make_async_copy(x_hbm.at[u], xb.at[u], x_sem.at[u])
    small = [
        pltpu.make_async_copy(src, dst, t_sem.at[k])
        for k, (src, dst) in enumerate(((gain_hbm, gain), (cos_hbm, cos_ref), (sin_hbm, sin_ref)))
    ]
    carry_copies = [
        pltpu.make_async_copy(carry.at[m], dyb.at[m, at_rows(0, me)], c_sem.at[m]) for m in (1, 0)
    ]
    top_copies = [
        pltpu.make_async_copy(top.at[t], dyb.at[1, at_rows(t + 1, me)], c_sem.at[2 + t])
        for t in range(ticks - 1)
    ]
    w_copies = [
        pltpu.make_async_copy(src.at[m], dst.at[m], w_sem.at[j, m])
        for m in (1, 0)
        for j, (src, dst) in enumerate(((wq_hbm, wq), (wo_hbm, wo)))
    ]
    carry_copies[0].start()
    small[0].start()
    x_copies[0, 1].start()
    carry_copies[1].start()
    for t, m in order[1:]:
        x_copies[t, m].start()
    for c in small[1:]:
        c.start()

    @pl.when(sec == 0)
    def _():
        for c in top_copies:
            c.start()

    def normalize(t, m):
        u = unit_of(t, m)
        x_copies[t, m].wait()
        x = xb[u].astype(f32)
        inverse = lax.rsqrt(jnp.mean(x * x, axis=-1, keepdims=True) + epsilon)
        nrm[m, at_rows(t, me)] = (x * inverse * gain[m]).astype(bf16)

    gtot[...] = jnp.zeros_like(gtot)
    neighbours = jnp.where(sec > 0, 1, 0) + jnp.where(sec < sections - 1, 1, 0)
    with jax.named_scope("barrier"):
        pl.semaphore_wait(barrier, n * reps - 1 + neighbours)

    def remote(src, dst, send, recv, where):
        return pltpu.make_async_remote_copy(
            src_ref=src, dst_ref=dst, send_sem=send, recv_sem=recv, device_id=where,
            device_id_type=MESH,
        )

    def hop(which, t, m, i, h, up):
        u = unit_of(t, m)
        at = (nrm, dyb)[which].at[m, at_rows(t, i), lanes(h)]
        return remote(
            at, at, g_send.at[which, u, up], g_recv.at[which, u, h, i],
            tensor_at(1 if up else -1),
        )

    def dy_peer(t, m, i, h, j):
        at = at_rows(t, i)
        return remote(
            dyb.at[m, at, lanes(h)], pdy.at[j - 1, m, at, lanes(h)],
            d_send.at[1, j - 1], d_recv.at[1, m, j - 1], dp_at(-j),
        )

    def nrm_peer(t, m, i, j):
        peer = lax.rem(rep - j + reps, reps)
        at = at_rows(t, i)
        return remote(
            nrm.at[m, at, pl.ds(pl.multiple_of(peer * wn, 128), wn)], pnrm.at[j - 1, m, at],
            d_send.at[0, j - 1], d_recv.at[0, m, j - 1], dp_at(-j),
        )

    def rest_peer(which, t, m, j):
        peer = lax.rem(rep - j + reps, reps)
        at = whole(t)
        src, dst = {
            2: (gpb.at[m, at], pgp),
            3: (attb.at[m, at, pl.ds(pl.multiple_of(peer * wa, 128), wa)], patt),
        }[which]
        return remote(
            src, dst.at[j - 1, m, at], d_send.at[which, j - 1], d_recv.at[which, m, j - 1],
            dp_at(-j),
        )

    def peer_layer(which, m, j):
        at = (pnrm, pdy, pgp, patt)[which].at[j - 1, m]
        return remote(at, at, d_send.at[which, j - 1], d_recv.at[which, m, j - 1], dp_at(-j))

    def peer_all(which, j):
        at = (pnrm, pdy, pgp, patt)[which].at[j - 1]
        return remote(at, at, d_send.at[which, j - 1], d_recv.at[which, 0, j - 1], dp_at(-j))

    others = range(1, reps)
    far = range(1, n)

    def to_peers(which, t, m, i, h):
        for j in others:
            if which:
                dy_peer(t, m, i, h, j).start()
            elif h == parts - 1:
                nrm_peer(t, m, i, j).start()

    def own_to_peers(which, t, m):
        for h in range(parts):
            to_peers(which, t, m, me, h)

    def own_hops(which, t, m, edge=None):
        for h in range(parts):
            for up in (1, 0):
                sends = me < n - 1 if up else me > 0
                if edge is not None:
                    sends = (me == 0 if up else me == n - 1) if edge else (me > 0) & (me < n - 1)

                @pl.when(sends)
                def _():
                    hop(which, t, m, me, h, up).start()

    def arrivals(which, t, m, d, forward, source):
        for h in range(parts):
            for up in (1, 0):
                i = me - d if up else me + d
                inside = me >= d if up else me + d < n
                if source == "edge":
                    inside = me == d if up else me + d == n - 1
                elif source == "middle":
                    inside = me > d if up else me + d < n - 1
                middle = me < n - 1 if up else me > 0
                edge = me == n - 1 if up else me == 0

                @pl.when(inside & (middle if forward else edge))
                def _():
                    with jax.named_scope("wait_fwd" if forward else "wait_end"):
                        hop(which, t, m, i, h, up).wait_recv()
                    if forward:
                        hop(which, t, m, i, h, up).start()
                    to_peers(which, t, m, i, h)

    def fwd(what, t, m, *ds, source=None):
        for d in ds:
            if 0 < d < n - 1:
                for which in what:
                    arrivals(which, t, m, d, True, source)

    def end(what, t, m, *ds):
        for d in ds:
            if 0 < d < n:
                for which in what:
                    arrivals(which, t, m, d, False, None)

    def sum_copy(t, m, d, h, way):
        u = unit_of(t, m)
        i = me + d if way else me - d
        return remote(
            pb.at[u, pl.ds(pl.multiple_of(i * own, own), own), lanes(h)],
            rb.at[u, way, d - 1, :, lanes(h)],
            r_send.at[u, way], r_recv.at[u, way, d - 1, h], tensor_at(1 if way else -1),
        )

    def sum_arrived(t, m, d, h, way):
        u = unit_of(t, m)
        at = rb.at[u, way, d, :, lanes(h)]
        remote(at, at, r_send.at[u, way], r_recv.at[u, way, d, h], tensor_at(1)).wait_recv()

    def sum_stage(t, m, stage):
        u = unit_of(t, m)
        for way in (1, 0):

            @pl.when(me == (stage if way else n - 1 - stage))
            def _():
                place = stage if way else n - 1 - stage
                for d in range(n - 1 - stage, 0, -1):
                    i = place + d if way else place - d
                    at = pl.ds(i * own, own)
                    for h in range(parts):
                        if stage:
                            with jax.named_scope("wait_sum"):
                                sum_arrived(t, m, d, h, way)
                            total = pb[u, at, lanes(h)].astype(f32)
                            total = total + rb[u, way, d, :, lanes(h)].astype(f32)
                            pb[u, at, lanes(h)] = total.astype(bf16)
                        sum_copy(t, m, d, h, way).start()

    def sums(t, m, *stages):
        for stage in stages:
            if 0 < stage < n - 1:
                sum_stage(t, m, stage)

    def hops_sent(which, t, m):
        u = unit_of(t, m)
        for up in (1, 0):
            for place in range(n):
                count = place + 1 if up else n - place
                if count < n or (place < n - 1 if up else place > 0):

                    @pl.when(me == place)
                    def _():
                        at = (nrm, dyb)[which].at[m, pl.ds(0, count * own)]
                        sem = g_send.at[which, u, up]
                        remote(at, at, sem, sem, tensor_at(1)).wait_send()

    def sums_sent(t, m):
        u = unit_of(t, m)
        for way in (1, 0):
            for stage in range(n - 1):

                @pl.when(me == (stage if way else n - 1 - stage))
                def _():
                    at = pb.at[u, pl.ds(0, (n - 1 - stage) * own)]
                    remote(at, at, r_send.at[u, way], r_send.at[u, way], tensor_at(1)).wait_send()

    def section_copy(t, m):
        step = 1 if m == 1 else -1
        return remote(
            out.at[unit_of(t, m)], dyb.at[m, at_rows(t + 1, me)], s_send.at[t, m],
            s_recv.at[t, m], {"section": sec + step},
        )

    def gain_copy(a, b):
        slot = a * reps + b
        return remote(
            gtot, grecv.at[slot], gain_send, gain_recv, {**tensor_at(-a), **dp_at(-b)}
        )

    def gain_all():
        at = grecv.at[pl.ds(1, n * reps - 1)]
        return remote(at, at, gain_send, gain_recv, tensor_at(1))

    def swap(values):
        wide = values.shape[1]
        lane = lax.broadcasted_iota(jnp.int32, values.shape, 1)
        low = lax.rem(lane, HD) < HD // 2
        return jnp.where(
            low, pltpu.roll(values, wide - HD // 2, 1), pltpu.roll(values, HD // 2, 1)
        )

    def dot(a, b, ca, cb):
        return lax.dot_general(a, b, (((ca,), (cb,)), ((), ())), preferred_element_type=f32)

    def stack_heads(values):
        return jnp.concatenate([values[:, h * HD : (h + 1) * HD] for h in range(GROUP)], axis=0)

    def spread_heads(values):
        return jnp.concatenate(
            [values[h * length : (h + 1) * length] for h in range(GROUP)], axis=1
        )

    def table(ref, wide):
        return jnp.concatenate([ref[...]] * (wide // 128), axis=1)

    span = (GROUP + 2) * HD

    def forward(t, m):
        u = unit_of(t, m)
        projected = dot(nrm[m, whole(t)], wq[m], 1, 0)
        rotated = projected * table(cos_ref, cols) + swap(projected) * table(sin_ref, cols)
        rotated = rotated.astype(bf16)
        row = lax.broadcasted_iota(jnp.int32, (length, length), 0)
        key_row = lax.broadcasted_iota(jnp.int32, (length, length), 1)
        bias = jnp.where(row >= key_row, 0.0, -1e30)
        for g in range(groups):
            at = g * span
            qs = stack_heads(rotated[:, at : at + GROUP * HD])
            key = rotated[:, at + GROUP * HD : at + (GROUP + 1) * HD]
            value = projected[:, at + (GROUP + 1) * HD : at + span].astype(bf16)
            scores = dot(qs, key, 1, 1) * scale
            scores = (scores.reshape(GROUP, length, length) + bias[None]).reshape(
                GROUP * length, length
            )
            e = jnp.exp(scores - jnp.max(scores, axis=-1, keepdims=True))
            sm = e / jnp.sum(e, axis=-1, keepdims=True)
            smb[u, g] = sm
            qsb[u, g] = qs
            kb[u, g] = key
            vb[u, g] = value
            attended = spread_heads(dot(sm.astype(bf16), value, 1, 0).astype(bf16))
            attb[m, whole(t), g * GROUP * HD : (g + 1) * GROUP * HD] = attended
        for j in others:
            rest_peer(3, t, m, j).start()

    def backward(t, m):
        u = unit_of(t, m)
        grad_att = dot(dyb[m, whole(t)], wo[m], 1, 1).astype(bf16)
        for g in range(groups):
            sm = smb[u, g]
            low = sm.astype(bf16)
            value = vb[u, g]
            gs = stack_heads(grad_att[:, g * GROUP * HD : (g + 1) * GROUP * HD])
            gsm = dot(gs, value, 1, 1)
            total = jnp.sum(sm * gsm, axis=-1, keepdims=True)
            gsc = (sm * (gsm - total) * scale).astype(bf16)
            g_value = dot(low, gs, 0, 0)
            g_query = spread_heads(dot(gsc, kb[u, g], 1, 0))
            g_key = dot(gsc, qsb[u, g], 0, 0)
            turned = jnp.concatenate([g_query, g_key, g_value], axis=1)
            back = turned * table(cos_ref, span) - swap(turned) * table(sin_ref, span)
            lane = lax.broadcasted_iota(jnp.int32, turned.shape, 1)
            back = jnp.where(lane < (GROUP + 1) * HD, back, turned)
            gpb[m, whole(t), g * span : (g + 1) * span] = back.astype(bf16)
        pb[u] = dot(gpb[m, whole(t)], wq[m], 1, 1).astype(bf16)
        sum_stage(t, m, 0)
        for j in others:
            rest_peer(2, t, m, j).start()

    def finish(t, m):
        u = unit_of(t, m)
        x = xb[u].astype(f32)
        inverse = lax.rsqrt(jnp.mean(x * x, axis=-1, keepdims=True) + epsilon)
        unit = x * inverse
        mine = pl.ds(pl.multiple_of(me * own, own), own)
        gsum[...] = pb[u, mine].astype(f32)
        for way in (1, 0):

            @pl.when(me > 0 if way else me < n - 1)
            def _():
                with jax.named_scope("wait_scatter"):
                    for h in range(parts):
                        sum_arrived(t, m, 0, h, way)
                gsum[...] = gsum[...] + rb[u, way, 0].astype(f32)

        gn = gsum[...]
        gu = gn * gain[m]
        grad = inverse * (gu - unit * jnp.mean(gu * unit, axis=-1, keepdims=True))
        out[u] = (dyb[m, at_rows(t, me)].astype(f32) + grad).astype(bf16)
        if (t, m) != (ticks - 1, 0):
            gtot[m] = gtot[m] + jnp.sum(gn * unit, axis=0, keepdims=True)

    def gain_of_parts(t, m):
        part = pb[unit_of(t, m)].astype(f32) * nrm[m, whole(t)].astype(f32)
        gtot[m] = gtot[m] + jnp.sum(part, axis=0, keepdims=True) / gain[m]

    def hand_over(t, m):
        if t + 1 == ticks:
            return

        @pl.when(sec < sections - 1 if m == 1 else sec > 0)
        def _():
            section_copy(t, m).start()

        if m == 1:

            @pl.when(sec == sections - 1)
            def _():
                dyb[0, at_rows(t + 1, me)] = out[unit_of(t, 1)]

    def taken_over(t, m):
        with jax.named_scope("wait_section"):

            @pl.when(sec > 0 if m == 1 else sec < sections - 1)
            def _():
                section_copy(t - 1, m).wait_recv()

            if m == 1:

                @pl.when(sec == 0)
                def _():
                    top_copies[t - 1].wait()

    def wait_peers(m, *kinds):
        with jax.named_scope("wait_dp"):
            for which in kinds:
                for j in others:
                    peer_layer(which, m, j).wait_recv()

    def rounded(a, b):
        return dot(a, b, 0, 0).astype(bf16).astype(f32)

    def grad_out(m):
        wide = 512 if width % 512 == 0 else 128
        att_at = pl.ds(pl.multiple_of(rep * wa, 128), wa)

        @pl.loop(0, width // wide)
        def _(c):
            at = pl.ds(pl.multiple_of(c * wide, 128), wide)
            total = rounded(attb[m, :, att_at], dyb[m, :, at])
            for j in others:
                total = total + rounded(patt[j - 1, m], pdy[j - 1, m, :, at])
            go_out[m, :, at] = total.astype(bf16)

    def grad_qkv(m):
        block = 256 if wn % 256 == 0 else 128

        @pl.loop(0, wn // block)
        def _(c):
            own_at = pl.ds(pl.multiple_of(rep * wn + c * block, 128), block)
            at = pl.ds(pl.multiple_of(c * block, 128), block)
            total = rounded(nrm[m, :, own_at], gpb[m])
            for j in others:
                total = total + rounded(pnrm[j - 1, m, :, at], pgp[j - 1, m])
            gq_out[m, at] = total.astype(bf16)

    def grads_of(m):
        wait_peers(m, 1, 3)
        with jax.named_scope("grad_out"):
            grad_out(m)
        wait_peers(m, 0, 2)
        with jax.named_scope("grad_qkv"):
            grad_qkv(m)

    inner = range(1, n - 1)
    dy, x = 1, 0
    both = (dy, x)

    carry_copies[0].wait()
    own_hops(dy, 0, 1)
    own_to_peers(dy, 0, 1)
    small[0].wait()
    normalize(0, 1)
    own_hops(x, 0, 1)
    own_to_peers(x, 0, 1)
    carry_copies[1].wait()
    own_to_peers(dy, 0, 0)
    for t, m in order[1:]:
        normalize(t, m)
        own_to_peers(x, t, m)
    for c in w_copies:
        c.start()
    fwd(both, 0, 1, *inner)
    end(both, 0, 1, *inner)
    for which in both:
        own_hops(which, 0, 0)
    with jax.named_scope("wait_weights"):
        for c in w_copies:
            c.wait()
        for c in small[1:]:
            c.wait()
    end(both, 0, 1, n - 1)
    with jax.named_scope("forward"):
        forward(0, 1)
    with jax.named_scope("backward"):
        backward(0, 1)
    own_hops(x, 1, 1, edge=True)
    fwd(both, 0, 0, 1)
    end(both, 0, 0, 1)
    fwd(both, 0, 0, *inner[1:])
    end(both, 0, 0, *inner[1:])

    def give(which, t, m):
        fwd((which,), t, m, 1, source="middle")
        fwd((which,), t, m, 1, source="edge")

    for t in range(1, ticks):
        late = both if t == 1 else (dy,)
        if t > 1:
            own_hops(x, t, 1, edge=True)
        sums(t - 1, 1, 1)
        end(late, t - 1, 0, n - 1)
        if t == 1:
            with jax.named_scope("forward"):
                forward(t - 1, 0)
        sums(t - 1, 1, *inner[1:])
        own_hops(x, t, 1, edge=False)
        with jax.named_scope("backward"):
            backward(t - 1, 0)
        give(x, t, 1)
        finish(t - 1, 1)
        hand_over(t - 1, 1)
        fwd((x,), t, 1, *inner[1:])
        end((x,), t, 1, 1)
        taken_over(t, 1)
        own_to_peers(dy, t, 1)
        own_hops(dy, t, 1)
        end((x,), t, 1, *far[1:-1])
        fwd((dy,), t, 1, 1, source="middle")
        end((x,), t, 1, n - 1)
        with jax.named_scope("forward"):
            forward(t, 1)
        own_hops(x, t, 0, edge=True)
        sums(t - 1, 0, 1)
        fwd((dy,), t, 1, 1, source="edge")
        sums(t - 1, 0, *inner[1:])
        fwd((dy,), t, 1, *inner[1:])
        own_hops(x, t, 0, edge=False)
        end((dy,), t, 1, *far)
        with jax.named_scope("backward"):
            backward(t, 1)
        finish(t - 1, 0)
        hand_over(t - 1, 0)
        give(x, t, 0)
        fwd((x,), t, 0, *inner[1:])
        end((x,), t, 0, 1)
        taken_over(t, 0)
        own_to_peers(dy, t, 0)
        own_hops(dy, t, 0)
        end((x,), t, 0, *far[1:-1])
        fwd((dy,), t, 0, 1, source="middle")
        if t + 1 == ticks:
            sums(t, 1, 1)
        end((x,), t, 0, n - 1)
        with jax.named_scope("forward"):
            forward(t, 0)
        fwd((dy,), t, 0, 1, source="edge")
        fwd((dy,), t, 0, *inner[1:])
        if t + 1 == ticks:
            sums(t, 1, *inner[1:])
        end((dy,), t, 0, *(far if t + 1 == ticks else far[:-1]))

    last = ticks - 1
    with jax.named_scope("backward"):
        backward(last, 0)
    finish(last, 1)
    gain_of_parts(last, 0)
    for a in range(n):
        for b in range(reps):
            if a or b:
                gain_copy(a, b).start()
    grads_of(1)
    sums(last, 0, *inner)
    edge = (me == 0) | (me == n - 1)

    @pl.when(edge)
    def _():
        grads_of(0)

    finish(last, 0)

    @pl.when(jnp.logical_not(edge))
    def _():
        grads_of(0)

    total = gtot[...]
    gain_all().wait_recv()
    for slot in range(1, n * reps):
        total = total + grecv[slot]
    gain_out[...] = total
    with jax.named_scope("wait_sends"):
        for t, m in order:
            sums_sent(t, m)
            for which in both:
                hops_sent(which, t, m)
        for j in others:
            for which in range(4):
                peer_all(which, j).wait_send()
        for t in range(ticks - 1):

            @pl.when(sec < sections - 1)
            def _():
                section_copy(t, 1).wait_send()

            @pl.when(sec > 0)
            def _():
                section_copy(t, 0).wait_send()

        gain_all().wait_send()


def write_back(a, b, c, d, a_out, b_out, c_out, d_out, sem):
    pairs = ((a, a_out), (b, b_out), (c, c_out), (d, d_out))
    copies = [pltpu.make_async_copy(src, dst, sem.at[k]) for k, (src, dst) in enumerate(pairs)]
    for c in copies:
        c.start()
    for c in copies:
        c.wait()


def lane_tables(length):
    cosine, sine = rope_tables(jnp.arange(length), HD)
    copies = 128 // HD
    cosine = jnp.tile(jnp.concatenate([cosine, cosine], axis=1), (1, copies))
    sine = jnp.tile(jnp.concatenate([-sine, sine], axis=1), (1, copies))
    return cosine, sine


def local(layer_in, carry_in, top_grad, w_qkv, w_out, gain):
    ticks, own, width = layer_in.shape[0], layer_in.shape[4], layer_in.shape[5]
    n = lax.axis_size("tensor")
    reps = lax.axis_size("dp")
    sections = lax.axis_size("section")
    cols, hq = w_qkv.shape[3], w_out.shape[2]
    lined = (width // reps) % 128 == 0 and (hq // reps) % 128 == 0 and cols % 128 == 0
    if not lined or own % 16 or ticks < 2 or n < 3:
        return local_permutes(layer_in, carry_in, top_grad, w_qkv, w_out, gain)
    length = n * own
    units = 2 * ticks
    deep = ticks * length
    groups = hq // (GROUP * HD)
    wn, wa = width // reps, hq // reps
    f32, bf16 = jnp.float32, jnp.bfloat16
    parts = PARTS if width % (PARTS * 128) == 0 else 1
    with jax.ensure_compile_time_eval():
        cosine, sine = lane_tables(length)
    vmem = pl.BlockSpec(memory_space=pltpu.VMEM)
    hbm = pl.BlockSpec(memory_space=pl.ANY)
    dma = pltpu.SemaphoreType.DMA
    outs = pl.pallas_call(
        functools.partial(fused, n, reps, ticks, sections, own),
        out_shape=(
            pltpu.VMEM((units, own, width), bf16),
            pltpu.VMEM((2, wn, cols), bf16),
            pltpu.VMEM((2, wa, width), bf16),
            pltpu.VMEM((2, 1, width), f32),
        ),
        in_specs=[hbm] * 8,
        out_specs=(vmem,) * 4,
        scratch_shapes=[
            pltpu.VMEM((2, width, cols), bf16),
            pltpu.VMEM((2, hq, width), bf16),
            pltpu.VMEM((units, own, width), bf16),
            pltpu.VMEM((2, 1, width), f32),
            pltpu.VMEM((length, 128), f32),
            pltpu.VMEM((length, 128), f32),
            pltpu.VMEM((2, deep, width), bf16),
            pltpu.VMEM((2, deep, width), bf16),
            pltpu.VMEM((2, deep, cols), bf16),
            pltpu.VMEM((2, deep, hq), bf16),
            pltpu.VMEM((reps - 1, 2, deep, wn), bf16),
            pltpu.VMEM((reps - 1, 2, deep, width), bf16),
            pltpu.VMEM((reps - 1, 2, deep, cols), bf16),
            pltpu.VMEM((reps - 1, 2, deep, wa), bf16),
            pltpu.VMEM((units, length, width), bf16),
            pltpu.VMEM((units, 2, n - 1, own, width), bf16),
            pltpu.VMEM((units, groups, GROUP * length, length), f32),
            pltpu.VMEM((units, groups, GROUP * length, HD), bf16),
            pltpu.VMEM((units, groups, length, HD), bf16),
            pltpu.VMEM((units, groups, length, HD), bf16),
            pltpu.VMEM((2, 1, width), f32),
            pltpu.VMEM((n * reps, 2, 1, width), f32),
            pltpu.VMEM((own, width), f32),
            dma((2, 2)),
            dma((units,)),
            dma((1 + ticks,)),
            dma((3,)),
            dma((2, units, 2)),
            dma((2, units, parts, n)),
            dma((units, 2)),
            dma((units, 2, n - 1, parts)),
            dma((ticks - 1, 2)),
            dma((ticks - 1, 2)),
            dma((4, reps - 1)),
            dma((4, 2, reps - 1)),
            dma(()),
            dma(()),
        ],
        compiler_params=pltpu.CompilerParams(
            collective_id=0, has_side_effects=True, vmem_limit_bytes=50 * 1024 * 1024
        ),
    )(
        layer_in[:, :, 0, 0].reshape(units, own, width),
        carry_in[:, 0, 0],
        top_grad[:, 0],
        gain,
        w_qkv[:, 0],
        w_out[:, 0],
        cosine,
        sine,
    )
    outs = pl.pallas_call(
        write_back,
        out_shape=(
            jax.ShapeDtypeStruct((units, own, width), bf16),
            jax.ShapeDtypeStruct((2, wn, cols), bf16),
            jax.ShapeDtypeStruct((2, wa, width), bf16),
            jax.ShapeDtypeStruct((2, 1, width), f32),
        ),
        in_specs=[vmem] * 4,
        out_specs=(hbm,) * 4,
        scratch_shapes=[dma((4,))],
        compiler_params=pltpu.CompilerParams(vmem_limit_bytes=1024 * 1024),
    )(*[pltpu.with_memory_space_constraint(o, pltpu.VMEM) for o in outs])
    return (
        outs[0].reshape(ticks, 2, 1, 1, own, width),
        outs[1][:, None],
        outs[2][:, None],
        outs[3],
    )


def solution(mesh):
    in_specs = (
        P(None, None, "section", "dp", "tensor", None),
        P(None, "section", "dp", "tensor", None),
        P(None, "dp", "tensor", None),
        P(None, "section", None, "tensor"),
        P(None, "section", "tensor", None),
        P(None, "section", None),
    )
    out_specs = (
        P(None, None, "section", "dp", "tensor", None),
        P(None, "section", "dp", "tensor"),
        P(None, "section", ("tensor", "dp"), None),
        P(None, "section", None),
    )
    return jax.shard_map(local, mesh=mesh, in_specs=in_specs, out_specs=out_specs, check_vma=False)
```

```python
import functools
import math

import jax
import jax.numpy as jnp
from jax import lax
from jax.experimental import pallas as pl
from jax.experimental.pallas import tpu as pltpu
from jax.sharding import PartitionSpec as P

HD = 64
GROUP = 8

epsilon = 1e-06
rope_base = 1000000.0


MESH = pl.DeviceIdType.MESH
PARTS = 2

contract_rows = (((0,), (0,)), ((), ()))
contract_cols = (((1,), (1,)), ((), ()))


def from_behind(value, axis, steps):
    count = lax.axis_size(axis)
    first, last = (max(0, -steps), min(count, count - steps))
    return lax.ppermute(value, axis, [(source, source + steps) for source in range(first, last)])


def from_ahead(value, axis, steps):
    count = lax.axis_size(axis)
    return lax.ppermute(value, axis, [((i + steps) % count, i) for i in range(count)])


def rope_tables(positions, head_width):
    half_width = head_width // 2
    exponent = jnp.arange(half_width, dtype=jnp.float32) * (2.0 / head_width)
    frequency = rope_base ** (-exponent)
    angle = positions.astype(jnp.float32)[:, None] * frequency[None, :]
    return (jnp.cos(angle), jnp.sin(angle))


def rotate(values, cosine_table, sine_table, direction):
    half_width = values.shape[-1] // 2
    table_shape = (values.shape[0],) + (1,) * (values.ndim - 2) + (half_width,)
    cosine = cosine_table.reshape(table_shape)
    sine_part = direction * sine_table.reshape(table_shape)
    lower_half = values[..., :half_width]
    upper_half = values[..., half_width:]
    return jnp.concatenate(
        [
            lower_half * cosine - upper_half * sine_part,
            upper_half * cosine + lower_half * sine_part,
        ],
        axis=-1,
    )


def unit_compute(normed, grad_full, w_qkv, w_out, tables, mask):
    length = normed.shape[0]
    kv_local = w_out.shape[0] // (GROUP * HD)
    cosine_table, sine_table = tables
    score_scale = 1.0 / math.sqrt(HD)
    projected = jnp.dot(normed, w_qkv, preferred_element_type=jnp.float32)
    projected = projected.reshape(length, kv_local, GROUP + 2, HD)
    query_rot = rotate(projected[:, :, :GROUP], cosine_table, sine_table, 1.0).astype(jnp.bfloat16)
    key_rot = rotate(projected[:, :, GROUP], cosine_table, sine_table, 1.0).astype(jnp.bfloat16)
    value_rows = projected[:, :, GROUP + 1].astype(jnp.bfloat16)
    f32 = dict(preferred_element_type=jnp.float32)
    scores = jnp.einsum("tkgd,ukd->kgtu", query_rot, key_rot, **f32) * score_scale
    scores = jnp.where(mask, scores, -1e30)
    exponentials = jnp.exp(scores - jnp.max(scores, axis=-1, keepdims=True))
    softmax_rows = exponentials / jnp.sum(exponentials, axis=-1, keepdims=True)
    softmax_low = softmax_rows.astype(jnp.bfloat16)
    attended = jnp.einsum("kgtu,ukd->tkgd", softmax_low, value_rows, **f32)
    attended = attended.astype(jnp.bfloat16).reshape(length, kv_local * GROUP * HD)
    grad_attended = lax.dot_general(grad_full, w_out, contract_cols, **f32).astype(jnp.bfloat16)
    grad_heads = grad_attended.reshape(length, kv_local, GROUP, HD)
    grad_softmax = jnp.einsum("tkgd,ukd->kgtu", grad_heads, value_rows, **f32)
    row_total = jnp.sum(softmax_rows * grad_softmax, axis=-1, keepdims=True)
    grad_scores = (softmax_rows * (grad_softmax - row_total) * score_scale).astype(jnp.bfloat16)
    grad_value = jnp.einsum("kgtu,tkgd->ukd", softmax_low, grad_heads, **f32)
    grad_query = rotate(
        jnp.einsum("kgtu,ukd->tkgd", grad_scores, key_rot, **f32), cosine_table, sine_table, -1.0
    )
    grad_key = rotate(
        jnp.einsum("kgtu,tkgd->ukd", grad_scores, query_rot, **f32), cosine_table, sine_table, -1.0
    )
    grad_projected = jnp.concatenate(
        [grad_query, grad_key[:, :, None], grad_value[:, :, None]], axis=2
    )
    grad_projected = grad_projected.reshape(length, kv_local * (GROUP + 2) * HD)
    grad_projected = grad_projected.astype(jnp.bfloat16)
    partial = lax.dot_general(grad_projected, w_qkv, contract_cols, **f32).astype(jnp.bfloat16)
    return attended, grad_projected, partial


def local_permutes(layer_in, carry_in, top_grad, w_qkv, w_out, gain):
    ticks = layer_in.shape[0]
    own = layer_in.shape[4]
    n_tensor = lax.axis_size("tensor")
    n_dp = lax.axis_size("dp")
    me_tensor = lax.axis_index("tensor")
    me_dp = lax.axis_index("dp")
    section_index = lax.axis_index("section")
    at_first = section_index == 0
    at_last = section_index == lax.axis_size("section") - 1
    owners = (me_tensor + jnp.arange(n_tensor)) % n_tensor
    positions = (owners[:, None] * own + jnp.arange(own)[None, :]).reshape(-1)
    tables = rope_tables(positions, HD)
    mask = positions[:, None] >= positions[None, :]
    layer_rows = layer_in[:, :, 0, 0]
    carried = carry_in[:, 0, 0]
    fresh_grads = top_grad[:, 0]
    weight_qkv = w_qkv[:, 0]
    weight_out = w_out[:, 0]
    gain_rows = gain[:, 0]

    def gather(value):
        return jnp.concatenate(
            [value] + [from_ahead(value, "tensor", k) for k in range(1, n_tensor)], axis=0
        )

    def scatter_sum(partial):
        total = partial[:own].astype(jnp.float32)
        for k in range(1, n_tensor):
            chunk = partial[k * own : (k + 1) * own]
            total = total + from_ahead(chunk, "tensor", -k).astype(jnp.float32)
        return total

    def columns_of(value, index):
        width = value.shape[1] // n_dp
        return lax.dynamic_slice_in_dim(value, index * width, width, axis=1)

    def exchange(value, cut):
        if cut:
            return [columns_of(value, me_dp)] + [
                from_ahead(columns_of(value, (me_dp - k) % n_dp), "dp", k) for k in range(1, n_dp)
            ]
        return [value] + [from_ahead(value, "dp", k) for k in range(1, n_dp)]

    members = (1, 0)
    unit_rows, inverse, normed = {}, {}, {}
    for t in range(ticks):
        for m in members:
            rows = layer_rows[t, m].astype(jnp.float32)
            inverse[t, m] = lax.rsqrt(jnp.mean(rows * rows, axis=-1, keepdims=True) + epsilon)
            unit_rows[t, m] = rows * inverse[t, m]
            normed[t, m] = (unit_rows[t, m] * gain_rows[m]).astype(jnp.bfloat16)
    inputs = [carried[0], carried[1]]
    factors = {}
    per_tick = []
    gain_totals = [0.0, 0.0]
    for t in range(ticks):
        outcome = [None, None]
        for m in members:
            dy = inputs[m]
            full_normed = gather(normed[t, m])
            full_grad = gather(dy)
            attended, grad_projected, partial = unit_compute(
                full_normed, full_grad, weight_qkv[m], weight_out[m], tables, mask
            )
            factors[t, m] = (
                exchange(full_normed, True),
                exchange(grad_projected, False),
                exchange(attended, True),
                exchange(full_grad, False),
            )
            grad_normed = scatter_sum(partial)
            grad_unit = grad_normed * gain_rows[m]
            unit = unit_rows[t, m]
            grad_rows = inverse[t, m] * (
                grad_unit - unit * jnp.mean(grad_unit * unit, axis=-1, keepdims=True)
            )
            outcome[m] = (dy.astype(jnp.float32) + grad_rows).astype(jnp.bfloat16)
            gain_totals[m] = gain_totals[m] + jnp.sum(grad_normed * unit, axis=0)
        if t + 1 < ticks:
            upward = from_behind(outcome[1], "section", 1)
            downward = from_behind(outcome[0], "section", -1)
            inputs = [
                jnp.where(at_last, outcome[1], downward),
                jnp.where(at_first, fresh_grads[t], upward),
            ]
        per_tick.append(jnp.stack(outcome))

    def weight_grad(m, left, right):
        total = None
        for k in range(n_dp):
            a = jnp.concatenate([factors[t, m][left][k] for t in range(ticks)], axis=0)
            b = jnp.concatenate([factors[t, m][right][k] for t in range(ticks)], axis=0)
            part = lax.dot_general(a, b, contract_rows, preferred_element_type=jnp.float32)
            part = part.astype(jnp.bfloat16).astype(jnp.float32)
            total = part if total is None else total + part
        return total.astype(jnp.bfloat16)

    grad_qkv = jnp.stack([weight_grad(m, 0, 1) for m in (0, 1)])
    grad_out = jnp.stack([weight_grad(m, 2, 3) for m in (0, 1)])
    gain_total = lax.psum(jnp.stack(gain_totals), ("tensor", "dp"))
    return (
        jnp.stack(per_tick)[:, :, None, None],
        grad_qkv[:, None],
        grad_out[:, None],
        gain_total[:, None],
    )


def fused(
    n, reps, ticks, sections, own,
    x_hbm, carry, top, gain_hbm, wq_hbm, wo_hbm, cos_hbm, sin_hbm,
    out, gq_out, go_out, gain_out,
    wq, wo, xb, gain, cos_ref, sin_ref,
    nrm, dyb, gpb, attb, pnrm, pdy, pgp, patt, pb, rb, smb, qsb, kb, vb, gtot, grecv, gsum,
    w_sem, x_sem, c_sem, t_sem, g_send, g_recv, r_send, r_recv, s_send, s_recv, d_send, d_recv,
    gain_send, gain_recv,
):
    f32 = jnp.float32
    bf16 = jnp.bfloat16
    me = lax.axis_index("tensor")
    rep = lax.axis_index("dp")
    sec = lax.axis_index("section")
    length = n * own
    units = 2 * ticks
    hq = wo.shape[1]
    width = wq.shape[1]
    cols = wq.shape[2]
    groups = hq // (GROUP * HD)
    wn = width // reps
    wa = hq // reps
    scale = 1.0 / math.sqrt(HD)
    parts = PARTS if width % (PARTS * 128) == 0 else 1
    piece = width // parts

    def tensor_at(k):
        return {"tensor": lax.rem(me + k + n, n)}

    def dp_at(k):
        return {"dp": lax.rem(rep + k + reps, reps)}

    barrier = pltpu.get_barrier_semaphore()
    for a in range(n):
        for b in range(reps):
            if a or b:
                pl.semaphore_signal(
                    barrier, inc=1, device_id={**tensor_at(a), **dp_at(b)}, device_id_type=MESH
                )

    @pl.when(sec > 0)
    def _():
        pl.semaphore_signal(barrier, inc=1, device_id={"section": sec - 1}, device_id_type=MESH)

    @pl.when(sec < sections - 1)
    def _():
        pl.semaphore_signal(barrier, inc=1, device_id={"section": sec + 1}, device_id_type=MESH)

    def at_rows(t, i):
        return pl.ds(pl.multiple_of(t * length + i * own, own), own)

    def whole(t):
        return pl.ds(t * length, length)

    def lanes(h):
        return pl.ds(h * piece, piece)

    def unit_of(t, m):
        return 2 * t + m

    order = [(t, m) for t in range(ticks) for m in (1, 0)]

    x_copies = {}
    for t, m in order:
        u = unit_of(t, m)
        x_copies[t, m] = pltpu.make_async_copy(x_hbm.at[u], xb.at[u], x_sem.at[u])
    small = [
        pltpu.make_async_copy(src, dst, t_sem.at[k])
        for k, (src, dst) in enumerate(((gain_hbm, gain), (cos_hbm, cos_ref), (sin_hbm, sin_ref)))
    ]
    carry_copies = [
        pltpu.make_async_copy(carry.at[m], dyb.at[m, at_rows(0, me)], c_sem.at[m]) for m in (1, 0)
    ]
    top_copies = [
        pltpu.make_async_copy(top.at[t], dyb.at[1, at_rows(t + 1, me)], c_sem.at[2 + t])
        for t in range(ticks - 1)
    ]
    w_copies = [
        pltpu.make_async_copy(src.at[m], dst.at[m], w_sem.at[j, m])
        for m in (1, 0)
        for j, (src, dst) in enumerate(((wq_hbm, wq), (wo_hbm, wo)))
    ]
    carry_copies[0].start()
    small[0].start()
    x_copies[0, 1].start()
    carry_copies[1].start()
    for t, m in order[1:]:
        x_copies[t, m].start()
    for c in small[1:]:
        c.start()

    @pl.when(sec == 0)
    def _():
        for c in top_copies:
            c.start()

    def normalize(t, m):
        u = unit_of(t, m)
        x_copies[t, m].wait()
        x = xb[u].astype(f32)
        inverse = lax.rsqrt(jnp.mean(x * x, axis=-1, keepdims=True) + epsilon)
        nrm[m, at_rows(t, me)] = (x * inverse * gain[m]).astype(bf16)

    gtot[...] = jnp.zeros_like(gtot)
    neighbours = jnp.where(sec > 0, 1, 0) + jnp.where(sec < sections - 1, 1, 0)
    with jax.named_scope("barrier"):
        pl.semaphore_wait(barrier, n * reps - 1 + neighbours)

    def remote(src, dst, send, recv, where):
        return pltpu.make_async_remote_copy(
            src_ref=src, dst_ref=dst, send_sem=send, recv_sem=recv, device_id=where,
            device_id_type=MESH,
        )

    def hop(which, t, m, i, h, up):
        u = unit_of(t, m)
        at = (nrm, dyb)[which].at[m, at_rows(t, i), lanes(h)]
        return remote(
            at, at, g_send.at[which, u, up], g_recv.at[which, u, h, i],
            tensor_at(1 if up else -1),
        )

    def dy_peer(t, m, i, h, j):
        at = at_rows(t, i)
        return remote(
            dyb.at[m, at, lanes(h)], pdy.at[j - 1, m, at, lanes(h)],
            d_send.at[1, j - 1], d_recv.at[1, m, j - 1], dp_at(-j),
        )

    def nrm_peer(t, m, i, j):
        peer = lax.rem(rep - j + reps, reps)
        at = at_rows(t, i)
        return remote(
            nrm.at[m, at, pl.ds(pl.multiple_of(peer * wn, 128), wn)], pnrm.at[j - 1, m, at],
            d_send.at[0, j - 1], d_recv.at[0, m, j - 1], dp_at(-j),
        )

    def rest_peer(which, t, m, j):
        peer = lax.rem(rep - j + reps, reps)
        at = whole(t)
        src, dst = {
            2: (gpb.at[m, at], pgp),
            3: (attb.at[m, at, pl.ds(pl.multiple_of(peer * wa, 128), wa)], patt),
        }[which]
        return remote(
            src, dst.at[j - 1, m, at], d_send.at[which, j - 1], d_recv.at[which, m, j - 1],
            dp_at(-j),
        )

    def peer_layer(which, m, j):
        at = (pnrm, pdy, pgp, patt)[which].at[j - 1, m]
        return remote(at, at, d_send.at[which, j - 1], d_recv.at[which, m, j - 1], dp_at(-j))

    def peer_all(which, j):
        at = (pnrm, pdy, pgp, patt)[which].at[j - 1]
        return remote(at, at, d_send.at[which, j - 1], d_recv.at[which, 0, j - 1], dp_at(-j))

    others = range(1, reps)
    far = range(1, n)

    def to_peers(which, t, m, i, h):
        for j in others:
            if which:
                dy_peer(t, m, i, h, j).start()
            elif h == parts - 1:
                nrm_peer(t, m, i, j).start()

    def own_to_peers(which, t, m):
        for h in range(parts):
            to_peers(which, t, m, me, h)

    def own_hops(which, t, m, edge=None):
        for h in range(parts):
            for up in (1, 0):
                sends = me < n - 1 if up else me > 0
                if edge is not None:
                    sends = (me == 0 if up else me == n - 1) if edge else (me > 0) & (me < n - 1)

                @pl.when(sends)
                def _():
                    hop(which, t, m, me, h, up).start()

    def arrivals(which, t, m, d, forward, source):
        for h in range(parts):
            for up in (1, 0):
                i = me - d if up else me + d
                inside = me >= d if up else me + d < n
                if source == "edge":
                    inside = me == d if up else me + d == n - 1
                elif source == "middle":
                    inside = me > d if up else me + d < n - 1
                middle = me < n - 1 if up else me > 0
                edge = me == n - 1 if up else me == 0

                @pl.when(inside & (middle if forward else edge))
                def _():
                    with jax.named_scope("wait_fwd" if forward else "wait_end"):
                        hop(which, t, m, i, h, up).wait_recv()
                    if forward:
                        hop(which, t, m, i, h, up).start()
                    to_peers(which, t, m, i, h)

    def fwd(what, t, m, *ds, source=None):
        for d in ds:
            if 0 < d < n - 1:
                for which in what:
                    arrivals(which, t, m, d, True, source)

    def end(what, t, m, *ds):
        for d in ds:
            if 0 < d < n:
                for which in what:
                    arrivals(which, t, m, d, False, None)

    def sum_copy(t, m, d, h, way):
        u = unit_of(t, m)
        i = me + d if way else me - d
        return remote(
            pb.at[u, pl.ds(pl.multiple_of(i * own, own), own), lanes(h)],
            rb.at[u, way, d - 1, :, lanes(h)],
            r_send.at[u, way], r_recv.at[u, way, d - 1, h], tensor_at(1 if way else -1),
        )

    def sum_arrived(t, m, d, h, way):
        u = unit_of(t, m)
        at = rb.at[u, way, d, :, lanes(h)]
        remote(at, at, r_send.at[u, way], r_recv.at[u, way, d, h], tensor_at(1)).wait_recv()

    def sum_stage(t, m, stage):
        u = unit_of(t, m)
        for way in (1, 0):

            @pl.when(me == (stage if way else n - 1 - stage))
            def _():
                place = stage if way else n - 1 - stage
                for d in range(n - 1 - stage, 0, -1):
                    i = place + d if way else place - d
                    at = pl.ds(i * own, own)
                    for h in range(parts):
                        if stage:
                            with jax.named_scope("wait_sum"):
                                sum_arrived(t, m, d, h, way)
                            total = pb[u, at, lanes(h)].astype(f32)
                            total = total + rb[u, way, d, :, lanes(h)].astype(f32)
                            pb[u, at, lanes(h)] = total.astype(bf16)
                        sum_copy(t, m, d, h, way).start()

    def sums(t, m, *stages):
        for stage in stages:
            if 0 < stage < n - 1:
                sum_stage(t, m, stage)

    def hops_sent(which, t, m):
        u = unit_of(t, m)
        for up in (1, 0):
            for place in range(n):
                count = place + 1 if up else n - place
                if count < n or (place < n - 1 if up else place > 0):

                    @pl.when(me == place)
                    def _():
                        at = (nrm, dyb)[which].at[m, pl.ds(0, count * own)]
                        sem = g_send.at[which, u, up]
                        remote(at, at, sem, sem, tensor_at(1)).wait_send()

    def sums_sent(t, m):
        u = unit_of(t, m)
        for way in (1, 0):
            for stage in range(n - 1):

                @pl.when(me == (stage if way else n - 1 - stage))
                def _():
                    at = pb.at[u, pl.ds(0, (n - 1 - stage) * own)]
                    remote(at, at, r_send.at[u, way], r_send.at[u, way], tensor_at(1)).wait_send()

    def section_copy(t, m):
        step = 1 if m == 1 else -1
        return remote(
            out.at[unit_of(t, m)], dyb.at[m, at_rows(t + 1, me)], s_send.at[t, m],
            s_recv.at[t, m], {"section": sec + step},
        )

    def gain_copy(a, b):
        slot = a * reps + b
        return remote(
            gtot, grecv.at[slot], gain_send, gain_recv, {**tensor_at(-a), **dp_at(-b)}
        )

    def gain_all():
        at = grecv.at[pl.ds(1, n * reps - 1)]
        return remote(at, at, gain_send, gain_recv, tensor_at(1))

    def swap(values):
        wide = values.shape[1]
        lane = lax.broadcasted_iota(jnp.int32, values.shape, 1)
        low = lax.rem(lane, HD) < HD // 2
        return jnp.where(
            low, pltpu.roll(values, wide - HD // 2, 1), pltpu.roll(values, HD // 2, 1)
        )

    def dot(a, b, ca, cb):
        return lax.dot_general(a, b, (((ca,), (cb,)), ((), ())), preferred_element_type=f32)

    def stack_heads(values):
        return jnp.concatenate([values[:, h * HD : (h + 1) * HD] for h in range(GROUP)], axis=0)

    def spread_heads(values):
        return jnp.concatenate(
            [values[h * length : (h + 1) * length] for h in range(GROUP)], axis=1
        )

    def table(ref, wide):
        return jnp.concatenate([ref[...]] * (wide // 128), axis=1)

    span = (GROUP + 2) * HD

    def forward(t, m):
        u = unit_of(t, m)
        projected = dot(nrm[m, whole(t)], wq[m], 1, 0)
        rotated = projected * table(cos_ref, cols) + swap(projected) * table(sin_ref, cols)
        rotated = rotated.astype(bf16)
        row = lax.broadcasted_iota(jnp.int32, (length, length), 0)
        key_row = lax.broadcasted_iota(jnp.int32, (length, length), 1)
        bias = jnp.where(row >= key_row, 0.0, -1e30)
        for g in range(groups):
            at = g * span
            qs = stack_heads(rotated[:, at : at + GROUP * HD])
            key = rotated[:, at + GROUP * HD : at + (GROUP + 1) * HD]
            value = projected[:, at + (GROUP + 1) * HD : at + span].astype(bf16)
            scores = dot(qs, key, 1, 1) * scale
            scores = (scores.reshape(GROUP, length, length) + bias[None]).reshape(
                GROUP * length, length
            )
            e = jnp.exp(scores - jnp.max(scores, axis=-1, keepdims=True))
            sm = e / jnp.sum(e, axis=-1, keepdims=True)
            smb[u, g] = sm
            qsb[u, g] = qs
            kb[u, g] = key
            vb[u, g] = value
            attended = spread_heads(dot(sm.astype(bf16), value, 1, 0).astype(bf16))
            attb[m, whole(t), g * GROUP * HD : (g + 1) * GROUP * HD] = attended
        for j in others:
            rest_peer(3, t, m, j).start()

    def backward(t, m):
        u = unit_of(t, m)
        grad_att = dot(dyb[m, whole(t)], wo[m], 1, 1).astype(bf16)
        for g in range(groups):
            sm = smb[u, g]
            low = sm.astype(bf16)
            value = vb[u, g]
            gs = stack_heads(grad_att[:, g * GROUP * HD : (g + 1) * GROUP * HD])
            gsm = dot(gs, value, 1, 1)
            total = jnp.sum(sm * gsm, axis=-1, keepdims=True)
            gsc = (sm * (gsm - total) * scale).astype(bf16)
            g_value = dot(low, gs, 0, 0)
            g_query = spread_heads(dot(gsc, kb[u, g], 1, 0))
            g_key = dot(gsc, qsb[u, g], 0, 0)
            turned = jnp.concatenate([g_query, g_key, g_value], axis=1)
            back = turned * table(cos_ref, span) - swap(turned) * table(sin_ref, span)
            lane = lax.broadcasted_iota(jnp.int32, turned.shape, 1)
            back = jnp.where(lane < (GROUP + 1) * HD, back, turned)
            gpb[m, whole(t), g * span : (g + 1) * span] = back.astype(bf16)
        pb[u] = dot(gpb[m, whole(t)], wq[m], 1, 1).astype(bf16)
        sum_stage(t, m, 0)
        for j in others:
            rest_peer(2, t, m, j).start()

    def finish(t, m):
        u = unit_of(t, m)
        x = xb[u].astype(f32)
        inverse = lax.rsqrt(jnp.mean(x * x, axis=-1, keepdims=True) + epsilon)
        unit = x * inverse
        mine = pl.ds(pl.multiple_of(me * own, own), own)
        gsum[...] = pb[u, mine].astype(f32)
        for way in (1, 0):

            @pl.when(me > 0 if way else me < n - 1)
            def _():
                with jax.named_scope("wait_scatter"):
                    for h in range(parts):
                        sum_arrived(t, m, 0, h, way)
                gsum[...] = gsum[...] + rb[u, way, 0].astype(f32)

        gn = gsum[...]
        gu = gn * gain[m]
        grad = inverse * (gu - unit * jnp.mean(gu * unit, axis=-1, keepdims=True))
        out[u] = (dyb[m, at_rows(t, me)].astype(f32) + grad).astype(bf16)
        if (t, m) != (ticks - 1, 0):
            gtot[m] = gtot[m] + jnp.sum(gn * unit, axis=0, keepdims=True)

    def gain_of_parts(t, m):
        part = pb[unit_of(t, m)].astype(f32) * nrm[m, whole(t)].astype(f32)
        gtot[m] = gtot[m] + jnp.sum(part, axis=0, keepdims=True) / gain[m]

    def hand_over(t, m):
        if t + 1 == ticks:
            return

        @pl.when(sec < sections - 1 if m == 1 else sec > 0)
        def _():
            section_copy(t, m).start()

        if m == 1:

            @pl.when(sec == sections - 1)
            def _():
                dyb[0, at_rows(t + 1, me)] = out[unit_of(t, 1)]

    def taken_over(t, m):
        with jax.named_scope("wait_section"):

            @pl.when(sec > 0 if m == 1 else sec < sections - 1)
            def _():
                section_copy(t - 1, m).wait_recv()

            if m == 1:

                @pl.when(sec == 0)
                def _():
                    top_copies[t - 1].wait()

    def wait_peers(m, *kinds):
        with jax.named_scope("wait_dp"):
            for which in kinds:
                for j in others:
                    peer_layer(which, m, j).wait_recv()

    def rounded(a, b):
        return dot(a, b, 0, 0).astype(bf16).astype(f32)

    def grad_out(m):
        wide = 512 if width % 512 == 0 else 128
        att_at = pl.ds(pl.multiple_of(rep * wa, 128), wa)

        @pl.loop(0, width // wide)
        def _(c):
            at = pl.ds(pl.multiple_of(c * wide, 128), wide)
            total = rounded(attb[m, :, att_at], dyb[m, :, at])
            for j in others:
                total = total + rounded(patt[j - 1, m], pdy[j - 1, m, :, at])
            go_out[m, :, at] = total.astype(bf16)

    def grad_qkv(m):
        block = 256 if wn % 256 == 0 else 128

        @pl.loop(0, wn // block)
        def _(c):
            own_at = pl.ds(pl.multiple_of(rep * wn + c * block, 128), block)
            at = pl.ds(pl.multiple_of(c * block, 128), block)
            total = rounded(nrm[m, :, own_at], gpb[m])
            for j in others:
                total = total + rounded(pnrm[j - 1, m, :, at], pgp[j - 1, m])
            gq_out[m, at] = total.astype(bf16)

    def grads_of(m):
        wait_peers(m, 1, 3)
        with jax.named_scope("grad_out"):
            grad_out(m)
        wait_peers(m, 0, 2)
        with jax.named_scope("grad_qkv"):
            grad_qkv(m)

    inner = range(1, n - 1)
    dy, x = 1, 0
    both = (dy, x)

    carry_copies[0].wait()
    own_hops(dy, 0, 1)
    own_to_peers(dy, 0, 1)
    small[0].wait()
    normalize(0, 1)
    own_hops(x, 0, 1)
    own_to_peers(x, 0, 1)
    carry_copies[1].wait()
    own_to_peers(dy, 0, 0)
    for t, m in order[1:]:
        normalize(t, m)
        own_to_peers(x, t, m)
    for c in w_copies:
        c.start()
    fwd(both, 0, 1, *inner)
    end(both, 0, 1, *inner)
    for which in both:
        own_hops(which, 0, 0)
    with jax.named_scope("wait_weights"):
        for c in w_copies:
            c.wait()
        for c in small[1:]:
            c.wait()
    end(both, 0, 1, n - 1)
    with jax.named_scope("forward"):
        forward(0, 1)
    with jax.named_scope("backward"):
        backward(0, 1)
    own_hops(x, 1, 1, edge=True)
    fwd(both, 0, 0, 1)
    end(both, 0, 0, 1)
    fwd(both, 0, 0, *inner[1:])
    end(both, 0, 0, *inner[1:])

    def give(which, t, m):
        fwd((which,), t, m, 1, source="middle")
        fwd((which,), t, m, 1, source="edge")

    for t in range(1, ticks):
        late = both if t == 1 else (dy,)
        if t > 1:
            own_hops(x, t, 1, edge=True)
        sums(t - 1, 1, 1)
        end(late, t - 1, 0, n - 1)
        if t == 1:
            with jax.named_scope("forward"):
                forward(t - 1, 0)
        sums(t - 1, 1, *inner[1:])
        own_hops(x, t, 1, edge=False)
        with jax.named_scope("backward"):
            backward(t - 1, 0)
        give(x, t, 1)
        finish(t - 1, 1)
        hand_over(t - 1, 1)
        fwd((x,), t, 1, *inner[1:])
        end((x,), t, 1, 1)
        taken_over(t, 1)
        own_to_peers(dy, t, 1)
        own_hops(dy, t, 1)
        end((x,), t, 1, *far[1:-1])
        fwd((dy,), t, 1, 1, source="middle")
        end((x,), t, 1, n - 1)
        with jax.named_scope("forward"):
            forward(t, 1)
        own_hops(x, t, 0, edge=True)
        sums(t - 1, 0, 1)
        fwd((dy,), t, 1, 1, source="edge")
        sums(t - 1, 0, *inner[1:])
        fwd((dy,), t, 1, *inner[1:])
        own_hops(x, t, 0, edge=False)
        end((dy,), t, 1, *far[:-1])
        finish(t - 1, 0)
        hand_over(t - 1, 0)
        give(x, t, 0)
        end((dy,), t, 1, n - 1)
        taken_over(t, 0)
        own_to_peers(dy, t, 0)
        own_hops(dy, t, 0)
        with jax.named_scope("backward"):
            backward(t, 1)
        fwd((x,), t, 0, *inner[1:])
        end((x,), t, 0, 1)
        end((x,), t, 0, *far[1:-1])
        give(dy, t, 0)
        end((x,), t, 0, n - 1)
        with jax.named_scope("forward"):
            forward(t, 0)
        fwd((dy,), t, 0, *inner[1:])
        if t + 1 == ticks:
            sums(t, 1, *inner)
        end((dy,), t, 0, *(far if t + 1 == ticks else far[:-1]))

    last = ticks - 1
    with jax.named_scope("backward"):
        backward(last, 0)
    finish(last, 1)
    gain_of_parts(last, 0)
    for a in range(n):
        for b in range(reps):
            if a or b:
                gain_copy(a, b).start()
    grads_of(1)
    sums(last, 0, *inner)
    grads_of(0)
    finish(last, 0)
    total = gtot[...]
    gain_all().wait_recv()
    for slot in range(1, n * reps):
        total = total + grecv[slot]
    gain_out[...] = total
    with jax.named_scope("wait_sends"):
        for t, m in order:
            sums_sent(t, m)
            for which in both:
                hops_sent(which, t, m)
        for j in others:
            for which in range(4):
                peer_all(which, j).wait_send()
        for t in range(ticks - 1):

            @pl.when(sec < sections - 1)
            def _():
                section_copy(t, 1).wait_send()

            @pl.when(sec > 0)
            def _():
                section_copy(t, 0).wait_send()

        gain_all().wait_send()


def write_back(a, b, c, d, a_out, b_out, c_out, d_out, sem):
    pairs = ((a, a_out), (b, b_out), (c, c_out), (d, d_out))
    copies = [pltpu.make_async_copy(src, dst, sem.at[k]) for k, (src, dst) in enumerate(pairs)]
    for c in copies:
        c.start()
    for c in copies:
        c.wait()


def lane_tables(length):
    cosine, sine = rope_tables(jnp.arange(length), HD)
    copies = 128 // HD
    cosine = jnp.tile(jnp.concatenate([cosine, cosine], axis=1), (1, copies))
    sine = jnp.tile(jnp.concatenate([-sine, sine], axis=1), (1, copies))
    return cosine, sine


def local(layer_in, carry_in, top_grad, w_qkv, w_out, gain):
    ticks, own, width = layer_in.shape[0], layer_in.shape[4], layer_in.shape[5]
    n = lax.axis_size("tensor")
    reps = lax.axis_size("dp")
    sections = lax.axis_size("section")
    cols, hq = w_qkv.shape[3], w_out.shape[2]
    lined = (width // reps) % 128 == 0 and (hq // reps) % 128 == 0 and cols % 128 == 0
    if not lined or own % 16 or ticks < 2 or n < 3:
        return local_permutes(layer_in, carry_in, top_grad, w_qkv, w_out, gain)
    length = n * own
    units = 2 * ticks
    deep = ticks * length
    groups = hq // (GROUP * HD)
    wn, wa = width // reps, hq // reps
    f32, bf16 = jnp.float32, jnp.bfloat16
    parts = PARTS if width % (PARTS * 128) == 0 else 1
    with jax.ensure_compile_time_eval():
        cosine, sine = lane_tables(length)
    vmem = pl.BlockSpec(memory_space=pltpu.VMEM)
    hbm = pl.BlockSpec(memory_space=pl.ANY)
    dma = pltpu.SemaphoreType.DMA
    outs = pl.pallas_call(
        functools.partial(fused, n, reps, ticks, sections, own),
        out_shape=(
            pltpu.VMEM((units, own, width), bf16),
            pltpu.VMEM((2, wn, cols), bf16),
            pltpu.VMEM((2, wa, width), bf16),
            pltpu.VMEM((2, 1, width), f32),
        ),
        in_specs=[hbm] * 8,
        out_specs=(vmem,) * 4,
        scratch_shapes=[
            pltpu.VMEM((2, width, cols), bf16),
            pltpu.VMEM((2, hq, width), bf16),
            pltpu.VMEM((units, own, width), bf16),
            pltpu.VMEM((2, 1, width), f32),
            pltpu.VMEM((length, 128), f32),
            pltpu.VMEM((length, 128), f32),
            pltpu.VMEM((2, deep, width), bf16),
            pltpu.VMEM((2, deep, width), bf16),
            pltpu.VMEM((2, deep, cols), bf16),
            pltpu.VMEM((2, deep, hq), bf16),
            pltpu.VMEM((reps - 1, 2, deep, wn), bf16),
            pltpu.VMEM((reps - 1, 2, deep, width), bf16),
            pltpu.VMEM((reps - 1, 2, deep, cols), bf16),
            pltpu.VMEM((reps - 1, 2, deep, wa), bf16),
            pltpu.VMEM((units, length, width), bf16),
            pltpu.VMEM((units, 2, n - 1, own, width), bf16),
            pltpu.VMEM((units, groups, GROUP * length, length), f32),
            pltpu.VMEM((units, groups, GROUP * length, HD), bf16),
            pltpu.VMEM((units, groups, length, HD), bf16),
            pltpu.VMEM((units, groups, length, HD), bf16),
            pltpu.VMEM((2, 1, width), f32),
            pltpu.VMEM((n * reps, 2, 1, width), f32),
            pltpu.VMEM((own, width), f32),
            dma((2, 2)),
            dma((units,)),
            dma((1 + ticks,)),
            dma((3,)),
            dma((2, units, 2)),
            dma((2, units, parts, n)),
            dma((units, 2)),
            dma((units, 2, n - 1, parts)),
            dma((ticks - 1, 2)),
            dma((ticks - 1, 2)),
            dma((4, reps - 1)),
            dma((4, 2, reps - 1)),
            dma(()),
            dma(()),
        ],
        compiler_params=pltpu.CompilerParams(
            collective_id=0, has_side_effects=True, vmem_limit_bytes=50 * 1024 * 1024
        ),
    )(
        layer_in[:, :, 0, 0].reshape(units, own, width),
        carry_in[:, 0, 0],
        top_grad[:, 0],
        gain,
        w_qkv[:, 0],
        w_out[:, 0],
        cosine,
        sine,
    )
    outs = pl.pallas_call(
        write_back,
        out_shape=(
            jax.ShapeDtypeStruct((units, own, width), bf16),
            jax.ShapeDtypeStruct((2, wn, cols), bf16),
            jax.ShapeDtypeStruct((2, wa, width), bf16),
            jax.ShapeDtypeStruct((2, 1, width), f32),
        ),
        in_specs=[vmem] * 4,
        out_specs=(hbm,) * 4,
        scratch_shapes=[dma((4,))],
        compiler_params=pltpu.CompilerParams(vmem_limit_bytes=1024 * 1024),
    )(*[pltpu.with_memory_space_constraint(o, pltpu.VMEM) for o in outs])
    return (
        outs[0].reshape(ticks, 2, 1, 1, own, width),
        outs[1][:, None],
        outs[2][:, None],
        outs[3],
    )


def solution(mesh):
    in_specs = (
        P(None, None, "section", "dp", "tensor", None),
        P(None, "section", "dp", "tensor", None),
        P(None, "dp", "tensor", None),
        P(None, "section", None, "tensor"),
        P(None, "section", "tensor", None),
        P(None, "section", None),
    )
    out_specs = (
        P(None, None, "section", "dp", "tensor", None),
        P(None, "section", "dp", "tensor"),
        P(None, "section", ("tensor", "dp"), None),
        P(None, "section", None),
    )
    return jax.shard_map(local, mesh=mesh, in_specs=in_specs, out_specs=out_specs, check_vma=False)
```

```python
import functools
import math

import jax
import jax.numpy as jnp
from jax import lax
from jax.experimental import pallas as pl
from jax.experimental.pallas import tpu as pltpu
from jax.sharding import PartitionSpec as P

HD = 64
GROUP = 8

epsilon = 1e-06
rope_base = 1000000.0


MESH = pl.DeviceIdType.MESH
PARTS = 2
LAST_PARTS = 4

contract_rows = (((0,), (0,)), ((), ()))
contract_cols = (((1,), (1,)), ((), ()))


def from_behind(value, axis, steps):
    count = lax.axis_size(axis)
    first, last = (max(0, -steps), min(count, count - steps))
    return lax.ppermute(value, axis, [(source, source + steps) for source in range(first, last)])


def from_ahead(value, axis, steps):
    count = lax.axis_size(axis)
    return lax.ppermute(value, axis, [((i + steps) % count, i) for i in range(count)])


def rope_tables(positions, head_width):
    half_width = head_width // 2
    exponent = jnp.arange(half_width, dtype=jnp.float32) * (2.0 / head_width)
    frequency = rope_base ** (-exponent)
    angle = positions.astype(jnp.float32)[:, None] * frequency[None, :]
    return (jnp.cos(angle), jnp.sin(angle))


def rotate(values, cosine_table, sine_table, direction):
    half_width = values.shape[-1] // 2
    table_shape = (values.shape[0],) + (1,) * (values.ndim - 2) + (half_width,)
    cosine = cosine_table.reshape(table_shape)
    sine_part = direction * sine_table.reshape(table_shape)
    lower_half = values[..., :half_width]
    upper_half = values[..., half_width:]
    return jnp.concatenate(
        [
            lower_half * cosine - upper_half * sine_part,
            upper_half * cosine + lower_half * sine_part,
        ],
        axis=-1,
    )


def unit_compute(normed, grad_full, w_qkv, w_out, tables, mask):
    length = normed.shape[0]
    kv_local = w_out.shape[0] // (GROUP * HD)
    cosine_table, sine_table = tables
    score_scale = 1.0 / math.sqrt(HD)
    projected = jnp.dot(normed, w_qkv, preferred_element_type=jnp.float32)
    projected = projected.reshape(length, kv_local, GROUP + 2, HD)
    query_rot = rotate(projected[:, :, :GROUP], cosine_table, sine_table, 1.0).astype(jnp.bfloat16)
    key_rot = rotate(projected[:, :, GROUP], cosine_table, sine_table, 1.0).astype(jnp.bfloat16)
    value_rows = projected[:, :, GROUP + 1].astype(jnp.bfloat16)
    f32 = dict(preferred_element_type=jnp.float32)
    scores = jnp.einsum("tkgd,ukd->kgtu", query_rot, key_rot, **f32) * score_scale
    scores = jnp.where(mask, scores, -1e30)
    exponentials = jnp.exp(scores - jnp.max(scores, axis=-1, keepdims=True))
    softmax_rows = exponentials / jnp.sum(exponentials, axis=-1, keepdims=True)
    softmax_low = softmax_rows.astype(jnp.bfloat16)
    attended = jnp.einsum("kgtu,ukd->tkgd", softmax_low, value_rows, **f32)
    attended = attended.astype(jnp.bfloat16).reshape(length, kv_local * GROUP * HD)
    grad_attended = lax.dot_general(grad_full, w_out, contract_cols, **f32).astype(jnp.bfloat16)
    grad_heads = grad_attended.reshape(length, kv_local, GROUP, HD)
    grad_softmax = jnp.einsum("tkgd,ukd->kgtu", grad_heads, value_rows, **f32)
    row_total = jnp.sum(softmax_rows * grad_softmax, axis=-1, keepdims=True)
    grad_scores = (softmax_rows * (grad_softmax - row_total) * score_scale).astype(jnp.bfloat16)
    grad_value = jnp.einsum("kgtu,tkgd->ukd", softmax_low, grad_heads, **f32)
    grad_query = rotate(
        jnp.einsum("kgtu,ukd->tkgd", grad_scores, key_rot, **f32), cosine_table, sine_table, -1.0
    )
    grad_key = rotate(
        jnp.einsum("kgtu,tkgd->ukd", grad_scores, query_rot, **f32), cosine_table, sine_table, -1.0
    )
    grad_projected = jnp.concatenate(
        [grad_query, grad_key[:, :, None], grad_value[:, :, None]], axis=2
    )
    grad_projected = grad_projected.reshape(length, kv_local * (GROUP + 2) * HD)
    grad_projected = grad_projected.astype(jnp.bfloat16)
    partial = lax.dot_general(grad_projected, w_qkv, contract_cols, **f32).astype(jnp.bfloat16)
    return attended, grad_projected, partial


def local_permutes(layer_in, carry_in, top_grad, w_qkv, w_out, gain):
    ticks = layer_in.shape[0]
    own = layer_in.shape[4]
    n_tensor = lax.axis_size("tensor")
    n_dp = lax.axis_size("dp")
    me_tensor = lax.axis_index("tensor")
    me_dp = lax.axis_index("dp")
    section_index = lax.axis_index("section")
    at_first = section_index == 0
    at_last = section_index == lax.axis_size("section") - 1
    owners = (me_tensor + jnp.arange(n_tensor)) % n_tensor
    positions = (owners[:, None] * own + jnp.arange(own)[None, :]).reshape(-1)
    tables = rope_tables(positions, HD)
    mask = positions[:, None] >= positions[None, :]
    layer_rows = layer_in[:, :, 0, 0]
    carried = carry_in[:, 0, 0]
    fresh_grads = top_grad[:, 0]
    weight_qkv = w_qkv[:, 0]
    weight_out = w_out[:, 0]
    gain_rows = gain[:, 0]

    def gather(value):
        return jnp.concatenate(
            [value] + [from_ahead(value, "tensor", k) for k in range(1, n_tensor)], axis=0
        )

    def scatter_sum(partial):
        total = partial[:own].astype(jnp.float32)
        for k in range(1, n_tensor):
            chunk = partial[k * own : (k + 1) * own]
            total = total + from_ahead(chunk, "tensor", -k).astype(jnp.float32)
        return total

    def columns_of(value, index):
        width = value.shape[1] // n_dp
        return lax.dynamic_slice_in_dim(value, index * width, width, axis=1)

    def exchange(value, cut):
        if cut:
            return [columns_of(value, me_dp)] + [
                from_ahead(columns_of(value, (me_dp - k) % n_dp), "dp", k) for k in range(1, n_dp)
            ]
        return [value] + [from_ahead(value, "dp", k) for k in range(1, n_dp)]

    members = (1, 0)
    unit_rows, inverse, normed = {}, {}, {}
    for t in range(ticks):
        for m in members:
            rows = layer_rows[t, m].astype(jnp.float32)
            inverse[t, m] = lax.rsqrt(jnp.mean(rows * rows, axis=-1, keepdims=True) + epsilon)
            unit_rows[t, m] = rows * inverse[t, m]
            normed[t, m] = (unit_rows[t, m] * gain_rows[m]).astype(jnp.bfloat16)
    inputs = [carried[0], carried[1]]
    factors = {}
    per_tick = []
    gain_totals = [0.0, 0.0]
    for t in range(ticks):
        outcome = [None, None]
        for m in members:
            dy = inputs[m]
            full_normed = gather(normed[t, m])
            full_grad = gather(dy)
            attended, grad_projected, partial = unit_compute(
                full_normed, full_grad, weight_qkv[m], weight_out[m], tables, mask
            )
            factors[t, m] = (
                exchange(full_normed, True),
                exchange(grad_projected, False),
                exchange(attended, True),
                exchange(full_grad, False),
            )
            grad_normed = scatter_sum(partial)
            grad_unit = grad_normed * gain_rows[m]
            unit = unit_rows[t, m]
            grad_rows = inverse[t, m] * (
                grad_unit - unit * jnp.mean(grad_unit * unit, axis=-1, keepdims=True)
            )
            outcome[m] = (dy.astype(jnp.float32) + grad_rows).astype(jnp.bfloat16)
            gain_totals[m] = gain_totals[m] + jnp.sum(grad_normed * unit, axis=0)
        if t + 1 < ticks:
            upward = from_behind(outcome[1], "section", 1)
            downward = from_behind(outcome[0], "section", -1)
            inputs = [
                jnp.where(at_last, outcome[1], downward),
                jnp.where(at_first, fresh_grads[t], upward),
            ]
        per_tick.append(jnp.stack(outcome))

    def weight_grad(m, left, right):
        total = None
        for k in range(n_dp):
            a = jnp.concatenate([factors[t, m][left][k] for t in range(ticks)], axis=0)
            b = jnp.concatenate([factors[t, m][right][k] for t in range(ticks)], axis=0)
            part = lax.dot_general(a, b, contract_rows, preferred_element_type=jnp.float32)
            part = part.astype(jnp.bfloat16).astype(jnp.float32)
            total = part if total is None else total + part
        return total.astype(jnp.bfloat16)

    grad_qkv = jnp.stack([weight_grad(m, 0, 1) for m in (0, 1)])
    grad_out = jnp.stack([weight_grad(m, 2, 3) for m in (0, 1)])
    gain_total = lax.psum(jnp.stack(gain_totals), ("tensor", "dp"))
    return (
        jnp.stack(per_tick)[:, :, None, None],
        grad_qkv[:, None],
        grad_out[:, None],
        gain_total[:, None],
    )


def fused(
    n, reps, ticks, sections, own,
    x_hbm, carry, top, gain_hbm, wq_hbm, wo_hbm, cos_hbm, sin_hbm,
    out, gq_out, go_out, gain_out,
    wq, wo, xb, gain, cos_ref, sin_ref,
    nrm, dyb, gpb, attb, pnrm, pdy, pgp, patt, pb, rb, smb, qsb, kb, vb, gtot, grecv, gsumd, gfull, gsum,
    w_sem, x_sem, c_sem, t_sem, g_send, g_recv, r_send, r_recv, l_recv, s_send, s_recv, d_send, d_recv,
    gain_send, gain_recv,
):
    f32 = jnp.float32
    bf16 = jnp.bfloat16
    me = lax.axis_index("tensor")
    rep = lax.axis_index("dp")
    sec = lax.axis_index("section")
    length = n * own
    units = 2 * ticks
    hq = wo.shape[1]
    width = wq.shape[1]
    cols = wq.shape[2]
    groups = hq // (GROUP * HD)
    wn = width // reps
    wa = hq // reps
    scale = 1.0 / math.sqrt(HD)
    parts = PARTS if width % (PARTS * 128) == 0 else 1
    last_parts = LAST_PARTS if width % (LAST_PARTS * 128) == 0 else 1
    piece = width // parts

    def tensor_at(k):
        return {"tensor": lax.rem(me + k + n, n)}

    def dp_at(k):
        return {"dp": lax.rem(rep + k + reps, reps)}

    barrier = pltpu.get_barrier_semaphore()
    for a in range(n):
        for b in range(reps):
            if a or b:
                pl.semaphore_signal(
                    barrier, inc=1, device_id={**tensor_at(a), **dp_at(b)}, device_id_type=MESH
                )

    @pl.when(sec > 0)
    def _():
        pl.semaphore_signal(barrier, inc=1, device_id={"section": sec - 1}, device_id_type=MESH)

    @pl.when(sec < sections - 1)
    def _():
        pl.semaphore_signal(barrier, inc=1, device_id={"section": sec + 1}, device_id_type=MESH)

    def at_rows(t, i):
        return pl.ds(pl.multiple_of(t * length + i * own, own), own)

    def whole(t):
        return pl.ds(t * length, length)

    def lanes(h):
        return pl.ds(h * piece, piece)

    def unit_of(t, m):
        return 2 * t + m

    order = [(t, m) for t in range(ticks) for m in (1, 0)]

    x_copies = {}
    for t, m in order:
        u = unit_of(t, m)
        x_copies[t, m] = pltpu.make_async_copy(x_hbm.at[u], xb.at[u], x_sem.at[u])
    small = [
        pltpu.make_async_copy(src, dst, t_sem.at[k])
        for k, (src, dst) in enumerate(((gain_hbm, gain), (cos_hbm, cos_ref), (sin_hbm, sin_ref)))
    ]
    carry_copies = [
        pltpu.make_async_copy(carry.at[m], dyb.at[m, at_rows(0, me)], c_sem.at[m]) for m in (1, 0)
    ]
    top_copies = [
        pltpu.make_async_copy(top.at[t], dyb.at[1, at_rows(t + 1, me)], c_sem.at[2 + t])
        for t in range(ticks - 1)
    ]
    w_copies = [
        pltpu.make_async_copy(src.at[m], dst.at[m], w_sem.at[j, m])
        for m in (1, 0)
        for j, (src, dst) in enumerate(((wq_hbm, wq), (wo_hbm, wo)))
    ]
    carry_copies[0].start()
    small[0].start()
    x_copies[0, 1].start()
    carry_copies[1].start()
    for t, m in order[1:]:
        x_copies[t, m].start()
    for c in small[1:]:
        c.start()

    @pl.when(sec == 0)
    def _():
        for c in top_copies:
            c.start()

    def normalize(t, m):
        u = unit_of(t, m)
        x_copies[t, m].wait()
        x = xb[u].astype(f32)
        inverse = lax.rsqrt(jnp.mean(x * x, axis=-1, keepdims=True) + epsilon)
        nrm[m, at_rows(t, me)] = (x * inverse * gain[m]).astype(bf16)

    gtot[...] = jnp.zeros_like(gtot)
    neighbours = jnp.where(sec > 0, 1, 0) + jnp.where(sec < sections - 1, 1, 0)
    with jax.named_scope("barrier"):
        pl.semaphore_wait(barrier, n * reps - 1 + neighbours)

    def remote(src, dst, send, recv, where):
        return pltpu.make_async_remote_copy(
            src_ref=src, dst_ref=dst, send_sem=send, recv_sem=recv, device_id=where,
            device_id_type=MESH,
        )

    def hop(which, t, m, i, h, up):
        u = unit_of(t, m)
        at = (nrm, dyb)[which].at[m, at_rows(t, i), lanes(h)]
        return remote(
            at, at, g_send.at[which, up], g_recv.at[which, u, h, i],
            tensor_at(1 if up else -1),
        )

    def dy_peer(t, m, i, h, j):
        at = at_rows(t, i)
        return remote(
            dyb.at[m, at, lanes(h)], pdy.at[j - 1, m, at, lanes(h)],
            d_send.at[1, j - 1], d_recv.at[1, m, j - 1], dp_at(-j),
        )

    def nrm_peer(t, m, i, j):
        peer = lax.rem(rep - j + reps, reps)
        at = at_rows(t, i)
        return remote(
            nrm.at[m, at, pl.ds(pl.multiple_of(peer * wn, 128), wn)], pnrm.at[j - 1, m, at],
            d_send.at[0, j - 1], d_recv.at[0, m, j - 1], dp_at(-j),
        )

    def rest_peer(which, t, m, j):
        peer = lax.rem(rep - j + reps, reps)
        at = whole(t)
        src, dst = {
            2: (gpb.at[m, at], pgp),
            3: (attb.at[m, at, pl.ds(pl.multiple_of(peer * wa, 128), wa)], patt),
        }[which]
        return remote(
            src, dst.at[j - 1, m, at], d_send.at[which, j - 1], d_recv.at[which, m, j - 1],
            dp_at(-j),
        )

    def peer_layer(which, m, j):
        at = (pnrm, pdy, pgp, patt)[which].at[j - 1, m]
        return remote(at, at, d_send.at[which, j - 1], d_recv.at[which, m, j - 1], dp_at(-j))

    def peer_all(which, j):
        at = (pnrm, pdy, pgp, patt)[which].at[j - 1]
        return remote(at, at, d_send.at[which, j - 1], d_recv.at[which, 0, j - 1], dp_at(-j))

    others = range(1, reps)
    far = range(1, n)

    def to_peers(which, t, m, i, h):
        for j in others:
            if which:
                dy_peer(t, m, i, h, j).start()
            elif h == parts - 1:
                nrm_peer(t, m, i, j).start()

    def own_to_peers(which, t, m):
        for h in range(parts):
            to_peers(which, t, m, me, h)

    def own_hops(which, t, m, edge=None):
        for h in range(parts):
            for up in (1, 0):
                sends = me < n - 1 if up else me > 0
                if edge is not None:
                    sends = (me == 0 if up else me == n - 1) if edge else (me > 0) & (me < n - 1)

                @pl.when(sends)
                def _():
                    hop(which, t, m, me, h, up).start()

    def arrivals(which, t, m, d, forward, source):
        for h in range(parts):
            for up in (1, 0):
                i = me - d if up else me + d
                inside = me >= d if up else me + d < n
                if source == "edge":
                    inside = me == d if up else me + d == n - 1
                elif source == "middle":
                    inside = me > d if up else me + d < n - 1
                middle = me < n - 1 if up else me > 0
                edge = me == n - 1 if up else me == 0

                @pl.when(inside & (middle if forward else edge))
                def _():
                    with jax.named_scope("wait_fwd" if forward else "wait_end"):
                        hop(which, t, m, i, h, up).wait_recv()
                    if forward:
                        hop(which, t, m, i, h, up).start()
                    to_peers(which, t, m, i, h)

    def fwd(what, t, m, *ds, source=None):
        for d in ds:
            if 0 < d < n - 1:
                for which in what:
                    arrivals(which, t, m, d, True, source)

    def end(what, t, m, *ds):
        for d in ds:
            if 0 < d < n:
                for which in what:
                    arrivals(which, t, m, d, False, None)

    def is_last(t, m):
        return (t, m) == (ticks - 1, 0)

    def sum_parts(t, m):
        return last_parts if is_last(t, m) else parts

    def sum_lanes(t, m, h):
        wide = width // sum_parts(t, m)
        return pl.ds(h * wide, wide)

    def sum_sem(t, m, way, d, h):
        return l_recv.at[way, d, h] if is_last(t, m) else r_recv.at[order.index((t, m)), way, d, h]

    def sum_copy(t, m, d, h, way):
        u = unit_of(t, m)
        i = me + d if way else me - d
        at = sum_lanes(t, m, h)
        return remote(
            pb.at[u, pl.ds(pl.multiple_of(i * own, own), own), at], rb.at[u, way, d - 1, :, at],
            r_send.at[way], sum_sem(t, m, way, d - 1, h), tensor_at(1 if way else -1),
        )

    def sum_arrived(t, m, d, h, way):
        u = unit_of(t, m)
        at = rb.at[u, way, d, :, sum_lanes(t, m, h)]
        remote(at, at, r_send.at[way], sum_sem(t, m, way, d, h), tensor_at(1)).wait_recv()

    def sum_step(t, m, stage, d):
        u = unit_of(t, m)
        for way in (1, 0):

            @pl.when(me == (stage if way else n - 1 - stage))
            def _():
                place = stage if way else n - 1 - stage
                i = place + d if way else place - d
                rows = pl.ds(i * own, own)
                for h in range(sum_parts(t, m)):
                    if stage:
                        at = sum_lanes(t, m, h)
                        with jax.named_scope("wait_sum"):
                            sum_arrived(t, m, d, h, way)
                        total = pb[u, rows, at].astype(f32)
                        total = total + rb[u, way, d, :, at].astype(f32)
                        pb[u, rows, at] = total.astype(bf16)
                    sum_copy(t, m, d, h, way).start()

    def sums_far(t, m):
        if n > 3:
            sum_step(t, m, 1, n - 2)

    def sums_near(t, m):
        steps = [(stage, d) for stage in range(1, n - 1) for d in range(1, n - stage)]
        for stage, d in sorted(steps, key=lambda step: (-step[1], -step[0])):
            if d < n - 2 or n == 3:
                sum_step(t, m, stage, d)

    def sums_sent():
        for way in (1, 0):
            for stage in range(n - 1):

                @pl.when(me == (stage if way else n - 1 - stage))
                def _():
                    at = pb.at[:, pl.ds(0, (n - 1 - stage) * own)]
                    remote(at, at, r_send.at[way], r_send.at[way], tensor_at(1)).wait_send()

    def hops_sent(which):
        for up in (1, 0):
            for place in range(n):
                count = place + 1 if up else n - place
                if count < n or (place < n - 1 if up else place > 0):

                    @pl.when(me == place)
                    def _():
                        at = (nrm, dyb)[which].at[:, pl.ds(0, ticks * count * own)]
                        sem = g_send.at[which, up]
                        remote(at, at, sem, sem, tensor_at(1)).wait_send()

    def section_copy(t, m):
        step = 1 if m == 1 else -1
        return remote(
            out.at[unit_of(t, m)], dyb.at[m, at_rows(t + 1, me)], s_send.at[t, m],
            s_recv.at[t, m], {"section": sec + step},
        )

    share = 2 * width // (n * reps)
    mates = [(a, b) for a in range(n) for b in range(reps) if a or b]

    def share_of(a, b):
        k = lax.rem(me + a, n) * reps + lax.rem(rep + b, reps)
        return pl.ds(pl.multiple_of(k * share, 128), share)

    def share_copy(a, b):
        return remote(
            gtot.at[:, share_of(a, b)], grecv.at[a * reps + b], gain_send.at[0], gain_recv.at[0],
            {**tensor_at(a), **dp_at(b)},
        )

    def spread_copy(a, b):
        return remote(
            gsumd, gfull.at[:, share_of(0, 0)], gain_send.at[1], gain_recv.at[1],
            {**tensor_at(a), **dp_at(b)},
        )

    def gain_all(step):
        at = grecv.at[pl.ds(1, n * reps - 1)]
        return remote(at, at, gain_send.at[step], gain_recv.at[step], tensor_at(1))

    def spread_gain():
        with jax.named_scope("spread_gain"):
            gain_all(0).wait_recv()
        total = gtot[:, share_of(0, 0)]
        for a, b in mates:
            total = total + grecv[a * reps + b]
        gsumd[...] = total
        gfull[:, share_of(0, 0)] = total
        for a, b in mates:
            spread_copy(a, b).start()

    def gain_lanes(m):
        return pl.ds(m * width, width)

    def swap(values):
        wide = values.shape[1]
        lane = lax.broadcasted_iota(jnp.int32, values.shape, 1)
        low = lax.rem(lane, HD) < HD // 2
        return jnp.where(
            low, pltpu.roll(values, wide - HD // 2, 1), pltpu.roll(values, HD // 2, 1)
        )

    def dot(a, b, ca, cb):
        return lax.dot_general(a, b, (((ca,), (cb,)), ((), ())), preferred_element_type=f32)

    def stack_heads(values):
        return jnp.concatenate([values[:, h * HD : (h + 1) * HD] for h in range(GROUP)], axis=0)

    def spread_heads(values):
        return jnp.concatenate(
            [values[h * length : (h + 1) * length] for h in range(GROUP)], axis=1
        )

    def table(ref, wide):
        return jnp.concatenate([ref[...]] * (wide // 128), axis=1)

    span = (GROUP + 2) * HD

    def forward(t, m):
        u = unit_of(t, m)
        projected = dot(nrm[m, whole(t)], wq[m], 1, 0)
        rotated = projected * table(cos_ref, cols) + swap(projected) * table(sin_ref, cols)
        rotated = rotated.astype(bf16)
        row = lax.broadcasted_iota(jnp.int32, (length, length), 0)
        key_row = lax.broadcasted_iota(jnp.int32, (length, length), 1)
        bias = jnp.where(row >= key_row, 0.0, -1e30)
        for g in range(groups):
            at = g * span
            qs = stack_heads(rotated[:, at : at + GROUP * HD])
            key = rotated[:, at + GROUP * HD : at + (GROUP + 1) * HD]
            value = projected[:, at + (GROUP + 1) * HD : at + span].astype(bf16)
            scores = dot(qs, key, 1, 1) * scale
            scores = (scores.reshape(GROUP, length, length) + bias[None]).reshape(
                GROUP * length, length
            )
            e = jnp.exp(scores - jnp.max(scores, axis=-1, keepdims=True))
            sm = e / jnp.sum(e, axis=-1, keepdims=True)
            smb[u, g] = sm
            qsb[u, g] = qs
            kb[u, g] = key
            vb[u, g] = value
            attended = spread_heads(dot(sm.astype(bf16), value, 1, 0).astype(bf16))
            attb[m, whole(t), g * GROUP * HD : (g + 1) * GROUP * HD] = attended
        for j in others:
            rest_peer(3, t, m, j).start()

    def backward(t, m):
        u = unit_of(t, m)
        grad_att = dot(dyb[m, whole(t)], wo[m], 1, 1).astype(bf16)
        for g in range(groups):
            sm = smb[u, g]
            low = sm.astype(bf16)
            value = vb[u, g]
            gs = stack_heads(grad_att[:, g * GROUP * HD : (g + 1) * GROUP * HD])
            gsm = dot(gs, value, 1, 1)
            total = jnp.sum(sm * gsm, axis=-1, keepdims=True)
            gsc = (sm * (gsm - total) * scale).astype(bf16)
            g_value = dot(low, gs, 0, 0)
            g_query = spread_heads(dot(gsc, kb[u, g], 1, 0))
            g_key = dot(gsc, qsb[u, g], 0, 0)
            turned = jnp.concatenate([g_query, g_key, g_value], axis=1)
            back = turned * table(cos_ref, span) - swap(turned) * table(sin_ref, span)
            lane = lax.broadcasted_iota(jnp.int32, turned.shape, 1)
            back = jnp.where(lane < (GROUP + 1) * HD, back, turned)
            gpb[m, whole(t), g * span : (g + 1) * span] = back.astype(bf16)
        pb[u] = dot(gpb[m, whole(t)], wq[m], 1, 1).astype(bf16)
        if is_last(t, m):
            gain_of_parts(t, m)
            for a, b in mates:
                share_copy(a, b).start()
        for d in range(n - 1, 0, -1):
            sum_step(t, m, 0, d)
        if (t, m) == (ticks - 1, 1):
            gain_of_parts(t, m)
        for j in others:
            rest_peer(2, t, m, j).start()

    def finish(t, m):
        u = unit_of(t, m)
        x = xb[u].astype(f32)
        inverse = lax.rsqrt(jnp.mean(x * x, axis=-1, keepdims=True) + epsilon)
        unit = x * inverse
        mine = pl.ds(pl.multiple_of(me * own, own), own)
        gsum[...] = pb[u, mine].astype(f32)
        for way in (1, 0):

            @pl.when(me > 0 if way else me < n - 1)
            def _():
                with jax.named_scope("wait_scatter"):
                    for h in range(sum_parts(t, m)):
                        sum_arrived(t, m, 0, h, way)
                gsum[...] = gsum[...] + rb[u, way, 0].astype(f32)

        gn = gsum[...]
        gu = gn * gain[m]
        grad = inverse * (gu - unit * jnp.mean(gu * unit, axis=-1, keepdims=True))
        out[u] = (dyb[m, at_rows(t, me)].astype(f32) + grad).astype(bf16)
        if t + 1 < ticks:
            at = gain_lanes(m)
            gtot[:, at] = gtot[:, at] + jnp.sum(gn * unit, axis=0, keepdims=True)

    def gain_of_parts(t, m):
        part = pb[unit_of(t, m)].astype(f32) * nrm[m, whole(t)].astype(f32)
        at = gain_lanes(m)
        gtot[:, at] = gtot[:, at] + jnp.sum(part, axis=0, keepdims=True) / gain[m]

    def hand_over(t, m):
        if t + 1 == ticks:
            return

        @pl.when(sec < sections - 1 if m == 1 else sec > 0)
        def _():
            section_copy(t, m).start()

        if m == 1:

            @pl.when(sec == sections - 1)
            def _():
                dyb[0, at_rows(t + 1, me)] = out[unit_of(t, 1)]

    def taken_over(t, m):
        with jax.named_scope("wait_section"):

            @pl.when(sec > 0 if m == 1 else sec < sections - 1)
            def _():
                section_copy(t - 1, m).wait_recv()

            if m == 1:

                @pl.when(sec == 0)
                def _():
                    top_copies[t - 1].wait()

    def wait_peers(m, *kinds):
        with jax.named_scope("wait_dp"):
            for which in kinds:
                for j in others:
                    peer_layer(which, m, j).wait_recv()

    def rounded(a, b):
        return dot(a, b, 0, 0).astype(bf16).astype(f32)

    def grad_out(m, own=True, peers=True):
        wide = 512 if width % 512 == 0 else 128
        att_at = pl.ds(pl.multiple_of(rep * wa, 128), wa)

        @pl.loop(0, width // wide)
        def _(c):
            at = pl.ds(pl.multiple_of(c * wide, 128), wide)
            if own:
                total = rounded(attb[m, :, att_at], dyb[m, :, at])
            else:
                total = go_out[m, :, at].astype(f32)
            for j in others if peers else ():
                total = total + rounded(patt[j - 1, m], pdy[j - 1, m, :, at])
            go_out[m, :, at] = total.astype(bf16)

    def grad_qkv(m, own=True, peers=True):
        block = 256 if wn % 256 == 0 else 128

        @pl.loop(0, wn // block)
        def _(c):
            own_at = pl.ds(pl.multiple_of(rep * wn + c * block, 128), block)
            at = pl.ds(pl.multiple_of(c * block, 128), block)
            if own:
                total = rounded(nrm[m, :, own_at], gpb[m])
            else:
                total = gq_out[m, at].astype(f32)
            for j in others if peers else ():
                total = total + rounded(pnrm[j - 1, m, :, at], pgp[j - 1, m])
            gq_out[m, at] = total.astype(bf16)

    def grads_of(m, own=True):
        wait_peers(m, 1, 3)
        with jax.named_scope("grad_out"):
            grad_out(m, own)
        wait_peers(m, 0, 2)
        with jax.named_scope("grad_qkv"):
            grad_qkv(m, own)

    inner = range(1, n - 1)
    dy, x = 1, 0
    both = (dy, x)

    carry_copies[0].wait()
    own_hops(dy, 0, 1)
    own_to_peers(dy, 0, 1)
    small[0].wait()
    normalize(0, 1)
    own_hops(x, 0, 1)
    own_to_peers(x, 0, 1)
    carry_copies[1].wait()
    own_to_peers(dy, 0, 0)
    for t, m in order[1:]:
        normalize(t, m)
        own_to_peers(x, t, m)
    for c in w_copies:
        c.start()
    fwd(both, 0, 1, *inner)
    end(both, 0, 1, *inner)
    for which in both:
        own_hops(which, 0, 0)
    with jax.named_scope("wait_weights"):
        for c in w_copies:
            c.wait()
        for c in small[1:]:
            c.wait()
    end(both, 0, 1, n - 1)
    with jax.named_scope("forward"):
        forward(0, 1)
    with jax.named_scope("backward"):
        backward(0, 1)
    own_hops(x, 1, 1, edge=True)
    fwd(both, 0, 0, 1)
    end(both, 0, 0, 1)
    fwd(both, 0, 0, *inner[1:])
    end(both, 0, 0, *inner[1:])

    def give(which, t, m):
        fwd((which,), t, m, 1, source="middle")
        fwd((which,), t, m, 1, source="edge")

    for t in range(1, ticks):
        late = both if t == 1 else (dy,)
        if t > 1:
            own_hops(x, t, 1, edge=True)
        sums_far(t - 1, 1)
        end(late, t - 1, 0, n - 1)
        if t == 1:
            with jax.named_scope("forward"):
                forward(t - 1, 0)
        sums_near(t - 1, 1)
        own_hops(x, t, 1, edge=False)
        with jax.named_scope("backward"):
            backward(t - 1, 0)
        give(x, t, 1)
        finish(t - 1, 1)
        hand_over(t - 1, 1)
        fwd((x,), t, 1, *inner[1:])
        end((x,), t, 1, 1)
        taken_over(t, 1)
        own_to_peers(dy, t, 1)
        own_hops(dy, t, 1)
        end((x,), t, 1, *far[1:-1])
        fwd((dy,), t, 1, 1, source="middle")
        end((x,), t, 1, n - 1)
        with jax.named_scope("forward"):
            forward(t, 1)
        own_hops(x, t, 0, edge=True)
        sums_far(t - 1, 0)
        fwd((dy,), t, 1, 1, source="edge")
        sums_near(t - 1, 0)
        fwd((dy,), t, 1, *inner[1:])
        own_hops(x, t, 0, edge=False)
        end((dy,), t, 1, *far[:-1])
        finish(t - 1, 0)
        hand_over(t - 1, 0)
        give(x, t, 0)
        end((dy,), t, 1, n - 1)
        taken_over(t, 0)
        own_to_peers(dy, t, 0)
        own_hops(dy, t, 0)
        with jax.named_scope("backward"):
            backward(t, 1)
        fwd((x,), t, 0, *inner[1:])
        end((x,), t, 0, 1)
        end((x,), t, 0, *far[1:-1])
        give(dy, t, 0)
        end((x,), t, 0, n - 1)
        with jax.named_scope("forward"):
            forward(t, 0)
        fwd((dy,), t, 0, *inner[1:])
        if t + 1 == ticks:
            sums_far(t, 1)
        end((dy,), t, 0, *(far if t + 1 == ticks else far[:-1]))

    last = ticks - 1
    with jax.named_scope("backward"):
        backward(last, 0)
    sums_near(last, 1)
    grads_of(1)
    with jax.named_scope("own_grads"):
        grad_out(0, peers=False)
        grad_qkv(0, peers=False)
    sums_far(last, 0)
    finish(last, 1)
    spread_gain()
    sums_near(last, 0)
    grads_of(0, own=False)
    gain_all(1).wait_recv()
    for m in (1, 0):
        gain_out[m] = gfull[:, gain_lanes(m)]
    with jax.named_scope("wait_sends"):
        sums_sent()
        for which in both:
            hops_sent(which)
        for j in others:
            for which in range(4):
                peer_all(which, j).wait_send()
        for t in range(ticks - 1):

            @pl.when(sec < sections - 1)
            def _():
                section_copy(t, 1).wait_send()

            @pl.when(sec > 0)
            def _():
                section_copy(t, 0).wait_send()

        for step in (0, 1):
            gain_all(step).wait_send()

    finish(last, 0)


def write_back(a, b, c, d, a_out, b_out, c_out, d_out, sem):
    pairs = ((a, a_out), (b, b_out), (c, c_out), (d, d_out))
    copies = [pltpu.make_async_copy(src, dst, sem.at[k]) for k, (src, dst) in enumerate(pairs)]
    for c in copies:
        c.start()
    for c in copies:
        c.wait()


def lane_tables(length):
    cosine, sine = rope_tables(jnp.arange(length), HD)
    copies = 128 // HD
    cosine = jnp.tile(jnp.concatenate([cosine, cosine], axis=1), (1, copies))
    sine = jnp.tile(jnp.concatenate([-sine, sine], axis=1), (1, copies))
    return cosine, sine


def local(layer_in, carry_in, top_grad, w_qkv, w_out, gain):
    ticks, own, width = layer_in.shape[0], layer_in.shape[4], layer_in.shape[5]
    n = lax.axis_size("tensor")
    reps = lax.axis_size("dp")
    sections = lax.axis_size("section")
    cols, hq = w_qkv.shape[3], w_out.shape[2]
    share = 2 * width // (n * reps)
    lined = share * n * reps == 2 * width and share % 128 == 0
    lined = lined and (width // reps) % 128 == 0 and (hq // reps) % 128 == 0 and cols % 128 == 0
    if not lined or own % 16 or ticks < 2 or n < 3:
        return local_permutes(layer_in, carry_in, top_grad, w_qkv, w_out, gain)
    length = n * own
    units = 2 * ticks
    deep = ticks * length
    groups = hq // (GROUP * HD)
    wn, wa = width // reps, hq // reps
    f32, bf16 = jnp.float32, jnp.bfloat16
    parts = PARTS if width % (PARTS * 128) == 0 else 1
    last_parts = LAST_PARTS if width % (LAST_PARTS * 128) == 0 else 1
    with jax.ensure_compile_time_eval():
        cosine, sine = lane_tables(length)
    vmem = pl.BlockSpec(memory_space=pltpu.VMEM)
    hbm = pl.BlockSpec(memory_space=pl.ANY)
    dma = pltpu.SemaphoreType.DMA
    outs = pl.pallas_call(
        functools.partial(fused, n, reps, ticks, sections, own),
        out_shape=(
            pltpu.VMEM((units, own, width), bf16),
            pltpu.VMEM((2, wn, cols), bf16),
            pltpu.VMEM((2, wa, width), bf16),
            pltpu.VMEM((2, 1, width), f32),
        ),
        in_specs=[hbm] * 8,
        out_specs=(vmem,) * 4,
        scratch_shapes=[
            pltpu.VMEM((2, width, cols), bf16),
            pltpu.VMEM((2, hq, width), bf16),
            pltpu.VMEM((units, own, width), bf16),
            pltpu.VMEM((2, 1, width), f32),
            pltpu.VMEM((length, 128), f32),
            pltpu.VMEM((length, 128), f32),
            pltpu.VMEM((2, deep, width), bf16),
            pltpu.VMEM((2, deep, width), bf16),
            pltpu.VMEM((2, deep, cols), bf16),
            pltpu.VMEM((2, deep, hq), bf16),
            pltpu.VMEM((reps - 1, 2, deep, wn), bf16),
            pltpu.VMEM((reps - 1, 2, deep, width), bf16),
            pltpu.VMEM((reps - 1, 2, deep, cols), bf16),
            pltpu.VMEM((reps - 1, 2, deep, wa), bf16),
            pltpu.VMEM((units, length, width), bf16),
            pltpu.VMEM((units, 2, n - 1, own, width), bf16),
            pltpu.VMEM((units, groups, GROUP * length, length), f32),
            pltpu.VMEM((units, groups, GROUP * length, HD), bf16),
            pltpu.VMEM((units, groups, length, HD), bf16),
            pltpu.VMEM((units, groups, length, HD), bf16),
            pltpu.VMEM((1, 2 * width), f32),
            pltpu.VMEM((n * reps, 1, share), f32),
            pltpu.VMEM((1, share), f32),
            pltpu.VMEM((1, 2 * width), f32),
            pltpu.VMEM((own, width), f32),
            dma((2, 2)),
            dma((units,)),
            dma((1 + ticks,)),
            dma((3,)),
            dma((2, 2)),
            dma((2, units, parts, n)),
            dma((2,)),
            dma((units - 1, 2, n - 1, parts)),
            dma((2, n - 1, last_parts)),
            dma((ticks - 1, 2)),
            dma((ticks - 1, 2)),
            dma((4, reps - 1)),
            dma((4, 2, reps - 1)),
            dma((2,)),
            dma((2,)),
        ],
        compiler_params=pltpu.CompilerParams(
            collective_id=0, has_side_effects=True, vmem_limit_bytes=50 * 1024 * 1024
        ),
    )(
        layer_in[:, :, 0, 0].reshape(units, own, width),
        carry_in[:, 0, 0],
        top_grad[:, 0],
        gain,
        w_qkv[:, 0],
        w_out[:, 0],
        cosine,
        sine,
    )
    outs = pl.pallas_call(
        write_back,
        out_shape=(
            jax.ShapeDtypeStruct((units, own, width), bf16),
            jax.ShapeDtypeStruct((2, wn, cols), bf16),
            jax.ShapeDtypeStruct((2, wa, width), bf16),
            jax.ShapeDtypeStruct((2, 1, width), f32),
        ),
        in_specs=[vmem] * 4,
        out_specs=(hbm,) * 4,
        scratch_shapes=[dma((4,))],
        compiler_params=pltpu.CompilerParams(vmem_limit_bytes=1024 * 1024),
    )(*[pltpu.with_memory_space_constraint(o, pltpu.VMEM) for o in outs])
    return (
        outs[0].reshape(ticks, 2, 1, 1, own, width),
        outs[1][:, None],
        outs[2][:, None],
        outs[3],
    )


def solution(mesh):
    in_specs = (
        P(None, None, "section", "dp", "tensor", None),
        P(None, "section", "dp", "tensor", None),
        P(None, "dp", "tensor", None),
        P(None, "section", None, "tensor"),
        P(None, "section", "tensor", None),
        P(None, "section", None),
    )
    out_specs = (
        P(None, None, "section", "dp", "tensor", None),
        P(None, "section", "dp", "tensor"),
        P(None, "section", ("tensor", "dp"), None),
        P(None, "section", None),
    )
    return jax.shard_map(local, mesh=mesh, in_specs=in_specs, out_specs=out_specs, check_vma=False)
```

```python
import functools
import math

import jax
import jax.numpy as jnp
from jax import lax
from jax.experimental import pallas as pl
from jax.experimental.pallas import tpu as pltpu
from jax.sharding import PartitionSpec as P

HD = 64
GROUP = 8

epsilon = 1e-06
rope_base = 1000000.0


MESH = pl.DeviceIdType.MESH
PARTS = 2
LAST_PARTS = 4

contract_rows = (((0,), (0,)), ((), ()))
contract_cols = (((1,), (1,)), ((), ()))


def from_behind(value, axis, steps):
    count = lax.axis_size(axis)
    first, last = (max(0, -steps), min(count, count - steps))
    return lax.ppermute(value, axis, [(source, source + steps) for source in range(first, last)])


def from_ahead(value, axis, steps):
    count = lax.axis_size(axis)
    return lax.ppermute(value, axis, [((i + steps) % count, i) for i in range(count)])


def rope_tables(positions, head_width):
    half_width = head_width // 2
    exponent = jnp.arange(half_width, dtype=jnp.float32) * (2.0 / head_width)
    frequency = rope_base ** (-exponent)
    angle = positions.astype(jnp.float32)[:, None] * frequency[None, :]
    return (jnp.cos(angle), jnp.sin(angle))


def rotate(values, cosine_table, sine_table, direction):
    half_width = values.shape[-1] // 2
    table_shape = (values.shape[0],) + (1,) * (values.ndim - 2) + (half_width,)
    cosine = cosine_table.reshape(table_shape)
    sine_part = direction * sine_table.reshape(table_shape)
    lower_half = values[..., :half_width]
    upper_half = values[..., half_width:]
    return jnp.concatenate(
        [
            lower_half * cosine - upper_half * sine_part,
            upper_half * cosine + lower_half * sine_part,
        ],
        axis=-1,
    )


def unit_compute(normed, grad_full, w_qkv, w_out, tables, mask):
    length = normed.shape[0]
    kv_local = w_out.shape[0] // (GROUP * HD)
    cosine_table, sine_table = tables
    score_scale = 1.0 / math.sqrt(HD)
    projected = jnp.dot(normed, w_qkv, preferred_element_type=jnp.float32)
    projected = projected.reshape(length, kv_local, GROUP + 2, HD)
    query_rot = rotate(projected[:, :, :GROUP], cosine_table, sine_table, 1.0).astype(jnp.bfloat16)
    key_rot = rotate(projected[:, :, GROUP], cosine_table, sine_table, 1.0).astype(jnp.bfloat16)
    value_rows = projected[:, :, GROUP + 1].astype(jnp.bfloat16)
    f32 = dict(preferred_element_type=jnp.float32)
    scores = jnp.einsum("tkgd,ukd->kgtu", query_rot, key_rot, **f32) * score_scale
    scores = jnp.where(mask, scores, -1e30)
    exponentials = jnp.exp(scores - jnp.max(scores, axis=-1, keepdims=True))
    softmax_rows = exponentials / jnp.sum(exponentials, axis=-1, keepdims=True)
    softmax_low = softmax_rows.astype(jnp.bfloat16)
    attended = jnp.einsum("kgtu,ukd->tkgd", softmax_low, value_rows, **f32)
    attended = attended.astype(jnp.bfloat16).reshape(length, kv_local * GROUP * HD)
    grad_attended = lax.dot_general(grad_full, w_out, contract_cols, **f32).astype(jnp.bfloat16)
    grad_heads = grad_attended.reshape(length, kv_local, GROUP, HD)
    grad_softmax = jnp.einsum("tkgd,ukd->kgtu", grad_heads, value_rows, **f32)
    row_total = jnp.sum(softmax_rows * grad_softmax, axis=-1, keepdims=True)
    grad_scores = (softmax_rows * (grad_softmax - row_total) * score_scale).astype(jnp.bfloat16)
    grad_value = jnp.einsum("kgtu,tkgd->ukd", softmax_low, grad_heads, **f32)
    grad_query = rotate(
        jnp.einsum("kgtu,ukd->tkgd", grad_scores, key_rot, **f32), cosine_table, sine_table, -1.0
    )
    grad_key = rotate(
        jnp.einsum("kgtu,tkgd->ukd", grad_scores, query_rot, **f32), cosine_table, sine_table, -1.0
    )
    grad_projected = jnp.concatenate(
        [grad_query, grad_key[:, :, None], grad_value[:, :, None]], axis=2
    )
    grad_projected = grad_projected.reshape(length, kv_local * (GROUP + 2) * HD)
    grad_projected = grad_projected.astype(jnp.bfloat16)
    partial = lax.dot_general(grad_projected, w_qkv, contract_cols, **f32).astype(jnp.bfloat16)
    return attended, grad_projected, partial


def local_permutes(layer_in, carry_in, top_grad, w_qkv, w_out, gain):
    ticks = layer_in.shape[0]
    own = layer_in.shape[4]
    n_tensor = lax.axis_size("tensor")
    n_dp = lax.axis_size("dp")
    me_tensor = lax.axis_index("tensor")
    me_dp = lax.axis_index("dp")
    section_index = lax.axis_index("section")
    at_first = section_index == 0
    at_last = section_index == lax.axis_size("section") - 1
    owners = (me_tensor + jnp.arange(n_tensor)) % n_tensor
    positions = (owners[:, None] * own + jnp.arange(own)[None, :]).reshape(-1)
    tables = rope_tables(positions, HD)
    mask = positions[:, None] >= positions[None, :]
    layer_rows = layer_in[:, :, 0, 0]
    carried = carry_in[:, 0, 0]
    fresh_grads = top_grad[:, 0]
    weight_qkv = w_qkv[:, 0]
    weight_out = w_out[:, 0]
    gain_rows = gain[:, 0]

    def gather(value):
        return jnp.concatenate(
            [value] + [from_ahead(value, "tensor", k) for k in range(1, n_tensor)], axis=0
        )

    def scatter_sum(partial):
        total = partial[:own].astype(jnp.float32)
        for k in range(1, n_tensor):
            chunk = partial[k * own : (k + 1) * own]
            total = total + from_ahead(chunk, "tensor", -k).astype(jnp.float32)
        return total

    def columns_of(value, index):
        width = value.shape[1] // n_dp
        return lax.dynamic_slice_in_dim(value, index * width, width, axis=1)

    def exchange(value, cut):
        if cut:
            return [columns_of(value, me_dp)] + [
                from_ahead(columns_of(value, (me_dp - k) % n_dp), "dp", k) for k in range(1, n_dp)
            ]
        return [value] + [from_ahead(value, "dp", k) for k in range(1, n_dp)]

    members = (1, 0)
    unit_rows, inverse, normed = {}, {}, {}
    for t in range(ticks):
        for m in members:
            rows = layer_rows[t, m].astype(jnp.float32)
            inverse[t, m] = lax.rsqrt(jnp.mean(rows * rows, axis=-1, keepdims=True) + epsilon)
            unit_rows[t, m] = rows * inverse[t, m]
            normed[t, m] = (unit_rows[t, m] * gain_rows[m]).astype(jnp.bfloat16)
    inputs = [carried[0], carried[1]]
    factors = {}
    per_tick = []
    gain_totals = [0.0, 0.0]
    for t in range(ticks):
        outcome = [None, None]
        for m in members:
            dy = inputs[m]
            full_normed = gather(normed[t, m])
            full_grad = gather(dy)
            attended, grad_projected, partial = unit_compute(
                full_normed, full_grad, weight_qkv[m], weight_out[m], tables, mask
            )
            factors[t, m] = (
                exchange(full_normed, True),
                exchange(grad_projected, False),
                exchange(attended, True),
                exchange(full_grad, False),
            )
            grad_normed = scatter_sum(partial)
            grad_unit = grad_normed * gain_rows[m]
            unit = unit_rows[t, m]
            grad_rows = inverse[t, m] * (
                grad_unit - unit * jnp.mean(grad_unit * unit, axis=-1, keepdims=True)
            )
            outcome[m] = (dy.astype(jnp.float32) + grad_rows).astype(jnp.bfloat16)
            gain_totals[m] = gain_totals[m] + jnp.sum(grad_normed * unit, axis=0)
        if t + 1 < ticks:
            upward = from_behind(outcome[1], "section", 1)
            downward = from_behind(outcome[0], "section", -1)
            inputs = [
                jnp.where(at_last, outcome[1], downward),
                jnp.where(at_first, fresh_grads[t], upward),
            ]
        per_tick.append(jnp.stack(outcome))

    def weight_grad(m, left, right):
        total = None
        for k in range(n_dp):
            a = jnp.concatenate([factors[t, m][left][k] for t in range(ticks)], axis=0)
            b = jnp.concatenate([factors[t, m][right][k] for t in range(ticks)], axis=0)
            part = lax.dot_general(a, b, contract_rows, preferred_element_type=jnp.float32)
            part = part.astype(jnp.bfloat16).astype(jnp.float32)
            total = part if total is None else total + part
        return total.astype(jnp.bfloat16)

    grad_qkv = jnp.stack([weight_grad(m, 0, 1) for m in (0, 1)])
    grad_out = jnp.stack([weight_grad(m, 2, 3) for m in (0, 1)])
    gain_total = lax.psum(jnp.stack(gain_totals), ("tensor", "dp"))
    return (
        jnp.stack(per_tick)[:, :, None, None],
        grad_qkv[:, None],
        grad_out[:, None],
        gain_total[:, None],
    )


def fused(
    n, reps, ticks, sections, own,
    x_hbm, carry, top, gain_hbm, wq_hbm, wo_hbm, cos_hbm, sin_hbm,
    out, gq_out, go_out, gain_out,
    wq, wo, xb, gain, cos_ref, sin_ref,
    nrm, dyb, gpb, attb, pnrm, pdy, pgp, patt, pb, rb, rd, smb, qsb, kb, vb, gtot, grecv, gsumd, gfull, gsum,
    w_sem, x_sem, c_sem, t_sem, g_send, g_recv, r_send, r_recv, l_recv, e_recv, s_send, s_recv, d_send, d_recv,
    gain_send, gain_recv,
):
    f32 = jnp.float32
    bf16 = jnp.bfloat16
    me = lax.axis_index("tensor")
    rep = lax.axis_index("dp")
    sec = lax.axis_index("section")
    length = n * own
    units = 2 * ticks
    hq = wo.shape[1]
    width = wq.shape[1]
    cols = wq.shape[2]
    groups = hq // (GROUP * HD)
    wn = width // reps
    wa = hq // reps
    scale = 1.0 / math.sqrt(HD)
    parts = PARTS if width % (PARTS * 128) == 0 else 1
    last_parts = LAST_PARTS if width % (LAST_PARTS * 128) == 0 else 1
    piece = width // parts

    def tensor_at(k):
        return {"tensor": lax.rem(me + k + n, n)}

    def dp_at(k):
        return {"dp": lax.rem(rep + k + reps, reps)}

    barrier = pltpu.get_barrier_semaphore()
    for a in range(n):
        for b in range(reps):
            if a or b:
                pl.semaphore_signal(
                    barrier, inc=1, device_id={**tensor_at(a), **dp_at(b)}, device_id_type=MESH
                )

    @pl.when(sec > 0)
    def _():
        pl.semaphore_signal(barrier, inc=1, device_id={"section": sec - 1}, device_id_type=MESH)

    @pl.when(sec < sections - 1)
    def _():
        pl.semaphore_signal(barrier, inc=1, device_id={"section": sec + 1}, device_id_type=MESH)

    def at_rows(t, i):
        return pl.ds(pl.multiple_of(t * length + i * own, own), own)

    def whole(t):
        return pl.ds(t * length, length)

    def lanes(h):
        return pl.ds(h * piece, piece)

    def unit_of(t, m):
        return 2 * t + m

    order = [(t, m) for t in range(ticks) for m in (1, 0)]

    x_copies = {}
    for t, m in order:
        u = unit_of(t, m)
        x_copies[t, m] = pltpu.make_async_copy(x_hbm.at[u], xb.at[u], x_sem.at[u])
    small = [
        pltpu.make_async_copy(src, dst, t_sem.at[k])
        for k, (src, dst) in enumerate(((gain_hbm, gain), (cos_hbm, cos_ref), (sin_hbm, sin_ref)))
    ]
    carry_copies = [
        pltpu.make_async_copy(carry.at[m], dyb.at[m, at_rows(0, me)], c_sem.at[m]) for m in (1, 0)
    ]
    top_copies = [
        pltpu.make_async_copy(top.at[t], dyb.at[1, at_rows(t + 1, me)], c_sem.at[2 + t])
        for t in range(ticks - 1)
    ]
    w_copies = [
        pltpu.make_async_copy(src.at[m], dst.at[m], w_sem.at[j, m])
        for m in (1, 0)
        for j, (src, dst) in enumerate(((wq_hbm, wq), (wo_hbm, wo)))
    ]
    carry_copies[0].start()
    small[0].start()
    x_copies[0, 1].start()
    carry_copies[1].start()
    for t, m in order[1:]:
        x_copies[t, m].start()
    for c in small[1:]:
        c.start()

    @pl.when(sec == 0)
    def _():
        for c in top_copies:
            c.start()

    def normalize(t, m):
        u = unit_of(t, m)
        x_copies[t, m].wait()
        x = xb[u].astype(f32)
        inverse = lax.rsqrt(jnp.mean(x * x, axis=-1, keepdims=True) + epsilon)
        nrm[m, at_rows(t, me)] = (x * inverse * gain[m]).astype(bf16)

    gtot[...] = jnp.zeros_like(gtot)
    neighbours = jnp.where(sec > 0, 1, 0) + jnp.where(sec < sections - 1, 1, 0)
    with jax.named_scope("barrier"):
        pl.semaphore_wait(barrier, n * reps - 1 + neighbours)

    def remote(src, dst, send, recv, where):
        return pltpu.make_async_remote_copy(
            src_ref=src, dst_ref=dst, send_sem=send, recv_sem=recv, device_id=where,
            device_id_type=MESH,
        )

    def hop(which, t, m, i, h, up):
        u = unit_of(t, m)
        at = (nrm, dyb)[which].at[m, at_rows(t, i), lanes(h)]
        return remote(
            at, at, g_send.at[which, up], g_recv.at[which, u, h, i],
            tensor_at(1 if up else -1),
        )

    def dy_peer(t, m, i, h, j):
        at = at_rows(t, i)
        return remote(
            dyb.at[m, at, lanes(h)], pdy.at[j - 1, m, at, lanes(h)],
            d_send.at[1, j - 1], d_recv.at[1, m, j - 1], dp_at(-j),
        )

    def nrm_peer(t, m, i, j):
        peer = lax.rem(rep - j + reps, reps)
        at = at_rows(t, i)
        return remote(
            nrm.at[m, at, pl.ds(pl.multiple_of(peer * wn, 128), wn)], pnrm.at[j - 1, m, at],
            d_send.at[0, j - 1], d_recv.at[0, m, j - 1], dp_at(-j),
        )

    def rest_peer(which, t, m, j):
        peer = lax.rem(rep - j + reps, reps)
        at = whole(t)
        src, dst = {
            2: (gpb.at[m, at], pgp),
            3: (attb.at[m, at, pl.ds(pl.multiple_of(peer * wa, 128), wa)], patt),
        }[which]
        return remote(
            src, dst.at[j - 1, m, at], d_send.at[which, j - 1], d_recv.at[which, m, j - 1],
            dp_at(-j),
        )

    def peer_layer(which, m, j):
        at = (pnrm, pdy, pgp, patt)[which].at[j - 1, m]
        return remote(at, at, d_send.at[which, j - 1], d_recv.at[which, m, j - 1], dp_at(-j))

    def peer_all(which, j):
        at = (pnrm, pdy, pgp, patt)[which].at[j - 1]
        return remote(at, at, d_send.at[which, j - 1], d_recv.at[which, 0, j - 1], dp_at(-j))

    others = range(1, reps)
    far = range(1, n)

    def to_peers(which, t, m, i, h):
        for j in others:
            if which:
                dy_peer(t, m, i, h, j).start()
            elif h == parts - 1:
                nrm_peer(t, m, i, j).start()

    def own_to_peers(which, t, m):
        for h in range(parts):
            to_peers(which, t, m, me, h)

    def own_hops(which, t, m, edge=None):
        for h in range(parts):
            for up in (1, 0):
                sends = me < n - 1 if up else me > 0
                if edge is not None:
                    sends = (me == 0 if up else me == n - 1) if edge else (me > 0) & (me < n - 1)

                @pl.when(sends)
                def _():
                    hop(which, t, m, me, h, up).start()

    def arrivals(which, t, m, d, forward, source):
        for h in range(parts):
            for up in (1, 0):
                i = me - d if up else me + d
                inside = me >= d if up else me + d < n
                if source == "edge":
                    inside = me == d if up else me + d == n - 1
                elif source == "middle":
                    inside = me > d if up else me + d < n - 1
                middle = me < n - 1 if up else me > 0
                edge = me == n - 1 if up else me == 0

                @pl.when(inside & (middle if forward else edge))
                def _():
                    with jax.named_scope("wait_fwd" if forward else "wait_end"):
                        hop(which, t, m, i, h, up).wait_recv()
                    if forward:
                        hop(which, t, m, i, h, up).start()
                    to_peers(which, t, m, i, h)

    def fwd(what, t, m, *ds, source=None):
        for d in ds:
            if 0 < d < n - 1:
                for which in what:
                    arrivals(which, t, m, d, True, source)

    def end(what, t, m, *ds):
        for d in ds:
            if 0 < d < n:
                for which in what:
                    arrivals(which, t, m, d, False, None)

    def is_last(t, m):
        return (t, m) == (ticks - 1, 0)

    def sum_parts(t, m):
        return last_parts if is_last(t, m) else parts

    def sum_lanes(t, m, h):
        wide = width // sum_parts(t, m)
        return pl.ds(h * wide, wide)

    def sum_sem(t, m, way, d, h):
        return l_recv.at[way, d, h] if is_last(t, m) else r_recv.at[order.index((t, m)), way, d, h]

    def sum_copy(t, m, d, h, way):
        u = unit_of(t, m)
        i = me + d if way else me - d
        at = sum_lanes(t, m, h)
        return remote(
            pb.at[u, pl.ds(pl.multiple_of(i * own, own), own), at], rb.at[u, way, d - 1, :, at],
            r_send.at[way], sum_sem(t, m, way, d - 1, h), tensor_at(1 if way else -1),
        )

    def sum_arrived(t, m, d, h, way):
        u = unit_of(t, m)
        at = rb.at[u, way, d, :, sum_lanes(t, m, h)]
        remote(at, at, r_send.at[way], sum_sem(t, m, way, d, h), tensor_at(1)).wait_recv()

    def straight(t, m, way):
        far_end = n - 1 if way else 0
        return remote(
            pb.at[unit_of(t, m), pl.ds(far_end * own, own)], rd.at[way], r_send.at[way],
            e_recv.at[way], {"tensor": far_end},
        )

    def sum_step(t, m, stage, d):
        u = unit_of(t, m)
        if is_last(t, m) and d == n - 1:
            for way in (1, 0):

                @pl.when(me == (0 if way else n - 1))
                def _():
                    straight(t, m, way).start()

            return
        incoming = stage > (1 if is_last(t, m) and stage + d == n - 1 else 0)
        for way in (1, 0):

            @pl.when(me == (stage if way else n - 1 - stage))
            def _():
                place = stage if way else n - 1 - stage
                i = place + d if way else place - d
                rows = pl.ds(i * own, own)
                for h in range(sum_parts(t, m)):
                    if incoming:
                        at = sum_lanes(t, m, h)
                        with jax.named_scope("wait_sum"):
                            sum_arrived(t, m, d, h, way)
                        total = pb[u, rows, at].astype(f32)
                        total = total + rb[u, way, d, :, at].astype(f32)
                        pb[u, rows, at] = total.astype(bf16)
                    sum_copy(t, m, d, h, way).start()

    def sums_far(t, m):
        if n > 3:
            sum_step(t, m, 1, n - 2)

    def sums_near(t, m):
        steps = [(stage, d) for stage in range(1, n - 1) for d in range(1, n - stage)]
        for stage, d in sorted(steps, key=lambda step: (-step[1], -step[0])):
            if d < n - 2 or n == 3:
                sum_step(t, m, stage, d)

    def sums_sent():
        for way in (1, 0):
            for stage in range(n - 1):

                @pl.when(me == (stage if way else n - 1 - stage))
                def _():
                    at = pb.at[:, pl.ds(0, (n - 1 - stage) * own)]
                    remote(at, at, r_send.at[way], r_send.at[way], tensor_at(1)).wait_send()

    def hops_sent(which):
        for up in (1, 0):
            for place in range(n):
                count = place + 1 if up else n - place
                if count < n or (place < n - 1 if up else place > 0):

                    @pl.when(me == place)
                    def _():
                        at = (nrm, dyb)[which].at[:, pl.ds(0, ticks * count * own)]
                        sem = g_send.at[which, up]
                        remote(at, at, sem, sem, tensor_at(1)).wait_send()

    def section_copy(t, m):
        step = 1 if m == 1 else -1
        return remote(
            out.at[unit_of(t, m)], dyb.at[m, at_rows(t + 1, me)], s_send.at[t, m],
            s_recv.at[t, m], {"section": sec + step},
        )

    share = 2 * width // n
    mates = [(a, b) for a in range(n) for b in range(reps) if a or b]

    def share_of(a):
        return pl.ds(pl.multiple_of(lax.rem(me + a, n) * share, 128), share)

    def share_copy(a, b):
        return remote(
            gtot.at[:, share_of(a)], grecv.at[a * reps + b], gain_send.at[0], gain_recv.at[0],
            {**tensor_at(a), **dp_at(b)},
        )

    def spread_copy(a):
        return remote(
            gsumd, gfull.at[:, share_of(0)], gain_send.at[1], gain_recv.at[1], tensor_at(a)
        )

    def gain_all(step):
        at = grecv.at[pl.ds(1, n - 1 if step else n * reps - 1)]
        return remote(at, at, gain_send.at[step], gain_recv.at[step], tensor_at(1))

    def spread_gain():
        with jax.named_scope("spread_gain"):
            gain_all(0).wait_recv()
        total = gtot[:, share_of(0)]
        for a, b in mates:
            total = total + grecv[a * reps + b]
        gsumd[...] = total
        gfull[:, share_of(0)] = total
        for a in far:
            spread_copy(a).start()

    def gain_lanes(m):
        return pl.ds(m * width, width)

    def swap(values):
        wide = values.shape[1]
        lane = lax.broadcasted_iota(jnp.int32, values.shape, 1)
        low = lax.rem(lane, HD) < HD // 2
        return jnp.where(
            low, pltpu.roll(values, wide - HD // 2, 1), pltpu.roll(values, HD // 2, 1)
        )

    def dot(a, b, ca, cb):
        return lax.dot_general(a, b, (((ca,), (cb,)), ((), ())), preferred_element_type=f32)

    def stack_heads(values):
        return jnp.concatenate([values[:, h * HD : (h + 1) * HD] for h in range(GROUP)], axis=0)

    def spread_heads(values):
        return jnp.concatenate(
            [values[h * length : (h + 1) * length] for h in range(GROUP)], axis=1
        )

    def table(ref, wide):
        return jnp.concatenate([ref[...]] * (wide // 128), axis=1)

    span = (GROUP + 2) * HD

    def forward(t, m):
        u = unit_of(t, m)
        projected = dot(nrm[m, whole(t)], wq[m], 1, 0)
        rotated = projected * table(cos_ref, cols) + swap(projected) * table(sin_ref, cols)
        rotated = rotated.astype(bf16)
        row = lax.broadcasted_iota(jnp.int32, (length, length), 0)
        key_row = lax.broadcasted_iota(jnp.int32, (length, length), 1)
        bias = jnp.where(row >= key_row, 0.0, -1e30)
        for g in range(groups):
            at = g * span
            qs = stack_heads(rotated[:, at : at + GROUP * HD])
            key = rotated[:, at + GROUP * HD : at + (GROUP + 1) * HD]
            value = projected[:, at + (GROUP + 1) * HD : at + span].astype(bf16)
            scores = dot(qs, key, 1, 1) * scale
            scores = (scores.reshape(GROUP, length, length) + bias[None]).reshape(
                GROUP * length, length
            )
            e = jnp.exp(scores - jnp.max(scores, axis=-1, keepdims=True))
            sm = e / jnp.sum(e, axis=-1, keepdims=True)
            smb[u, g] = sm
            qsb[u, g] = qs
            kb[u, g] = key
            vb[u, g] = value
            attended = spread_heads(dot(sm.astype(bf16), value, 1, 0).astype(bf16))
            attb[m, whole(t), g * GROUP * HD : (g + 1) * GROUP * HD] = attended
        for j in others:
            rest_peer(3, t, m, j).start()

    def backward(t, m):
        u = unit_of(t, m)
        grad_att = dot(dyb[m, whole(t)], wo[m], 1, 1).astype(bf16)
        for g in range(groups):
            sm = smb[u, g]
            low = sm.astype(bf16)
            value = vb[u, g]
            gs = stack_heads(grad_att[:, g * GROUP * HD : (g + 1) * GROUP * HD])
            gsm = dot(gs, value, 1, 1)
            total = jnp.sum(sm * gsm, axis=-1, keepdims=True)
            gsc = (sm * (gsm - total) * scale).astype(bf16)
            g_value = dot(low, gs, 0, 0)
            g_query = spread_heads(dot(gsc, kb[u, g], 1, 0))
            g_key = dot(gsc, qsb[u, g], 0, 0)
            turned = jnp.concatenate([g_query, g_key, g_value], axis=1)
            back = turned * table(cos_ref, span) - swap(turned) * table(sin_ref, span)
            lane = lax.broadcasted_iota(jnp.int32, turned.shape, 1)
            back = jnp.where(lane < (GROUP + 1) * HD, back, turned)
            gpb[m, whole(t), g * span : (g + 1) * span] = back.astype(bf16)
        pb[u] = dot(gpb[m, whole(t)], wq[m], 1, 1).astype(bf16)
        if is_last(t, m):
            gain_of_parts(t, m)
            for a, b in mates:
                share_copy(a, b).start()
        for d in range(n - 1, 1 if is_last(t, m) else 0, -1):
            sum_step(t, m, 0, d)
        if (t, m) == (ticks - 1, 1):
            gain_of_parts(t, m)
        for j in others:
            rest_peer(2, t, m, j).start()

    def finish(t, m):
        u = unit_of(t, m)
        x = xb[u].astype(f32)
        inverse = lax.rsqrt(jnp.mean(x * x, axis=-1, keepdims=True) + epsilon)
        unit = x * inverse
        mine = pl.ds(pl.multiple_of(me * own, own), own)
        gsum[...] = pb[u, mine].astype(f32)
        for way in (1, 0):

            @pl.when(me > 0 if way else me < n - 1)
            def _():
                with jax.named_scope("wait_scatter"):
                    for h in range(sum_parts(t, m)):
                        sum_arrived(t, m, 0, h, way)
                gsum[...] = gsum[...] + rb[u, way, 0].astype(f32)

        if is_last(t, m):
            for way in (1, 0):

                @pl.when(me == (n - 1 if way else 0))
                def _():
                    with jax.named_scope("wait_straight"):
                        straight(t, m, way).wait_recv()
                    gsum[...] = gsum[...] + rd[way].astype(f32)

        gn = gsum[...]
        gu = gn * gain[m]
        grad = inverse * (gu - unit * jnp.mean(gu * unit, axis=-1, keepdims=True))
        out[u] = (dyb[m, at_rows(t, me)].astype(f32) + grad).astype(bf16)
        if t + 1 < ticks:
            at = gain_lanes(m)
            gtot[:, at] = gtot[:, at] + jnp.sum(gn * unit, axis=0, keepdims=True)

    def gain_of_parts(t, m):
        part = pb[unit_of(t, m)].astype(f32) * nrm[m, whole(t)].astype(f32)
        at = gain_lanes(m)
        gtot[:, at] = gtot[:, at] + jnp.sum(part, axis=0, keepdims=True) / gain[m]

    def hand_over(t, m):
        if t + 1 == ticks:
            return

        @pl.when(sec < sections - 1 if m == 1 else sec > 0)
        def _():
            section_copy(t, m).start()

        if m == 1:

            @pl.when(sec == sections - 1)
            def _():
                dyb[0, at_rows(t + 1, me)] = out[unit_of(t, 1)]

    def taken_over(t, m):
        with jax.named_scope("wait_section"):

            @pl.when(sec > 0 if m == 1 else sec < sections - 1)
            def _():
                section_copy(t - 1, m).wait_recv()

            if m == 1:

                @pl.when(sec == 0)
                def _():
                    top_copies[t - 1].wait()

    def wait_peers(m, *kinds):
        with jax.named_scope("wait_dp"):
            for which in kinds:
                for j in others:
                    peer_layer(which, m, j).wait_recv()

    def rounded(a, b):
        return dot(a, b, 0, 0).astype(bf16).astype(f32)

    def grad_out(m, own=True, peers=True):
        wide = 512 if width % 512 == 0 else 128
        att_at = pl.ds(pl.multiple_of(rep * wa, 128), wa)

        @pl.loop(0, width // wide)
        def _(c):
            at = pl.ds(pl.multiple_of(c * wide, 128), wide)
            if own:
                total = rounded(attb[m, :, att_at], dyb[m, :, at])
            else:
                total = go_out[m, :, at].astype(f32)
            for j in others if peers else ():
                total = total + rounded(patt[j - 1, m], pdy[j - 1, m, :, at])
            go_out[m, :, at] = total.astype(bf16)

    def grad_qkv(m, own=True, peers=True):
        block = 256 if wn % 256 == 0 else 128

        @pl.loop(0, wn // block)
        def _(c):
            own_at = pl.ds(pl.multiple_of(rep * wn + c * block, 128), block)
            at = pl.ds(pl.multiple_of(c * block, 128), block)
            if own:
                total = rounded(nrm[m, :, own_at], gpb[m])
            else:
                total = gq_out[m, at].astype(f32)
            for j in others if peers else ():
                total = total + rounded(pnrm[j - 1, m, :, at], pgp[j - 1, m])
            gq_out[m, at] = total.astype(bf16)

    def grads_of(m, own=True):
        wait_peers(m, 1, 3)
        with jax.named_scope("grad_out"):
            grad_out(m, own)
        wait_peers(m, 0, 2)
        with jax.named_scope("grad_qkv"):
            grad_qkv(m, own)

    inner = range(1, n - 1)
    dy, x = 1, 0
    both = (dy, x)

    carry_copies[0].wait()
    own_hops(dy, 0, 1)
    own_to_peers(dy, 0, 1)
    small[0].wait()
    normalize(0, 1)
    own_hops(x, 0, 1)
    own_to_peers(x, 0, 1)
    carry_copies[1].wait()
    own_to_peers(dy, 0, 0)
    for t, m in order[1:]:
        normalize(t, m)
        own_to_peers(x, t, m)
    for c in w_copies:
        c.start()
    fwd(both, 0, 1, *inner)
    end(both, 0, 1, *inner)
    for which in both:
        own_hops(which, 0, 0)
    with jax.named_scope("wait_weights"):
        for c in w_copies:
            c.wait()
        for c in small[1:]:
            c.wait()
    end(both, 0, 1, n - 1)
    with jax.named_scope("forward"):
        forward(0, 1)
    with jax.named_scope("backward"):
        backward(0, 1)
    own_hops(x, 1, 1, edge=True)
    fwd(both, 0, 0, 1)
    end(both, 0, 0, 1)
    fwd(both, 0, 0, *inner[1:])
    end(both, 0, 0, *inner[1:])

    def give(which, t, m):
        fwd((which,), t, m, 1, source="middle")
        fwd((which,), t, m, 1, source="edge")

    for t in range(1, ticks):
        late = both if t == 1 else (dy,)
        if t > 1:
            own_hops(x, t, 1, edge=True)
        sums_far(t - 1, 1)
        end(late, t - 1, 0, n - 1)
        if t == 1:
            with jax.named_scope("forward"):
                forward(t - 1, 0)
        sums_near(t - 1, 1)
        own_hops(x, t, 1, edge=False)
        with jax.named_scope("backward"):
            backward(t - 1, 0)
        give(x, t, 1)
        finish(t - 1, 1)
        hand_over(t - 1, 1)
        fwd((x,), t, 1, *inner[1:])
        end((x,), t, 1, 1)
        taken_over(t, 1)
        own_to_peers(dy, t, 1)
        own_hops(dy, t, 1)
        end((x,), t, 1, *far[1:-1])
        fwd((dy,), t, 1, 1, source="middle")
        end((x,), t, 1, n - 1)
        with jax.named_scope("forward"):
            forward(t, 1)
        own_hops(x, t, 0, edge=True)
        sums_far(t - 1, 0)
        fwd((dy,), t, 1, 1, source="edge")
        sums_near(t - 1, 0)
        fwd((dy,), t, 1, *inner[1:])
        own_hops(x, t, 0, edge=False)
        end((dy,), t, 1, *far[:-1])
        finish(t - 1, 0)
        hand_over(t - 1, 0)
        give(x, t, 0)
        end((dy,), t, 1, n - 1)
        taken_over(t, 0)
        own_to_peers(dy, t, 0)
        own_hops(dy, t, 0)
        with jax.named_scope("backward"):
            backward(t, 1)
        fwd((x,), t, 0, *inner[1:])
        end((x,), t, 0, 1)
        end((x,), t, 0, *far[1:-1])
        give(dy, t, 0)
        end((x,), t, 0, n - 1)
        with jax.named_scope("forward"):
            forward(t, 0)
        fwd((dy,), t, 0, *inner[1:])
        if t + 1 == ticks:
            sums_far(t, 1)
        end((dy,), t, 0, *(far if t + 1 == ticks else far[:-1]))

    last = ticks - 1
    with jax.named_scope("backward"):
        backward(last, 0)
    sums_far(last, 0)
    sums_near(last, 1)
    grads_of(1)
    with jax.named_scope("own_grads"):
        grad_out(0, peers=False)
        grad_qkv(0, peers=False)
    spread_gain()
    sum_step(last, 0, 0, 1)
    sums_near(last, 0)
    finish(last, 1)
    grads_of(0, own=False)
    gain_all(1).wait_recv()
    for m in (1, 0):
        gain_out[m] = gfull[:, gain_lanes(m)]
    with jax.named_scope("wait_sends"):
        sums_sent()
        for which in both:
            hops_sent(which)
        for j in others:
            for which in range(4):
                peer_all(which, j).wait_send()
        for t in range(ticks - 1):

            @pl.when(sec < sections - 1)
            def _():
                section_copy(t, 1).wait_send()

            @pl.when(sec > 0)
            def _():
                section_copy(t, 0).wait_send()

        for step in (0, 1):
            gain_all(step).wait_send()

    finish(last, 0)


def write_back(a, b, c, d, a_out, b_out, c_out, d_out, sem):
    pairs = ((a, a_out), (b, b_out), (c, c_out), (d, d_out))
    copies = [pltpu.make_async_copy(src, dst, sem.at[k]) for k, (src, dst) in enumerate(pairs)]
    for c in copies:
        c.start()
    for c in copies:
        c.wait()


def lane_tables(length):
    cosine, sine = rope_tables(jnp.arange(length), HD)
    copies = 128 // HD
    cosine = jnp.tile(jnp.concatenate([cosine, cosine], axis=1), (1, copies))
    sine = jnp.tile(jnp.concatenate([-sine, sine], axis=1), (1, copies))
    return cosine, sine


def local(layer_in, carry_in, top_grad, w_qkv, w_out, gain):
    ticks, own, width = layer_in.shape[0], layer_in.shape[4], layer_in.shape[5]
    n = lax.axis_size("tensor")
    reps = lax.axis_size("dp")
    sections = lax.axis_size("section")
    cols, hq = w_qkv.shape[3], w_out.shape[2]
    share = 2 * width // n
    lined = share * n == 2 * width and share % 128 == 0
    lined = lined and (width // reps) % 128 == 0 and (hq // reps) % 128 == 0 and cols % 128 == 0
    if not lined or own % 16 or ticks < 2 or n < 3:
        return local_permutes(layer_in, carry_in, top_grad, w_qkv, w_out, gain)
    length = n * own
    units = 2 * ticks
    deep = ticks * length
    groups = hq // (GROUP * HD)
    wn, wa = width // reps, hq // reps
    f32, bf16 = jnp.float32, jnp.bfloat16
    parts = PARTS if width % (PARTS * 128) == 0 else 1
    last_parts = LAST_PARTS if width % (LAST_PARTS * 128) == 0 else 1
    with jax.ensure_compile_time_eval():
        cosine, sine = lane_tables(length)
    vmem = pl.BlockSpec(memory_space=pltpu.VMEM)
    hbm = pl.BlockSpec(memory_space=pl.ANY)
    dma = pltpu.SemaphoreType.DMA
    outs = pl.pallas_call(
        functools.partial(fused, n, reps, ticks, sections, own),
        out_shape=(
            pltpu.VMEM((units, own, width), bf16),
            pltpu.VMEM((2, wn, cols), bf16),
            pltpu.VMEM((2, wa, width), bf16),
            pltpu.VMEM((2, 1, width), f32),
        ),
        in_specs=[hbm] * 8,
        out_specs=(vmem,) * 4,
        scratch_shapes=[
            pltpu.VMEM((2, width, cols), bf16),
            pltpu.VMEM((2, hq, width), bf16),
            pltpu.VMEM((units, own, width), bf16),
            pltpu.VMEM((2, 1, width), f32),
            pltpu.VMEM((length, 128), f32),
            pltpu.VMEM((length, 128), f32),
            pltpu.VMEM((2, deep, width), bf16),
            pltpu.VMEM((2, deep, width), bf16),
            pltpu.VMEM((2, deep, cols), bf16),
            pltpu.VMEM((2, deep, hq), bf16),
            pltpu.VMEM((reps - 1, 2, deep, wn), bf16),
            pltpu.VMEM((reps - 1, 2, deep, width), bf16),
            pltpu.VMEM((reps - 1, 2, deep, cols), bf16),
            pltpu.VMEM((reps - 1, 2, deep, wa), bf16),
            pltpu.VMEM((units, length, width), bf16),
            pltpu.VMEM((units, 2, n - 1, own, width), bf16),
            pltpu.VMEM((2, own, width), bf16),
            pltpu.VMEM((units, groups, GROUP * length, length), f32),
            pltpu.VMEM((units, groups, GROUP * length, HD), bf16),
            pltpu.VMEM((units, groups, length, HD), bf16),
            pltpu.VMEM((units, groups, length, HD), bf16),
            pltpu.VMEM((1, 2 * width), f32),
            pltpu.VMEM((n * reps, 1, share), f32),
            pltpu.VMEM((1, share), f32),
            pltpu.VMEM((1, 2 * width), f32),
            pltpu.VMEM((own, width), f32),
            dma((2, 2)),
            dma((units,)),
            dma((1 + ticks,)),
            dma((3,)),
            dma((2, 2)),
            dma((2, units, parts, n)),
            dma((2,)),
            dma((units - 1, 2, n - 1, parts)),
            dma((2, n - 1, last_parts)),
            dma((2,)),
            dma((ticks - 1, 2)),
            dma((ticks - 1, 2)),
            dma((4, reps - 1)),
            dma((4, 2, reps - 1)),
            dma((2,)),
            dma((2,)),
        ],
        compiler_params=pltpu.CompilerParams(
            collective_id=0, has_side_effects=True, vmem_limit_bytes=50 * 1024 * 1024
        ),
    )(
        layer_in[:, :, 0, 0].reshape(units, own, width),
        carry_in[:, 0, 0],
        top_grad[:, 0],
        gain,
        w_qkv[:, 0],
        w_out[:, 0],
        cosine,
        sine,
    )
    outs = pl.pallas_call(
        write_back,
        out_shape=(
            jax.ShapeDtypeStruct((units, own, width), bf16),
            jax.ShapeDtypeStruct((2, wn, cols), bf16),
            jax.ShapeDtypeStruct((2, wa, width), bf16),
            jax.ShapeDtypeStruct((2, 1, width), f32),
        ),
        in_specs=[vmem] * 4,
        out_specs=(hbm,) * 4,
        scratch_shapes=[dma((4,))],
        compiler_params=pltpu.CompilerParams(vmem_limit_bytes=1024 * 1024),
    )(*[pltpu.with_memory_space_constraint(o, pltpu.VMEM) for o in outs])
    return (
        outs[0].reshape(ticks, 2, 1, 1, own, width),
        outs[1][:, None],
        outs[2][:, None],
        outs[3],
    )


def solution(mesh):
    in_specs = (
        P(None, None, "section", "dp", "tensor", None),
        P(None, "section", "dp", "tensor", None),
        P(None, "dp", "tensor", None),
        P(None, "section", None, "tensor"),
        P(None, "section", "tensor", None),
        P(None, "section", None),
    )
    out_specs = (
        P(None, None, "section", "dp", "tensor", None),
        P(None, "section", "dp", "tensor"),
        P(None, "section", ("tensor", "dp"), None),
        P(None, "section", None),
    )
    return jax.shard_map(local, mesh=mesh, in_specs=in_specs, out_specs=out_specs, check_vma=False)
```
